32 devices in a mesh: gx: 8 (over z, y), gy: 4 (over x, core).
Axes of the slice: x: 2, y: 2, z: 4, core: 2. Of those that a mesh axis runs over, the one named last changes fastest.
Arguments:
- checkpoint: float32 [16, 32, 1024], P(None, 'gy', 'gx'), may hold values from -6 to 6
- trajectory: float32 [16, 32, 1024], P(None, 'gy', 'gx'), may hold values from -6 to 6
- adjoint_forcing: float32 [16, 32, 1024], P(None, 'gy', 'gx'), may hold values from -6 to 6
- east_diffusion: float32 [16, 32, 1024], P(None, 'gy', 'gx'), may hold values from 0.1 to 1
- north_diffusion: float32 [16, 32, 1024], P(None, 'gy', 'gx'), may hold values from 0.3 to 3
- east_wind: float32 [16, 32, 1024], P(None, 'gy', 'gx'), may hold values from -0.6 to 0.6
- north_wind: float32 [16, 32, 1024], P(None, 'gy', 'gx'), may hold values from -6 to 6, as said below
- level_diffusion: float32 [16], replicated, may hold values from 0.1 to 1
- damping: float32 [16], replicated, may hold values from 0.2 to 2
- source: float32 [16, 32, 1024], P(None, 'gy', 'gx'), may hold values from -4 to 5
- observations: float32 [16, 32, 1024], P(None, 'gy', 'gx'), may hold values from -6 to 6
- observation_weight: float32 [16, 32, 1024], P(None, 'gy', 'gx'), may hold values from 0.1 to 1
- step_index: int32 [1], replicated, may hold values from 0 to 95
Outputs:
- forward_state: float32 [16, 32, 1024], P(None, 'gy', 'gx')
- forward_residual: float32 [16, 32, 1024], P(None, 'gy', 'gx')
- adjoint_state: float32 [16, 32, 1024], P(None, 'gy', 'gx')
The draws below stay inside these ranges and needn't reach their ends.
Inputs may be any that keep to these rules, and one draw needn't show every extreme that they name: At every face the magnitude of north_wind is at most twice north_diffusion.
All inputs are finite; a program needn't handle non-finite values.
Results may differ from the reference program's by a relative error of at most 0.000091.
Values sent between devices are 32-bit elements; how exact they have to be, the bound alone decides.
A program may use at most 64 MiB of HBM per device.

```python
import math
import jax
import jax.numpy as jnp

LEVELS = 16
OUTER = 2
INNER = 4
DAY_STEPS = 96
NLAT = 32
NLON = 1024


def draw_source(key, part):
    noise = jnp.clip(jax.random.normal(key, (LEVELS, NLAT, NLON), jnp.float32), -4.0, 4.0)
    return noise


def flow_parts(key):
    diffusion_key = jax.random.fold_in(key, 4101)
    speed_key = jax.random.fold_in(key, 4102)
    shape = (LEVELS, NLAT, NLON)
    low_log = math.log(0.3)
    high_log = math.log(3.0)
    speed_ratio = jax.random.uniform(speed_key, shape, jnp.float32, -2.0, 2.0)
    diffusion = jnp.exp(jax.random.uniform(diffusion_key, shape, jnp.float32, low_log, high_log))
    diffusion = jnp.clip(diffusion, 0.3, 3.0)
    speed_ratio = jnp.clip(speed_ratio, -2.0, 2.0)
    return (diffusion, diffusion * speed_ratio)


def draw_north_diffusion(key, part):
    return flow_parts(key)[0]


def draw_north_wind(key, part):
    return flow_parts(key)[1]


def level_of(own_key, shape, shards, low, top_value):
    loudness, own = 1.0, jax.random.fold_in(own_key, 6)
    for position, shards_of in shards:
        heights = jnp.exp(jax.random.uniform(jax.random.fold_in(own, position), (shards_of,), jnp.float32, low / len(shards), top_value / len(shards)))
        loudness = loudness * jnp.repeat(heights, shape[position] // shards_of).reshape([-1 if axis == position else 1 for axis in range(len(shape))])
    return loudness


def scatter_about(stream_key, extent, spread, most, pieces=(), kind=jnp.bfloat16):
    loudness = level_of(stream_key, extent, pieces, -0.22, 0.18) if pieces else 1.0
    values = jax.random.normal(stream_key, extent, jnp.float32) * spread * loudness
    return jnp.minimum(jnp.maximum(values, -most), most).astype(kind)


def setup_inputs(seed: int = 0) -> dict:
    streams_of = jax.random.split(jax.random.key(seed), 14)
    checkpoint = scatter_about(streams_of[0], (LEVELS, NLAT, NLON), 1.0, 6.0, ((1, 4), (2, 8)), jnp.float32)
    trajectory = scatter_about(streams_of[1], (LEVELS, NLAT, NLON), 1.0, 6.0, ((1, 4), (2, 8)), jnp.float32)
    adjoint_forcing = scatter_about(streams_of[2], (LEVELS, NLAT, NLON), 1.0, 6.0, ((1, 4), (2, 8)), jnp.float32)
    east_diffusion = jnp.clip(jnp.exp(math.log(1.0) - 2.3025851 * jax.random.uniform(streams_of[3], (LEVELS, NLAT, NLON), jnp.float32) ** level_of(streams_of[3], (LEVELS, NLAT, NLON), ((1, 4), (2, 8)), -0.2, 0.2)), 0.1, 1.0)
    north_diffusion = draw_north_diffusion(jax.random.fold_in(streams_of[13], 71), 0)
    east_wind = jnp.clip(jax.random.uniform(streams_of[5], (LEVELS, NLAT, NLON), jnp.float32, -0.6, 0.6) * level_of(streams_of[5], (LEVELS, NLAT, NLON), ((1, 4), (2, 8)), -0.4, 0.0), -0.6, 0.6)
    north_wind = draw_north_wind(jax.random.fold_in(streams_of[13], 71), 0)
    level_diffusion = jnp.clip(jnp.exp(jax.random.uniform(streams_of[7], (LEVELS,), jnp.float32, math.log(0.1), math.log(1.0))), 0.1, 1.0)
    damping = jnp.clip(jnp.exp(jax.random.uniform(streams_of[8], (LEVELS,), jnp.float32, math.log(0.2), math.log(2.0))), 0.2, 2.0)
    source = draw_source(jax.random.fold_in(streams_of[13], 71), 0)
    observations = scatter_about(streams_of[10], (LEVELS, NLAT, NLON), 1.0, 6.0, ((1, 4), (2, 8)), jnp.float32)
    observation_weight = jnp.clip(jnp.exp(math.log(1.0) - 2.3025851 * jax.random.uniform(streams_of[11], (LEVELS, NLAT, NLON), jnp.float32) ** level_of(streams_of[11], (LEVELS, NLAT, NLON), ((1, 4), (2, 8)), -0.2, 0.2)), 0.1, 1.0)
    step_index = jax.random.randint(streams_of[12], (1,), 0, DAY_STEPS).astype(jnp.int32)
    return {"checkpoint": checkpoint, "trajectory": trajectory, "adjoint_forcing": adjoint_forcing, "east_diffusion": east_diffusion, "north_diffusion": north_diffusion, "east_wind": east_wind, "north_wind": north_wind, "level_diffusion": level_diffusion, "damping": damping, "source": source, "observations": observations, "observation_weight": observation_weight, "step_index": step_index}


RELAXATION = 0.7


def vertical_part(field, up_coef):
    zero_level = jnp.zeros_like(field[:1])
    padded = jnp.concatenate([zero_level, field, zero_level], axis=0)
    flux = up_coef[:, None, None] * (padded[1:] - padded[:-1])
    return -(flux[1:] - flux[:-1])


def apply_forward(west_east, south_north, field, faces):
    east_coef, east_flow, north_coef, north_flow, up_coef = faces
    flux_east = east_flow * (west_east[..., 1:] + west_east[..., :-1]) * 0.5 - east_coef * (west_east[..., 1:] - west_east[..., :-1])
    flux_north = north_flow * (south_north[:, 1:] + south_north[:, :-1]) * 0.5 - north_coef * (south_north[:, 1:] - south_north[:, :-1])
    return (flux_east[..., 1:] - flux_east[..., :-1]) + (flux_north[:, 1:] - flux_north[:, :-1]) + vertical_part(field, up_coef)


def apply_transposed(west_east, south_north, field, faces):
    east_coef, east_flow, north_coef, north_flow, up_coef = faces
    jump_east = west_east[..., :-1] - west_east[..., 1:]
    lower_east = east_flow * 0.5 + east_coef
    upper_east = east_flow * 0.5 - east_coef
    part_east = jump_east[..., 1:] * lower_east[..., 1:] + jump_east[..., :-1] * upper_east[..., :-1]
    jump_north = south_north[:, :-1] - south_north[:, 1:]
    lower_north = north_flow * 0.5 + north_coef
    upper_north = north_flow * 0.5 - north_coef
    part_north = jump_north[:, 1:] * lower_north[:, 1:] + jump_north[:, :-1] * upper_north[:, :-1]
    return part_east + part_north + vertical_part(field, up_coef)


def diagonal_of(tangent, faces, damping):
    east_coef, east_flow, north_coef, north_flow, up_coef = faces
    total = 1.0 + east_coef[..., 1:] + east_coef[..., :-1] + north_coef[:, 1:] + north_coef[:, :-1]
    total = total + (up_coef[1:] + up_coef[:-1])[:, None, None]
    return total + damping[:, None, None] * (1.0 - tangent * tangent)


def global_faces(east_diffusion, north_diffusion, east_wind, north_wind, level_diffusion):
    levels, lat_rows, lon_cols = east_diffusion.shape
    row_mask = (jnp.arange(lat_rows) < lat_rows - 1).astype(jnp.float32)[None, :, None]
    level_mask = (jnp.arange(levels) < levels - 1).astype(jnp.float32)
    north_masked = north_diffusion * row_mask
    flow_masked = north_wind * row_mask
    zero_row = jnp.zeros_like(north_masked[:, :1])
    east_coef = jnp.concatenate([east_diffusion[..., -1:], east_diffusion], axis=2)
    east_flow = jnp.concatenate([east_wind[..., -1:], east_wind], axis=2)
    north_coef = jnp.concatenate([zero_row, north_masked], axis=1)
    north_flow = jnp.concatenate([zero_row, flow_masked], axis=1)
    up_coef = jnp.concatenate([jnp.zeros_like(level_diffusion[:1]), level_diffusion * level_mask])
    return east_coef, east_flow, north_coef, north_flow, up_coef


def wrap_east(field):
    return jnp.concatenate([field[..., -1:], field, field[..., :1]], axis=2)


def pad_north(field):
    zero_row = jnp.zeros_like(field[:, :1])
    return jnp.concatenate([zero_row, field, zero_row], axis=1)


def reference(checkpoint, trajectory, adjoint_forcing, east_diffusion, north_diffusion, east_wind, north_wind, level_diffusion, damping, source, observations, observation_weight, step_index):
    faces = global_faces(east_diffusion, north_diffusion, east_wind, north_wind, level_diffusion)
    levels, lat_rows, lon_cols = checkpoint.shape
    column = jnp.arange(lon_cols).astype(jnp.float32)
    phase = 2.0 * math.pi * column / lon_cols - 2.0 * math.pi * step_index[0].astype(jnp.float32) / DAY_STEPS
    forcing = source * jnp.cos(phase)[None, None, :]
    damp = damping[:, None, None]

    def operate(field):
        return apply_forward(wrap_east(field), pad_north(field), field, faces)

    def operate_transposed(field):
        return apply_transposed(wrap_east(field), pad_north(field), field, faces)

    state = checkpoint
    for newton_step in range(OUTER):
        tangent = jnp.tanh(state)
        diagonal = diagonal_of(tangent, faces, damping)
        resid = state - checkpoint + operate(state) + damp * tangent - forcing
        delta = -RELAXATION * resid / diagonal
        for inner_step in range(INNER - 1):
            image = delta + operate(delta) + damp * (1.0 - tangent * tangent) * delta
            delta = delta + RELAXATION * (-resid - image) / diagonal
        state = state + delta
    final = state - checkpoint + operate(state) + damp * jnp.tanh(state) - forcing

    tangent_n = jnp.tanh(trajectory)
    diagonal_n = diagonal_of(tangent_n, faces, damping)
    local_n = damp * (1.0 - tangent_n * tangent_n)
    multiplier = jnp.zeros_like(trajectory)
    for newton_step in range(OUTER):
        if newton_step == 0:
            resid = -adjoint_forcing
        else:
            resid = multiplier + operate_transposed(multiplier) + local_n * multiplier - adjoint_forcing
        delta = -RELAXATION * resid / diagonal_n
        for inner_step in range(INNER - 1):
            image = delta + operate_transposed(delta) + local_n * delta
            delta = delta + RELAXATION * (-resid - image) / diagonal_n
        multiplier = multiplier + delta
    adjoint_state = multiplier + observation_weight * (state - observations)
    return state, final, adjoint_state
```

```python
import functools
import math

import jax
import jax.numpy as jnp
from jax import lax
from jax.experimental import pallas as pl
from jax.experimental.pallas import tpu as pltpu
from jax.sharding import PartitionSpec as P

OUTER = 2
INNER = 4
DAY_STEPS = 96
RELAXATION = 0.7

FORWARD = 6
FIELDS = 8
CKPT, SOURCE, ED, EW, ND, NW, TRAJ, ADJF = range(FIELDS)

DEPTH = OUTER * INNER + 1
SLOT = DEPTH - 1
GROUP = 32
NINTH = (CKPT, ED, EW)

MESH = pl.DeviceIdType.MESH


def kernel(
    nx,
    ny,
    ckpt_h,
    traj_h,
    adjf_h,
    ed_h,
    nd_h,
    ew_h,
    nw_h,
    level_h,
    damp_h,
    source_h,
    obs_h,
    weight_h,
    step_h,
    state_out,
    resid_out,
    adj_out,
    raw,
    rawx,
    pack_e,
    pack_w,
    recv_e,
    recv_w,
    recvx_e,
    recvx_w,
    coef,
    cf,
    xm,
    x1x,
    x2,
    mu2,
    res,
    fw,
    fg,
    fd,
    fa,
    fb,
    aw,
    ag,
    ad,
    ad2,
    aa,
    ab,
    vert,
    obs_ref,
    weight_ref,
    level_ref,
    damp_ref,
    step_ref,
    load_sem,
    send_lat,
    got_lat,
    send_lon,
    got_lon,
    send_one,
    got_one,
    hello,
):
    levels, rows, lanes = state_out.shape
    wide = INNER
    ring = 2 * rows
    groups = lanes // GROUP
    per = levels // groups
    strips = levels + 2
    tiles = strips + 2 * per
    halo = DEPTH
    kept = GROUP - halo
    gx = lax.axis_index("gx")
    gy = lax.axis_index("gy")
    east = lax.rem(gx + 1, nx)
    west = lax.rem(gx + nx - 1, nx)
    has_n = gy < ny - 1
    has_s = gy > 0
    north = gy + 1
    south = gy - 1
    first_x = gx == 0
    last_x = gx == nx - 1

    inside = pl.ds(1, levels)
    outer = pl.ds(strips, 2 * per)
    main = pl.ds(0, rows)

    order = (ckpt_h, source_h, ed_h, ew_h, nd_h, nw_h, traj_h, adjf_h)
    loads = [
        pltpu.make_async_copy(h, raw.at[f, inside, main, :], load_sem.at[f])
        for f, h in enumerate(order)
    ]
    late_loads = [
        pltpu.make_async_copy(obs_h, obs_ref, load_sem.at[FIELDS]),
        pltpu.make_async_copy(weight_h, weight_ref, load_sem.at[FIELDS + 1]),
    ]
    scalar_loads = [
        pltpu.make_async_copy(level_h, level_ref, load_sem.at[FIELDS + 2]),
        pltpu.make_async_copy(damp_h, damp_ref, load_sem.at[FIELDS + 3]),
        pltpu.make_async_copy(step_h, step_ref, load_sem.at[FIELDS + 4]),
    ]

    barrier = pltpu.get_barrier_semaphore()
    neighbours = (
        (east, gy, True, last_x),
        (west, gy, True, jnp.logical_not(first_x)),
        (gx, north, has_n, False),
        (gx, south, has_s, True),
        (east, north, has_n, last_x),
        (west, north, has_n, jnp.logical_not(first_x)),
        (east, south, has_s, last_x),
        (west, south, has_s, jnp.logical_not(first_x)),
    )
    opposite = (1, 0, 3, 2, 7, 6, 5, 4)

    behind = 0
    for column, row, there, before in neighbours:
        behind = behind + jnp.logical_and(there, before).astype(jnp.int32)

        @pl.when(jnp.logical_and(there, jnp.logical_not(before)))
        def _():
            pl.semaphore_signal(
                barrier, inc=1, device_id={"gx": column, "gy": row}, device_id_type=MESH
            )

    for copy in loads + scalar_loads + late_loads:
        copy.start()

    @pl.when(behind > 0)
    def _():
        pl.semaphore_wait(barrier, behind)

    for k, (column, row, there, before) in enumerate(neighbours):

        @pl.when(jnp.logical_and(there, before))
        def _():
            pl.semaphore_signal(
                hello.at[opposite[k]], inc=1, device_id={"gx": column, "gy": row}, device_id_type=MESH
            )

    def known(*ks):
        for k in ks:
            _, _, there, before = neighbours[k]

            @pl.when(jnp.logical_and(there, jnp.logical_not(before)))
            def _():
                pl.semaphore_wait(hello.at[k], 1)

    def remote(src, dst, send, got, column, row):
        return pltpu.make_async_remote_copy(
            src_ref=src,
            dst_ref=dst,
            send_sem=send,
            recv_sem=got,
            device_id={"gx": column, "gy": row},
            device_id_type=MESH,
        )

    low = pl.ds(0, wide)
    high = pl.ds(rows - wide, wide)
    from_n = pl.ds(rows, wide)
    from_s = pl.ds(ring - wide, wide)
    next_low = pl.ds(wide, 1)
    next_high = pl.ds(rows - wide - 1, 1)
    extra_n = pl.ds(wide - 1, 1)
    extra_s = pl.ds(wide, 1)

    fwd = pl.ds(0, FORWARD)
    adj = pl.ds(FORWARD, FIELDS - FORWARD)
    faces = pl.ds(ND, 2)

    def lat(k, src, dst, column, row):
        return remote(src, dst, send_lat.at[k], got_lat.at[k], column, row)

    up0 = [
        lat(0, raw.at[fwd, inside, high, :], raw.at[fwd, inside, from_s, :], gx, north),
        lat(1, raw.at[faces, inside, next_high, :], rawx.at[:, inside, extra_s, :], gx, north),
        lat(2, raw.at[adj, inside, high, :], raw.at[adj, inside, from_s, :], gx, north),
    ]
    down0 = [
        lat(3, raw.at[fwd, inside, low, :], raw.at[fwd, inside, from_n, :], gx, south),
        lat(4, raw.at[adj, inside, low, :], raw.at[adj, inside, from_n, :], gx, south),
    ]

    def lon(k, src, dst, column, row):
        return remote(src, dst, send_lon.at[k], got_lon.at[k], column, row)

    def lon_copies(k, pack, recv, recvx, column):
        return (
            lon(k, pack, recv.at[:, main, :], column, gy),
            [
                lon(k + 1, pack.at[:, high, :], recv.at[:, from_s, :], column, north),
                lon(k + 2, pack.at[faces, next_high, :], recvx.at[:, extra_s, :], column, north),
            ],
            [lon(k + 3, pack.at[:, low, :], recv.at[:, from_n, :], column, south)],
        )

    lon_e = lon_copies(0, pack_e, recv_w, recvx_w, east)
    lon_w = lon_copies(4, pack_w, recv_e, recvx_e, west)

    def one(k, part):
        def copy(i, src, dst, row):
            return remote(src, dst, send_one.at[k + i], got_one.at[k + i], gx, row)

        return (
            [
                copy(0, xm.at[:, part, high, :], xm.at[:, part, from_s, :], north),
                copy(1, xm.at[0, part, next_high, :], x1x.at[part, extra_s, :], north),
            ],
            [
                copy(2, xm.at[:, part, low, :], xm.at[:, part, from_n, :], south),
                copy(3, xm.at[0, part, next_low, :], x1x.at[part, extra_n, :], south),
            ],
        )

    one_main = one(0, inside)
    one_strips = one(4, outer)

    def start_up(up):
        @pl.when(has_n)
        def _():
            for copy in up:
                copy.start()

    def start_down(down):
        @pl.when(has_s)
        def _():
            for copy in down:
                copy.start()

    def start_lon(copies):
        copies[0].start()
        start_up(copies[1])
        start_down(copies[2])

    def arrive(up, down):
        @pl.when(has_s)
        def _():
            for copy in up:
                copy.wait_recv()

        @pl.when(has_n)
        def _():
            for copy in down:
                copy.wait_recv()

    def flush(up, down):
        @pl.when(has_n)
        def _():
            for copy in up:
                copy.wait_send()

        @pl.when(has_s)
        def _():
            for copy in down:
                copy.wait_send()

    zero_ring = jnp.zeros((ring, lanes), jnp.float32)
    zero_tile = jnp.zeros((rows, lanes), jnp.float32)
    for t in (0, levels + 1):
        raw[CKPT, t] = zero_ring
        for ref in (fa, fb, aa, ab, x2):
            ref[t] = zero_ring
        for k in range(2):
            xm[k, t] = zero_ring

    def clear(part):
        zero = jnp.zeros((wide, lanes), jnp.float32)

        def body(l, carry):
            for f in range(FIELDS):
                raw[f, l + 1, part, :] = zero
            for k in range(2):
                xm[k, l + 1, part, :] = zero
            return carry

        lax.fori_loop(0, levels, body, 0)
        for t in range(strips, tiles):
            for k in range(2):
                xm[k, t, part, :] = zero
        for f in range(FIELDS + 1):
            recv_e[f, part, :] = zero
            recv_w[f, part, :] = zero

    def clear_extra(part):
        zero = jnp.zeros((1, lanes), jnp.float32)
        for t in [*range(1, levels + 1), *range(strips, tiles)]:
            x1x[t, part, :] = zero

    @pl.when(jnp.logical_not(has_n))
    def _():
        clear(from_n)
        clear_extra(extra_n)

    @pl.when(jnp.logical_not(has_s))
    def _():
        clear(from_s)
        clear_extra(extra_s)
        zero = jnp.zeros((1, lanes), jnp.float32)
        for k in range(2):
            for t in range(1, levels + 1):
                rawx[k, t, extra_s, :] = zero
            recvx_e[k, extra_s, :] = zero
            recvx_w[k, extra_s, :] = zero

    for copy in loads:
        copy.wait()
    start_down(down0)

    lane_row = lax.broadcasted_iota(jnp.int32, (rows, lanes), 1)
    lane_ring = lax.broadcasted_iota(jnp.int32, (ring, lanes), 1)
    row_ring = lax.broadcasted_iota(jnp.int32, (ring, lanes), 0)

    def turn(v, shift, axis=1):
        shift = shift % v.shape[axis]
        return pltpu.roll(v, shift, axis) if shift else v

    def choose(place, values):
        out = values[-1]
        for k in range(len(values) - 2, -1, -1):
            out = jnp.where(place == k, values[k], out)
        return out

    def gather(read, place, side, j):
        start = halo if side == 0 else kept
        return choose(place, [turn(read(j + per * g), GROUP * g + start) for g in range(groups)])

    group_row = lane_row // GROUP
    slot_row = (lane_row % GROUP) // SLOT
    nine_row = lane_row % SLOT

    for f in range(FIELDS):
        edge = []
        for side in range(2):
            for j in range(per):
                tile = gather(lambda l: raw[f, l + 1, :rows, :], group_row, side, j)
                raw[f, strips + per * side + j, :rows, :] = tile
                edge.append(tile)
        pack_w[f] = choose(slot_row, [turn(edge[j], SLOT * j - halo) for j in range(per)])
        pack_e[f] = choose(
            slot_row, [turn(edge[per + j], SLOT * j - (kept - SLOT)) for j in range(per)]
        )
    nine_e = [
        choose(
            slot_row,
            [turn(raw[f, strips + per + j, :rows, :], SLOT * j + i - (kept - DEPTH)) for j in range(per)],
        )
        for i, f in enumerate(NINTH)
    ]
    pack_e[FIELDS] = choose(nine_row, nine_e)
    pack_w[FIELDS] = choose(
        slot_row, [turn(raw[CKPT, strips + j, :rows, :], SLOT * j - (halo + SLOT)) for j in range(per)]
    )

    @pl.when(last_x)
    def _():
        start_lon(lon_e)

    @pl.when(jnp.logical_not(first_x))
    def _():
        start_lon(lon_w)

    known(2)
    start_up(up0)

    @pl.when(jnp.logical_not(last_x))
    def _():
        known(0, 4, 6)
        start_lon(lon_e)

    for copy in scalar_loads:
        copy.wait()

    total_lanes = lanes * nx

    def heat_of(column):
        column = gx * lanes + column
        column = jnp.where(column < 0, column + total_lanes, column)
        column = jnp.where(column >= total_lanes, column - total_lanes, column)
        phase = (
            2.0 * math.pi * column.astype(jnp.float32) / total_lanes
            - 2.0 * math.pi * step_ref[0].astype(jnp.float32) / DAY_STEPS
        )
        return jnp.cos(phase)

    lane_one = lax.broadcasted_iota(jnp.int32, (1, lanes), 1)
    heat_main = heat_of(lane_one)
    heat_side = (
        heat_of(lane_one % GROUP - halo),
        heat_of(lane_one % GROUP + (lanes - kept)),
    )
    row_global = gy * rows + jnp.where(row_ring < rows + wide, row_ring, row_ring - ring)
    open_face = (row_global >= 0) & (row_global < rows * ny - 1)

    def level_terms(l):
        up = jnp.where(l < levels - 1, level_ref[l], 0.0)
        down = jnp.where(l > 0, level_ref[jnp.maximum(l - 1, 0)], 0.0)
        return up, down, damp_ref[l]

    group_one = lane_ring // GROUP
    for j in range(per):
        terms = [level_terms(j + per * g) for g in range(groups)]
        for k in range(3):
            vert[k, j] = choose(group_one, [jnp.full((ring, lanes), term[k]) for term in terms])

    class Main:
        def __init__(self, l):
            self.t = l + 1
            self.l = l
            self.heat = heat_main

        def terms(self):
            return level_terms(self.l)

        def above(self, ref):
            return ref[self.t + 1]

        def below(self, ref):
            return ref[self.t - 1]

    class Strip:
        def __init__(self, k):
            self.t = strips + k
            self.j = k % per
            self.base = strips + k - self.j
            self.heat = heat_side[k // per]

        def terms(self):
            return vert[0, self.j], vert[1, self.j], vert[2, self.j]

        def above(self, ref):
            if self.j < per - 1:
                return ref[self.t + 1]
            return turn(ref[self.base], -GROUP)

        def below(self, ref):
            if self.j > 0:
                return ref[self.t - 1]
            return turn(ref[self.base + per - 1], GROUP)

    def each_main(body):
        def step(l, carry):
            body(Main(l))
            return carry

        lax.fori_loop(0, levels, step, 0, unroll=True)

    def each_strip(body):
        for k in range(2 * per):
            body(Strip(k))

    def off_forward(c, ref, extra=None):
        up, down, _ = c.terms()
        v = ref[c.t]
        above = turn(v, -1, 0)
        below = turn(v, 1, 0)
        if extra is not None:
            more = jnp.concatenate([extra[c.t], extra[c.t]], axis=0)
            above = jnp.where(row_ring == rows + wide - 1, more, above)
            below = jnp.where(row_ring == rows + wide, more, below)
        off = (
            turn(v, -1) * coef[1, c.t]
            - turn(v, 1) * coef[2, c.t]
            + above * coef[5, c.t]
            - below * coef[6, c.t]
            - up * c.above(ref)
            - down * c.below(ref)
        )
        return v, off

    def off_adjoint(c, ref):
        up, down, _ = c.terms()
        v = ref[c.t]
        off = (
            turn(v, 1) * coef[3, c.t]
            - turn(v, -1) * coef[0, c.t]
            + turn(v, 1, 0) * coef[7, c.t]
            - turn(v, -1, 0) * coef[4, c.t]
            - up * c.above(ref)
            - down * c.below(ref)
        )
        return v, off

    def resid_forward(c, ref, extra=None):
        _, _, damp = c.terms()
        x, off = off_forward(c, ref, extra)
        t = jnp.tanh(x)
        local = damp * (1.0 - t * t)
        diag = coef[8, c.t]
        r = x * diag + off + damp * t - cf[c.t]
        w = RELAXATION / (coef[9, c.t] + local)
        d = -w * r
        fw[c.t] = w
        fg[c.t] = 1.0 - w * (diag + local)
        fd[c.t] = d
        fa[c.t] = d

    def resid_adjoint(c, ref):
        m, off = off_adjoint(c, ref)
        d = ad[c.t] - (1.0 - ag[c.t]) * m - aw[c.t] * off
        ad2[c.t] = d
        aa[c.t] = d

    def lin_forward(c, src):
        v, off = off_forward(c, src)
        return fg[c.t] * v + fd[c.t] - fw[c.t] * off

    def lin_adjoint(c, src, base):
        v, off = off_adjoint(c, src)
        return ag[c.t] * v + base[c.t] - aw[c.t] * off

    def prepare(c):
        up, down, damp = c.terms()
        de = raw[ED, c.t]
        fe = 0.5 * raw[EW, c.t]
        dn = jnp.where(open_face, raw[ND, c.t], 0.0)
        fn = jnp.where(open_face, 0.5 * raw[NW, c.t], 0.0)
        dnx = rawx[0, c.t]
        fnx = 0.5 * rawx[1, c.t]
        anx, bnx = fnx + dnx, fnx - dnx
        a, b = fe + de, fe - de
        an, bn = fn + dn, fn - dn
        a_w = turn(a, 1)
        b_w = turn(b, 1)
        last = row_ring == rows + wide
        an_s = jnp.where(last, jnp.concatenate([anx, anx], axis=0), turn(an, 1, 0))
        bn_s = jnp.where(last, jnp.concatenate([bnx, bnx], axis=0), turn(bn, 1, 0))
        diag = 1.0 + (a - b_w) + (an - bn_s) + (up + down)
        total = 1.0 + de + 0.5 * (a_w - b_w) + dn + 0.5 * (an_s - bn_s) + (up + down)
        for k, value in enumerate((a, b, a_w, b_w, an, bn, an_s, bn_s, diag, total)):
            coef[k, c.t] = value
        cf[c.t] = raw[CKPT, c.t] + raw[SOURCE, c.t] * c.heat
        t = jnp.tanh(raw[TRAJ, c.t])
        local = damp * (1.0 - t * t)
        w = RELAXATION / (total + local)
        start_delta = w * raw[ADJF, c.t]
        aw[c.t] = w
        ag[c.t] = 1.0 - w * (diag + local)
        ad[c.t] = start_delta
        aa[c.t] = start_delta
        resid_forward(c, raw.at[CKPT])

    pairs = ((fa, fb, aa, ab), (fb, fa, ab, aa))
    last = pairs[(INNER - 2) % 2]

    def sweeps(each, base):
        for k in range(INNER - 2):
            f_src, f_dst, a_src, a_dst = pairs[k % 2]

            def body(c):
                f_dst[c.t] = lin_forward(c, f_src)
                a_dst[c.t] = lin_adjoint(c, a_src, base)

            each(body)

    def close1(c):
        xm[0, c.t, :rows, :] = raw[CKPT, c.t, :rows, :] + lin_forward(c, last[0])[:rows]
        xm[1, c.t, :rows, :] = lin_adjoint(c, last[2], ad)[:rows]

    def second(c):
        resid_forward(c, xm.at[0], x1x)
        resid_adjoint(c, xm.at[1])

    def close2(c):
        x2[c.t] = xm[0, c.t] + lin_forward(c, last[0])
        mu2[c.t] = xm[1, c.t, :rows, :] + lin_adjoint(c, last[2], ad2)[:rows]

    def finish(c):
        _, _, damp = c.terms()
        x, off = off_forward(c, x2)
        r = x * coef[8, c.t] + off + damp * jnp.tanh(x) - cf[c.t]
        res[c.t] = r[:rows]

    @pl.when(first_x)
    def _():
        known(1, 5, 7)
        start_lon(lon_w)

    arrive(up0, down0)
    each_main(prepare)
    sweeps(each_main, ad)
    each_main(close1)
    start_up(one_main[0])
    start_down(one_main[1])

    spot = lane_ring % GROUP
    from_w = (spot > 0) & (spot < halo)
    from_e = (spot >= kept) & (spot < GROUP - 1)
    spot_row = spot[:rows]
    for f in range(FIELDS):
        for side in range(2):
            for j in range(per):
                raw[f, strips + per * side + j, rows:, :] = gather(
                    lambda l: raw[f, l + 1, rows:, :], group_row, side, j
                )
    for copies in (lon_e, lon_w):
        copies[0].wait_recv()
        arrive(copies[1], copies[2])

    for f in range(FIELDS):
        for j in range(per):
            t = strips + j
            tile = jnp.where(from_w, turn(recv_w[f], 1 - SLOT * j), raw[f, t])
            if f in NINTH:
                nine = turn(recv_w[FIELDS], -(SLOT * j + NINTH.index(f)))
                tile = jnp.where(spot == 0, nine, tile)
            raw[f, t] = tile
            t = strips + per + j
            tile = jnp.where(from_e, turn(recv_e[f], kept - SLOT * j), raw[f, t])
            if f == CKPT:
                nine = turn(recv_e[FIELDS], GROUP - 1 - SLOT * j)
                tile = jnp.where(spot == GROUP - 1, nine, tile)
            raw[f, t] = tile
    for k in range(2):
        for j in range(per):
            for side, (recvx, shift, where) in enumerate(
                ((recvx_w, 1 - SLOT * j, from_w), (recvx_e, kept - SLOT * j, from_e))
            ):
                t = strips + per * side + j
                tile = gather(lambda l: rawx[k, l + 1], group_row, side, j)
                rawx[k, t] = jnp.where(where[:rows], turn(recvx[k], shift), tile)

    each_strip(prepare)
    sweeps(each_strip, ad)
    each_strip(close1)
    start_up(one_strips[0])
    start_down(one_strips[1])

    arrive(*one_main)
    each_main(second)
    sweeps(each_main, ad2)
    each_main(close2)
    each_main(finish)

    arrive(*one_strips)
    each_strip(second)
    sweeps(each_strip, ad2)
    each_strip(close2)
    each_strip(finish)

    for copy in late_loads:
        copy.wait()

    west_edge = lane_row < DEPTH
    east_edge = lane_row >= lanes - DEPTH

    def merged(ref, l):
        j, g = l % per, l // per
        w = turn(ref[strips + j][:rows], -(GROUP * g + halo))
        e = turn(ref[strips + per + j][:rows], lanes - kept - GROUP * g)
        return jnp.where(west_edge, w, jnp.where(east_edge, e, ref[l + 1][:rows]))

    for l in range(levels):
        x = merged(x2, l)
        state_out[l] = x
        adj_out[l] = merged(mu2, l) + weight_ref[l] * (x - obs_ref[l])
        resid_out[l] = merged(res, l)

    flush(up0, down0)
    flush(*one_main)
    flush(*one_strips)
    for copies in (lon_e, lon_w):
        copies[0].wait_send()
        flush(copies[1], copies[2])


def hand_over(a, b, c, x, y, z, sem):
    gives = [
        pltpu.make_async_copy(held, ref, sem.at[k])
        for k, (held, ref) in enumerate(((a, x), (b, y), (c, z)))
    ]
    for copy in gives:
        copy.start()
    for copy in gives:
        copy.wait()


def solution(mesh):
    nx, ny = mesh.shape["gx"], mesh.shape["gy"]

    def per_device(*arrays):
        levels, rows, lanes = arrays[0].shape
        groups = lanes // GROUP
        assert rows >= 2 * INNER and rows >= INNER + 1 and levels % groups == 0 and nx > 2
        per = levels // groups
        assert per * SLOT <= GROUP and GROUP >= 3 * DEPTH and len(NINTH) <= SLOT
        ring = 2 * rows
        tiles = levels + 2 + 2 * per
        f32 = jnp.float32
        out = jax.ShapeDtypeStruct((levels, rows, lanes), f32)
        hbm = pl.BlockSpec(memory_space=pltpu.HBM)
        vmem = pl.BlockSpec(memory_space=pltpu.VMEM)

        def buf(*shape):
            return pltpu.VMEM(shape, f32)

        def full():
            return buf(tiles, ring, lanes)

        def dma(n):
            return pltpu.SemaphoreType.DMA((n,))

        results = pl.pallas_call(
            functools.partial(kernel, nx, ny),
            name="step_pair",
            out_shape=(pltpu.VMEM(out.shape, f32),) * 3,
            in_specs=[hbm] * 13,
            out_specs=(vmem,) * 3,
            scratch_shapes=[
                buf(FIELDS, tiles, ring, lanes),
                buf(2, tiles, rows, lanes),
                buf(FIELDS + 1, rows, lanes),
                buf(FIELDS + 1, rows, lanes),
                buf(FIELDS + 1, ring, lanes),
                buf(FIELDS + 1, ring, lanes),
                buf(2, rows, lanes),
                buf(2, rows, lanes),
                buf(10, tiles, ring, lanes),
                full(),
                buf(2, tiles, ring, lanes),
                buf(tiles, rows, lanes),
                full(),
                buf(tiles, rows, lanes),
                buf(tiles, rows, lanes),
            ]
            + [full() for _ in range(11)]
            + [
                buf(3, per, ring, lanes),
                buf(levels, rows, lanes),
                buf(levels, rows, lanes),
                pltpu.SMEM((levels,), f32),
                pltpu.SMEM((levels,), f32),
                pltpu.SMEM((1,), jnp.int32),
                dma(FIELDS + 5),
                dma(5),
                dma(5),
                dma(8),
                dma(8),
                dma(8),
                dma(8),
                pltpu.SemaphoreType.REGULAR((8,)),
            ],
            compiler_params=pltpu.CompilerParams(
                collective_id=0, has_side_effects=True, vmem_limit_bytes=67043328 - 3 * 4 * math.prod(out.shape)
            ),
        )(*arrays)
        return pl.pallas_call(
            hand_over,
            name="hand_over",
            out_shape=(out, out, out),
            in_specs=[vmem] * 3,
            out_specs=(hbm, hbm, hbm),
            scratch_shapes=[dma(3)],
            compiler_params=pltpu.CompilerParams(vmem_limit_bytes=4 * 2**20),
        )(*results)

    block = P(None, "gy", "gx")
    return jax.shard_map(
        per_device,
        mesh=mesh,
        in_specs=(block,) * 7 + (P(), P(), block, block, block, P()),
        out_specs=(block,) * 3,
        check_vma=False,
    )
```

```python
import functools
import math

import jax
import jax.numpy as jnp
from jax import lax
from jax.experimental import pallas as pl
from jax.experimental.pallas import tpu as pltpu
from jax.sharding import PartitionSpec as P

OUTER = 2
INNER = 4
DAY_STEPS = 96
RELAXATION = 0.7

FORWARD = 6
FIELDS = 8
CKPT, SOURCE, ED, EW, ND, NW, TRAJ, ADJF = range(FIELDS)

DEPTH = OUTER * INNER + 1
SLOT = DEPTH - 1
GROUP = 32
NINTH = (CKPT, ED, EW)

MESH = pl.DeviceIdType.MESH


def kernel(
    nx,
    ny,
    ckpt_h,
    traj_h,
    adjf_h,
    ed_h,
    nd_h,
    ew_h,
    nw_h,
    level_h,
    damp_h,
    source_h,
    obs_h,
    weight_h,
    step_h,
    state_out,
    resid_out,
    adj_out,
    raw,
    rawx,
    pack_e,
    pack_w,
    recv_e,
    recv_w,
    recvx_e,
    recvx_w,
    coef,
    cf,
    xm,
    x1x,
    x2,
    mu2,
    res,
    fw,
    fg,
    fd,
    fa,
    fb,
    aw,
    ag,
    ad,
    ad2,
    aa,
    ab,
    vert,
    obs_ref,
    weight_ref,
    level_ref,
    damp_ref,
    step_ref,
    load_sem,
    send_lat,
    got_lat,
    send_lon,
    got_lon,
    send_one,
    got_one,
    hello,
):
    levels, rows, lanes = state_out.shape
    wide = INNER
    ring = 2 * rows
    groups = lanes // GROUP
    per = levels // groups
    strips = levels + 2
    tiles = strips + 2 * per
    halo = DEPTH
    kept = GROUP - halo
    gx = lax.axis_index("gx")
    gy = lax.axis_index("gy")
    east = lax.rem(gx + 1, nx)
    west = lax.rem(gx + nx - 1, nx)
    has_n = gy < ny - 1
    has_s = gy > 0
    north = gy + 1
    south = gy - 1
    first_x = gx == 0
    last_x = gx == nx - 1

    inside = pl.ds(1, levels)
    main = pl.ds(0, rows)

    order = (ckpt_h, source_h, ed_h, ew_h, nd_h, nw_h, traj_h, adjf_h)
    loads = [
        pltpu.make_async_copy(h, raw.at[f, inside, main, :], load_sem.at[f])
        for f, h in enumerate(order)
    ]
    late_loads = [
        pltpu.make_async_copy(obs_h, obs_ref, load_sem.at[FIELDS]),
        pltpu.make_async_copy(weight_h, weight_ref, load_sem.at[FIELDS + 1]),
    ]
    scalar_loads = [
        pltpu.make_async_copy(level_h, level_ref, load_sem.at[FIELDS + 2]),
        pltpu.make_async_copy(damp_h, damp_ref, load_sem.at[FIELDS + 3]),
        pltpu.make_async_copy(step_h, step_ref, load_sem.at[FIELDS + 4]),
    ]

    barrier = pltpu.get_barrier_semaphore()
    odd_x = lax.rem(gx, 2) == 1
    odd_y = lax.rem(gy, 2) == 1
    even_y = jnp.logical_not(odd_y)
    inner_x = jnp.logical_not(first_x)
    before_e = jnp.logical_or(last_x, odd_x)
    before_w = jnp.logical_and(inner_x, odd_x)
    before_de = jnp.logical_or(last_x, even_y)
    before_dw = jnp.logical_and(inner_x, even_y)
    neighbours = (
        (east, gy, True, before_e),
        (west, gy, True, before_w),
        (gx, north, has_n, odd_y),
        (gx, south, has_s, odd_y),
        (east, north, has_n, before_de),
        (west, north, has_n, before_dw),
        (east, south, has_s, before_de),
        (west, south, has_s, before_dw),
    )
    opposite = (1, 0, 3, 2, 7, 6, 5, 4)

    behind = 0
    for column, row, there, before in neighbours:
        behind = behind + jnp.logical_and(there, before).astype(jnp.int32)

        @pl.when(jnp.logical_and(there, jnp.logical_not(before)))
        def _():
            pl.semaphore_signal(
                barrier, inc=1, device_id={"gx": column, "gy": row}, device_id_type=MESH
            )

    for copy in loads + scalar_loads + late_loads:
        copy.start()

    @pl.when(behind > 0)
    def _():
        pl.semaphore_wait(barrier, behind)

    for k, (column, row, there, before) in enumerate(neighbours):

        @pl.when(jnp.logical_and(there, before))
        def _():
            pl.semaphore_signal(
                hello.at[opposite[k]], inc=1, device_id={"gx": column, "gy": row}, device_id_type=MESH
            )

    def known(*ks):
        for k in ks:
            _, _, there, before = neighbours[k]

            @pl.when(jnp.logical_and(there, jnp.logical_not(before)))
            def _():
                pl.semaphore_wait(hello.at[k], 1)

    def remote(src, dst, send, got, column, row):
        return pltpu.make_async_remote_copy(
            src_ref=src,
            dst_ref=dst,
            send_sem=send,
            recv_sem=got,
            device_id={"gx": column, "gy": row},
            device_id_type=MESH,
        )

    low = pl.ds(0, wide)
    high = pl.ds(rows - wide, wide)
    from_n = pl.ds(rows, wide)
    from_s = pl.ds(ring - wide, wide)
    next_low = pl.ds(wide, 1)
    next_high = pl.ds(rows - wide - 1, 1)
    extra_n = pl.ds(wide - 1, 1)
    extra_s = pl.ds(wide, 1)

    fwd = pl.ds(0, FORWARD)
    adj = pl.ds(FORWARD, FIELDS - FORWARD)
    faces = pl.ds(ND, 2)

    def lat(k, src, dst, column, row):
        return remote(src, dst, send_lat.at[k], got_lat.at[k], column, row)

    up0 = [
        lat(0, raw.at[fwd, inside, high, :], raw.at[fwd, inside, from_s, :], gx, north),
        lat(1, raw.at[faces, inside, next_high, :], rawx.at[:, inside, extra_s, :], gx, north),
        lat(2, raw.at[adj, inside, high, :], raw.at[adj, inside, from_s, :], gx, north),
    ]
    down0 = [
        lat(3, raw.at[fwd, inside, low, :], raw.at[fwd, inside, from_n, :], gx, south),
        lat(4, raw.at[adj, inside, low, :], raw.at[adj, inside, from_n, :], gx, south),
    ]

    def lon(k, src, dst, column, row):
        return remote(src, dst, send_lon.at[k], got_lon.at[k], column, row)

    def lon_copies(k, pack, recv, recvx, column):
        return (
            lon(k, pack, recv.at[:, main, :], column, gy),
            [
                lon(k + 1, pack.at[:, high, :], recv.at[:, from_s, :], column, north),
                lon(k + 2, pack.at[faces, next_high, :], recvx.at[:, extra_s, :], column, north),
            ],
            [lon(k + 3, pack.at[:, low, :], recv.at[:, from_n, :], column, south)],
        )

    lon_e = lon_copies(0, pack_e, recv_w, recvx_w, east)
    lon_w = lon_copies(4, pack_w, recv_e, recvx_e, west)

    def one(k, part):
        def copy(i, src, dst, row):
            return remote(src, dst, send_one.at[k + i], got_one.at[k + i], gx, row)

        return (
            [
                copy(0, xm.at[:, part, high, :], xm.at[:, part, from_s, :], north),
                copy(1, xm.at[0, part, next_high, :], x1x.at[part, extra_s, :], north),
            ],
            [
                copy(2, xm.at[:, part, low, :], xm.at[:, part, from_n, :], south),
                copy(3, xm.at[0, part, next_low, :], x1x.at[part, extra_n, :], south),
            ],
        )

    one_main = one(0, inside)

    def start_up(up):
        @pl.when(has_n)
        def _():
            for copy in up:
                copy.start()

    def start_down(down):
        @pl.when(has_s)
        def _():
            for copy in down:
                copy.start()

    def start_lon(copies):
        copies[0].start()
        start_up(copies[1])
        start_down(copies[2])

    def arrive(up, down):
        @pl.when(has_s)
        def _():
            for copy in up:
                copy.wait_recv()

        @pl.when(has_n)
        def _():
            for copy in down:
                copy.wait_recv()

    def flush(up, down):
        @pl.when(has_n)
        def _():
            for copy in up:
                copy.wait_send()

        @pl.when(has_s)
        def _():
            for copy in down:
                copy.wait_send()

    zero_ring = jnp.zeros((ring, lanes), jnp.float32)
    zero_tile = jnp.zeros((rows, lanes), jnp.float32)
    for t in (0, levels + 1):
        raw[CKPT, t] = zero_ring
        for ref in (fa, fb, aa, ab, x2):
            ref[t] = zero_ring
        for k in range(2):
            xm[k, t] = zero_ring

    def clear(part):
        zero = jnp.zeros((wide, lanes), jnp.float32)

        def body(l, carry):
            for f in range(FIELDS):
                raw[f, l + 1, part, :] = zero
            for k in range(2):
                xm[k, l + 1, part, :] = zero
            return carry

        lax.fori_loop(0, levels, body, 0)
        for t in range(strips, tiles):
            for k in range(2):
                xm[k, t, part, :] = zero
        for f in range(FIELDS + 1):
            recv_e[f, part, :] = zero
            recv_w[f, part, :] = zero

    def clear_extra(part):
        zero = jnp.zeros((1, lanes), jnp.float32)
        for t in [*range(1, levels + 1), *range(strips, tiles)]:
            x1x[t, part, :] = zero

    @pl.when(jnp.logical_not(has_n))
    def _():
        clear(from_n)
        clear_extra(extra_n)

    @pl.when(jnp.logical_not(has_s))
    def _():
        clear(from_s)
        clear_extra(extra_s)
        zero = jnp.zeros((1, lanes), jnp.float32)
        for k in range(2):
            for t in range(1, levels + 1):
                rawx[k, t, extra_s, :] = zero
            recvx_e[k, extra_s, :] = zero
            recvx_w[k, extra_s, :] = zero

    for copy in loads:
        copy.wait()

    def send_lat():
        known(2)
        start_up(up0)
        known(3)
        start_down(down0)

    @pl.when(jnp.logical_not(last_x))
    def _():
        send_lat()


    lane_row = lax.broadcasted_iota(jnp.int32, (rows, lanes), 1)
    lane_ring = lax.broadcasted_iota(jnp.int32, (ring, lanes), 1)
    row_ring = lax.broadcasted_iota(jnp.int32, (ring, lanes), 0)

    def turn(v, shift, axis=1):
        shift = shift % v.shape[axis]
        return pltpu.roll(v, shift, axis) if shift else v

    def choose(place, values):
        out = values[-1]
        for k in range(len(values) - 2, -1, -1):
            out = jnp.where(place == k, values[k], out)
        return out

    def gather(read, place, side, j):
        start = halo if side == 0 else kept
        return choose(place, [turn(read(j + per * g), GROUP * g + start) for g in range(groups)])

    group_row = lane_row // GROUP
    nine_row = lane_row % SLOT

    def slots(f, shift, turns=(0,)):
        rolled = [turn(raw[f, level_of(k) + 1, :rows, :], SLOT * k + shift) for k in range(levels)]
        return [choose((lane_row // SLOT + move) % levels, rolled) for move in turns]

    def level_of(k):
        return k % per + per * (k // per)

    nine = None
    for f in range(FIELDS):
        if f in NINTH:
            pack_e[f], beside = slots(f, SLOT, (0, 1))
            i = NINTH.index(f)
            beside = turn(beside, -i)
            nine = beside if nine is None else jnp.where(nine_row == SLOT - 1 - i, beside, nine)
        else:
            (pack_e[f],) = slots(f, SLOT)
    pack_e[FIELDS] = nine

    @pl.when(last_x)
    def _():
        start_lon(lon_e)
        send_lat()

    for f in range(FIELDS):
        if f == CKPT:
            pack_w[f], pack_w[FIELDS] = slots(f, 0, (0, -1))
        else:
            (pack_w[f],) = slots(f, 0)

    @pl.when(inner_x)
    def _():
        known(1, 5, 7)
        start_lon(lon_w)

    @pl.when(jnp.logical_not(last_x))
    def _():
        known(0, 4, 6)
        start_lon(lon_e)

    for f in range(FIELDS):
        for side in range(2):
            for j in range(per):
                raw[f, strips + per * side + j, :rows, :] = gather(
                    lambda l: raw[f, l + 1, :rows, :], group_row, side, j
                )

    for copy in scalar_loads:
        copy.wait()

    total_lanes = lanes * nx

    def heat_of(column):
        column = gx * lanes + column
        column = jnp.where(column < 0, column + total_lanes, column)
        column = jnp.where(column >= total_lanes, column - total_lanes, column)
        phase = (
            2.0 * math.pi * column.astype(jnp.float32) / total_lanes
            - 2.0 * math.pi * step_ref[0].astype(jnp.float32) / DAY_STEPS
        )
        return jnp.cos(phase)

    lane_one = lax.broadcasted_iota(jnp.int32, (1, lanes), 1)
    heat_main = heat_of(lane_one)
    heat_side = (
        heat_of(lane_one % GROUP - halo),
        heat_of(lane_one % GROUP + (lanes - kept)),
    )
    row_global = gy * rows + jnp.where(row_ring < rows + wide, row_ring, row_ring - ring)
    open_face = (row_global >= 0) & (row_global < rows * ny - 1)

    def level_terms(l):
        up = jnp.where(l < levels - 1, level_ref[l], 0.0)
        down = jnp.where(l > 0, level_ref[jnp.maximum(l - 1, 0)], 0.0)
        return up, down, damp_ref[l]

    group_one = lane_ring // GROUP
    for j in range(per):
        terms = [level_terms(j + per * g) for g in range(groups)]
        for k in range(3):
            vert[k, j] = choose(group_one, [jnp.full((ring, lanes), term[k]) for term in terms])

    class Main:
        def __init__(self, l):
            self.t = l + 1
            self.l = l
            self.heat = heat_main

        def terms(self):
            return level_terms(self.l)

        def above(self, ref):
            return ref[self.t + 1]

        def below(self, ref):
            return ref[self.t - 1]

    class Strip:
        def __init__(self, k):
            self.t = strips + k
            self.j = k % per
            self.base = strips + k - self.j
            self.heat = heat_side[k // per]

        def terms(self):
            return vert[0, self.j], vert[1, self.j], vert[2, self.j]

        def above(self, ref):
            if self.j < per - 1:
                return ref[self.t + 1]
            return turn(ref[self.base], -GROUP)

        def below(self, ref):
            if self.j > 0:
                return ref[self.t - 1]
            return turn(ref[self.base + per - 1], GROUP)

    def each_main(body):
        def step(l, carry):
            body(Main(l))
            return carry

        lax.fori_loop(0, levels, step, 0, unroll=True)

    def each_strip(side, body):
        for j in range(per):
            body(Strip(per * side + j))

    def off_forward(c, ref, extra=None):
        up, down, _ = c.terms()
        v = ref[c.t]
        above = turn(v, -1, 0)
        below = turn(v, 1, 0)
        if extra is not None:
            more = jnp.concatenate([extra[c.t], extra[c.t]], axis=0)
            above = jnp.where(row_ring == rows + wide - 1, more, above)
            below = jnp.where(row_ring == rows + wide, more, below)
        off = (
            turn(v, -1) * coef[1, c.t]
            - turn(v, 1) * coef[2, c.t]
            + above * coef[5, c.t]
            - below * coef[6, c.t]
            - up * c.above(ref)
            - down * c.below(ref)
        )
        return v, off

    def off_adjoint(c, ref):
        up, down, _ = c.terms()
        v = ref[c.t]
        off = (
            turn(v, 1) * coef[3, c.t]
            - turn(v, -1) * coef[0, c.t]
            + turn(v, 1, 0) * coef[7, c.t]
            - turn(v, -1, 0) * coef[4, c.t]
            - up * c.above(ref)
            - down * c.below(ref)
        )
        return v, off

    def resid_forward(c, ref, extra=None):
        _, _, damp = c.terms()
        x, off = off_forward(c, ref, extra)
        t = jnp.tanh(x)
        local = damp * (1.0 - t * t)
        diag = coef[8, c.t]
        r = x * diag + off + damp * t - cf[c.t]
        w = RELAXATION / (coef[9, c.t] + local)
        d = -w * r
        fw[c.t] = w
        fg[c.t] = 1.0 - w * (diag + local)
        fd[c.t] = d
        fa[c.t] = d

    def resid_adjoint(c, ref):
        m, off = off_adjoint(c, ref)
        d = ad[c.t] - (1.0 - ag[c.t]) * m - aw[c.t] * off
        ad2[c.t] = d
        aa[c.t] = d

    def lin_forward(c, src):
        v, off = off_forward(c, src)
        return fg[c.t] * v + fd[c.t] - fw[c.t] * off

    def lin_adjoint(c, src, base):
        v, off = off_adjoint(c, src)
        return ag[c.t] * v + base[c.t] - aw[c.t] * off

    def prepare(c):
        up, down, damp = c.terms()
        de = raw[ED, c.t]
        fe = 0.5 * raw[EW, c.t]
        dn = jnp.where(open_face, raw[ND, c.t], 0.0)
        fn = jnp.where(open_face, 0.5 * raw[NW, c.t], 0.0)
        dnx = rawx[0, c.t]
        fnx = 0.5 * rawx[1, c.t]
        anx, bnx = fnx + dnx, fnx - dnx
        a, b = fe + de, fe - de
        an, bn = fn + dn, fn - dn
        a_w = turn(a, 1)
        b_w = turn(b, 1)
        last = row_ring == rows + wide
        an_s = jnp.where(last, jnp.concatenate([anx, anx], axis=0), turn(an, 1, 0))
        bn_s = jnp.where(last, jnp.concatenate([bnx, bnx], axis=0), turn(bn, 1, 0))
        diag = 1.0 + (a - b_w) + (an - bn_s) + (up + down)
        total = 1.0 + de + 0.5 * (a_w - b_w) + dn + 0.5 * (an_s - bn_s) + (up + down)
        for k, value in enumerate((a, b, a_w, b_w, an, bn, an_s, bn_s, diag, total)):
            coef[k, c.t] = value
        cf[c.t] = raw[CKPT, c.t] + raw[SOURCE, c.t] * c.heat
        t = jnp.tanh(raw[TRAJ, c.t])
        local = damp * (1.0 - t * t)
        w = RELAXATION / (total + local)
        start_delta = w * raw[ADJF, c.t]
        aw[c.t] = w
        ag[c.t] = 1.0 - w * (diag + local)
        ad[c.t] = start_delta
        aa[c.t] = start_delta
        resid_forward(c, raw.at[CKPT])

    pairs = ((fa, fb, aa, ab), (fb, fa, ab, aa))
    last = pairs[(INNER - 2) % 2]

    def sweeps(each, base):
        for k in range(INNER - 2):
            f_src, f_dst, a_src, a_dst = pairs[k % 2]

            def body(c):
                f_dst[c.t] = lin_forward(c, f_src)
                a_dst[c.t] = lin_adjoint(c, a_src, base)

            each(body)

    def close1(c):
        xm[0, c.t, :rows, :] = raw[CKPT, c.t, :rows, :] + lin_forward(c, last[0])[:rows]
        xm[1, c.t, :rows, :] = lin_adjoint(c, last[2], ad)[:rows]

    def second(c):
        resid_forward(c, xm.at[0], x1x)
        resid_adjoint(c, xm.at[1])

    def close2(c):
        x2[c.t] = xm[0, c.t] + lin_forward(c, last[0])
        mu2[c.t] = xm[1, c.t, :rows, :] + lin_adjoint(c, last[2], ad2)[:rows]

    def finish(c):
        _, _, damp = c.terms()
        x, off = off_forward(c, x2)
        r = x * coef[8, c.t] + off + damp * jnp.tanh(x) - cf[c.t]
        res[c.t] = r[:rows]

    @pl.when(first_x)
    def _():
        known(1, 5, 7)
        start_lon(lon_w)

    arrive(up0, down0)
    each_main(prepare)
    sweeps(each_main, ad)
    each_main(close1)
    start_up(one_main[0])
    start_down(one_main[1])

    spot = lane_ring % GROUP
    from_w = (spot > 0) & (spot < halo)
    from_e = (spot >= kept) & (spot < GROUP - 1)
    spot_row = spot[:rows]
    for f in range(FIELDS):
        for side in range(2):
            for j in range(per):
                raw[f, strips + per * side + j, rows:, :] = gather(
                    lambda l: raw[f, l + 1, rows:, :], group_row, side, j
                )
    for k in range(2):
        for side in range(2):
            for j in range(per):
                rawx[k, strips + per * side + j] = gather(lambda l: rawx[k, l + 1], group_row, side, j)
    def unpack(side):
        recv, recvx, where, lead, nines = (
            (recv_w, recvx_w, from_w, 1, NINTH),
            (recv_e, recvx_e, from_e, kept, (CKPT,)),
        )[side]
        beyond = spot == (0 if side == 0 else GROUP - 1)
        for j in range(per):
            t = strips + per * side + j
            shift = lead - SLOT * j
            for f in range(FIELDS):
                tile = jnp.where(where, turn(recv[f], shift), raw[f, t])
                if f in nines:
                    tile = jnp.where(beyond, turn(recv[FIELDS], shift + nines.index(f)), tile)
                raw[f, t] = tile
            for k in range(2):
                rawx[k, t] = jnp.where(where[:rows], turn(recvx[k], shift), rawx[k, t])

    one_strips = (one(4, pl.ds(strips, per)), one(8, pl.ds(strips + per, per)))
    for side, copies in ((1, lon_w), (0, lon_e)):
        copies[0].wait_recv()
        arrive(copies[1], copies[2])
        unpack(side)
        each = functools.partial(each_strip, side)
        each(prepare)
        sweeps(each, ad)
        each(close1)
        start_up(one_strips[side][0])
        start_down(one_strips[side][1])

    arrive(*one_main)
    each_main(second)
    sweeps(each_main, ad2)
    each_main(close2)
    each_main(finish)

    for side in (1, 0):
        arrive(*one_strips[side])
        each = functools.partial(each_strip, side)
        each(second)
        sweeps(each, ad2)
        each(close2)
        each(finish)

    for copy in late_loads:
        copy.wait()

    west_edge = lane_row < DEPTH
    east_edge = lane_row >= lanes - DEPTH

    def merged(ref, l):
        j, g = l % per, l // per
        w = turn(ref[strips + j][:rows], -(GROUP * g + halo))
        e = turn(ref[strips + per + j][:rows], lanes - kept - GROUP * g)
        return jnp.where(west_edge, w, jnp.where(east_edge, e, ref[l + 1][:rows]))

    for l in range(levels):
        x = merged(x2, l)
        state_out[l] = x
        adj_out[l] = merged(mu2, l) + weight_ref[l] * (x - obs_ref[l])
        resid_out[l] = merged(res, l)

    flush(up0, down0)
    flush(*one_main)
    for copies in one_strips:
        flush(*copies)
    for copies in (lon_e, lon_w):
        copies[0].wait_send()
        flush(copies[1], copies[2])


def hand_over(a, b, c, x, y, z, sem):
    gives = [
        pltpu.make_async_copy(held, ref, sem.at[k])
        for k, (held, ref) in enumerate(((a, x), (b, y), (c, z)))
    ]
    for copy in gives:
        copy.start()
    for copy in gives:
        copy.wait()


def solution(mesh):
    nx, ny = mesh.shape["gx"], mesh.shape["gy"]

    def per_device(*arrays):
        levels, rows, lanes = arrays[0].shape
        groups = lanes // GROUP
        assert rows >= 2 * INNER and rows >= INNER + 1 and levels % groups == 0 and nx > 2
        per = levels // groups
        assert per * SLOT <= GROUP and GROUP >= 3 * DEPTH and len(NINTH) <= SLOT
        ring = 2 * rows
        tiles = levels + 2 + 2 * per
        f32 = jnp.float32
        out = jax.ShapeDtypeStruct((levels, rows, lanes), f32)
        hbm = pl.BlockSpec(memory_space=pltpu.HBM)
        vmem = pl.BlockSpec(memory_space=pltpu.VMEM)

        def buf(*shape):
            return pltpu.VMEM(shape, f32)

        def full():
            return buf(tiles, ring, lanes)

        def dma(n):
            return pltpu.SemaphoreType.DMA((n,))

        results = pl.pallas_call(
            functools.partial(kernel, nx, ny),
            name="step_pair",
            out_shape=(pltpu.VMEM(out.shape, f32),) * 3,
            in_specs=[hbm] * 13,
            out_specs=(vmem,) * 3,
            scratch_shapes=[
                buf(FIELDS, tiles, ring, lanes),
                buf(2, tiles, rows, lanes),
                buf(FIELDS + 1, rows, lanes),
                buf(FIELDS + 1, rows, lanes),
                buf(FIELDS + 1, ring, lanes),
                buf(FIELDS + 1, ring, lanes),
                buf(2, rows, lanes),
                buf(2, rows, lanes),
                buf(10, tiles, ring, lanes),
                full(),
                buf(2, tiles, ring, lanes),
                buf(tiles, rows, lanes),
                full(),
                buf(tiles, rows, lanes),
                buf(tiles, rows, lanes),
            ]
            + [full() for _ in range(11)]
            + [
                buf(3, per, ring, lanes),
                buf(levels, rows, lanes),
                buf(levels, rows, lanes),
                pltpu.SMEM((levels,), f32),
                pltpu.SMEM((levels,), f32),
                pltpu.SMEM((1,), jnp.int32),
                dma(FIELDS + 5),
                dma(5),
                dma(5),
                dma(8),
                dma(8),
                dma(12),
                dma(12),
                pltpu.SemaphoreType.REGULAR((8,)),
            ],
            compiler_params=pltpu.CompilerParams(
                collective_id=0, has_side_effects=True, vmem_limit_bytes=67043328 - 3 * 4 * math.prod(out.shape)
            ),
        )(*arrays)
        return pl.pallas_call(
            hand_over,
            name="hand_over",
            out_shape=(out, out, out),
            in_specs=[vmem] * 3,
            out_specs=(hbm, hbm, hbm),
            scratch_shapes=[dma(3)],
            compiler_params=pltpu.CompilerParams(vmem_limit_bytes=4 * 2**20),
        )(*results)

    block = P(None, "gy", "gx")
    return jax.shard_map(
        per_device,
        mesh=mesh,
        in_specs=(block,) * 7 + (P(), P(), block, block, block, P()),
        out_specs=(block,) * 3,
        check_vma=False,
    )
```

```python
import functools
import math

import jax
import jax.numpy as jnp
from jax import lax
from jax.experimental import pallas as pl
from jax.experimental.pallas import tpu as pltpu
from jax.sharding import PartitionSpec as P

OUTER = 2
INNER = 4
DAY_STEPS = 96
RELAXATION = 0.7

FIELDS = 8
CKPT, SOURCE, ED, EW, ND, NW, TRAJ, ADJF = range(FIELDS)

DEPTH = OUTER * INNER + 1
SLOT = DEPTH - 1
GROUP = 32
NINTH = (CKPT, ED, EW)

MESH = pl.DeviceIdType.MESH


def kernel(
    nx,
    ny,
    ckpt_h,
    traj_h,
    adjf_h,
    ed_h,
    nd_h,
    ew_h,
    nw_h,
    level_h,
    damp_h,
    source_h,
    obs_h,
    weight_h,
    step_h,
    state_out,
    resid_out,
    adj_out,
    raw,
    rawx,
    pack_e,
    pack_w,
    recv_e,
    recv_w,
    recvx_e,
    recvx_w,
    coef,
    cf,
    xm,
    x1x,
    x2,
    mu2,
    res,
    fw,
    fg,
    fd,
    fa,
    fb,
    aw,
    ag,
    ad,
    ad2,
    aa,
    ab,
    vert,
    late_ref,
    bytes_ref,
    level_ref,
    damp_ref,
    step_ref,
    load_sem,
    send,
    got,
    hello,
):
    levels, rows, lanes = state_out.shape
    wide = INNER
    ring = 2 * rows
    groups = lanes // GROUP
    per = levels // groups
    strips = levels + 2
    tiles = strips + 2 * per
    halo = DEPTH
    kept = GROUP - halo
    gx = lax.axis_index("gx")
    gy = lax.axis_index("gy")
    east = lax.rem(gx + 1, nx)
    west = lax.rem(gx + nx - 1, nx)
    has_n = gy < ny - 1
    has_s = gy > 0
    north = gy + 1
    south = gy - 1
    first_x = gx == 0
    last_x = gx == nx - 1

    inside = pl.ds(1, levels)
    main = pl.ds(0, rows)

    order = (ckpt_h, source_h, ed_h, ew_h, nd_h, nw_h, traj_h, adjf_h)
    loads = [
        pltpu.make_async_copy(h, raw.at[f, inside, main, :], load_sem.at[0])
        for f, h in enumerate(order)
    ]
    late_loads = [
        pltpu.make_async_copy(obs_h, late_ref.at[0], load_sem.at[1]),
        pltpu.make_async_copy(weight_h, late_ref.at[1], load_sem.at[1]),
    ]
    scalar_loads = [
        pltpu.make_async_copy(level_h, level_ref, load_sem.at[2]),
        pltpu.make_async_copy(damp_h, damp_ref, load_sem.at[3]),
        pltpu.make_async_copy(step_h, step_ref, load_sem.at[4]),
    ]

    barrier = pltpu.get_barrier_semaphore()
    odd_x = lax.rem(gx, 2) == 1
    odd_y = lax.rem(gy, 2) == 1
    even_y = jnp.logical_not(odd_y)
    inner_x = jnp.logical_not(first_x)
    before_e = jnp.logical_or(last_x, odd_x)
    before_w = jnp.logical_and(inner_x, odd_x)
    before_de = jnp.logical_or(last_x, even_y)
    before_dw = jnp.logical_and(inner_x, even_y)
    neighbours = (
        (east, gy, True, before_e),
        (west, gy, True, before_w),
        (gx, north, has_n, odd_y),
        (gx, south, has_s, odd_y),
        (east, north, has_n, before_de),
        (west, north, has_n, before_dw),
        (east, south, has_s, before_de),
        (west, south, has_s, before_dw),
    )
    answer_to = (1, 0, 3, 2, 1, 0, 1, 0)

    behind = 0
    for column, row, there, before in neighbours:
        behind = behind + jnp.logical_and(there, before).astype(jnp.int32)

        @pl.when(jnp.logical_and(there, jnp.logical_not(before)))
        def _():
            pl.semaphore_signal(
                barrier, inc=1, device_id={"gx": column, "gy": row}, device_id_type=MESH
            )

    for copy in loads + scalar_loads + late_loads:
        copy.start()

    @pl.when(behind > 0)
    def _():
        pl.semaphore_wait(barrier, behind)

    for k, (column, row, there, before) in enumerate(neighbours):

        @pl.when(jnp.logical_and(there, before))
        def _():
            pl.semaphore_signal(
                hello.at[answer_to[k]], inc=1, device_id={"gx": column, "gy": row}, device_id_type=MESH
            )

    def known(side, *ks):
        count = 0
        for k in ks:
            _, _, there, before = neighbours[k]
            count = count + jnp.logical_and(there, jnp.logical_not(before)).astype(jnp.int32)

        @pl.when(count > 0)
        def _():
            pl.semaphore_wait(hello.at[side], count)

    def wait_rows(n, sem):
        part = bytes_ref.at[pl.ds(0, n), :]
        pltpu.make_async_copy(part, part, sem).wait()

    def rows_of(copies):
        return sum(math.prod(copy.src_ref.shape) for copy in copies) // lanes

    def remote(src, dst, send, got, column, row):
        return pltpu.make_async_remote_copy(
            src_ref=src,
            dst_ref=dst,
            send_sem=send,
            recv_sem=got,
            device_id={"gx": column, "gy": row},
            device_id_type=MESH,
        )

    low = pl.ds(0, wide)
    high = pl.ds(rows - wide, wide)
    from_n = pl.ds(rows, wide)
    from_s = pl.ds(ring - wide, wide)
    next_low = pl.ds(wide, 1)
    next_high = pl.ds(rows - wide - 1, 1)
    extra_n = pl.ds(wide - 1, 1)
    extra_s = pl.ds(wide, 1)

    faces = pl.ds(ND, 2)

    up0 = [
        remote(raw.at[:, inside, high, :], raw.at[:, inside, from_s, :], send.at[0], got.at[0], gx, north),
        remote(
            raw.at[faces, inside, next_high, :], rawx.at[:, inside, extra_s, :], send.at[0], got.at[0], gx, north
        ),
    ]
    down0 = [
        remote(raw.at[:, inside, low, :], raw.at[:, inside, from_n, :], send.at[1], got.at[1], gx, south)
    ]

    def lon_copies(k, pack, recv, recvx, column):
        return (
            [remote(pack, recv.at[:, main, :], send.at[2], got.at[k], column, gy)],
            [
                remote(
                    pack.at[:, high, :], recv.at[:, from_s, :], send.at[0], got.at[k + 1], column, north
                ),
                remote(
                    pack.at[faces, next_high, :],
                    recvx.at[:, extra_s, :],
                    send.at[0],
                    got.at[k + 1],
                    column,
                    north,
                ),
            ],
            [
                remote(
                    pack.at[:, low, :], recv.at[:, from_n, :], send.at[1], got.at[k + 2], column, south
                )
            ],
        )

    lon_e = lon_copies(2, pack_e, recv_w, recvx_w, east)
    lon_w = lon_copies(5, pack_w, recv_e, recvx_e, west)

    def one(k, part):
        def copy(way, src, dst, row):
            return remote(src, dst, send.at[way], got.at[k + way], gx, row)

        return (
            [
                copy(0, xm.at[:, part, high, :], xm.at[:, part, from_s, :], north),
                copy(0, xm.at[0, part, next_high, :], x1x.at[part, extra_s, :], north),
            ],
            [
                copy(1, xm.at[:, part, low, :], xm.at[:, part, from_n, :], south),
                copy(1, xm.at[0, part, next_low, :], x1x.at[part, extra_n, :], south),
            ],
        )

    one_main = one(8, inside)
    one_strips = (one(10, pl.ds(strips, per)), one(12, pl.ds(strips + per, per)))

    def start_up(up):
        @pl.when(has_n)
        def _():
            for copy in up:
                copy.start()

    def start_down(down):
        @pl.when(has_s)
        def _():
            for copy in down:
                copy.start()

    def start_lon(copies):
        copies[0][0].start()
        start_up(copies[1])
        start_down(copies[2])

    def arrive(k, up, down):
        @pl.when(has_s)
        def _():
            wait_rows(rows_of(up), got.at[k])

        @pl.when(has_n)
        def _():
            wait_rows(rows_of(down), got.at[k + 1])

    def arrive_lon(k, copies):
        wait_rows(rows_of(copies[0]), got.at[k])
        arrive(k + 1, copies[1], copies[2])

    def flush():
        exchanges = ((up0, down0), one_main, *one_strips, lon_e[1:], lon_w[1:])

        @pl.when(has_n)
        def _():
            wait_rows(sum(rows_of(up) for up, _ in exchanges), send.at[0])

        @pl.when(has_s)
        def _():
            wait_rows(sum(rows_of(down) for _, down in exchanges), send.at[1])

        wait_rows(rows_of(lon_e[0] + lon_w[0]), send.at[2])

    zero_ring = jnp.zeros((ring, lanes), jnp.float32)
    zero_tile = jnp.zeros((rows, lanes), jnp.float32)
    for t in (0, levels + 1):
        raw[CKPT, t] = zero_ring
        for ref in (fa, fb, aa, ab, x2):
            ref[t] = zero_ring
        for k in range(2):
            xm[k, t] = zero_ring

    def clear(part):
        zero = jnp.zeros((wide, lanes), jnp.float32)

        def body(l, carry):
            for f in range(FIELDS):
                raw[f, l + 1, part, :] = zero
            for k in range(2):
                xm[k, l + 1, part, :] = zero
            return carry

        lax.fori_loop(0, levels, body, 0)
        for t in range(strips, tiles):
            for k in range(2):
                xm[k, t, part, :] = zero
        for f in range(FIELDS + 1):
            recv_e[f, part, :] = zero
            recv_w[f, part, :] = zero

    def clear_extra(part):
        zero = jnp.zeros((1, lanes), jnp.float32)
        for t in [*range(1, levels + 1), *range(strips, tiles)]:
            x1x[t, part, :] = zero

    @pl.when(jnp.logical_not(has_n))
    def _():
        clear(from_n)
        clear_extra(extra_n)

    @pl.when(jnp.logical_not(has_s))
    def _():
        clear(from_s)
        clear_extra(extra_s)
        zero = jnp.zeros((1, lanes), jnp.float32)
        for k in range(2):
            for t in range(1, levels + 1):
                rawx[k, t, extra_s, :] = zero
            recvx_e[k, extra_s, :] = zero
            recvx_w[k, extra_s, :] = zero

    wait_rows(levels * FIELDS * rows, load_sem.at[0])

    def send_lat():
        known(2, 2)
        start_up(up0)
        known(3, 3)
        start_down(down0)

    @pl.when(jnp.logical_not(last_x))
    def _():
        send_lat()


    lane_row = lax.broadcasted_iota(jnp.int32, (rows, lanes), 1)
    lane_ring = lax.broadcasted_iota(jnp.int32, (ring, lanes), 1)
    row_ring = lax.broadcasted_iota(jnp.int32, (ring, lanes), 0)

    def turn(v, shift, axis=1):
        shift = shift % v.shape[axis]
        return pltpu.roll(v, shift, axis) if shift else v

    def choose(place, values):
        out = values[-1]
        for k in range(len(values) - 2, -1, -1):
            out = jnp.where(place == k, values[k], out)
        return out

    def gather(read, place, side, j):
        start = halo if side == 0 else kept
        return choose(place, [turn(read(j + per * g), GROUP * g + start) for g in range(groups)])

    group_row = lane_row // GROUP
    nine_row = lane_row % SLOT

    def slots(f, shift, turns=(0,)):
        rolled = [turn(raw[f, level_of(k) + 1, :rows, :], SLOT * k + shift) for k in range(levels)]
        return [choose((lane_row // SLOT + move) % levels, rolled) for move in turns]

    def level_of(k):
        return k % per + per * (k // per)

    nine = None
    for f in range(FIELDS):
        if f in NINTH:
            pack_e[f], beside = slots(f, SLOT, (0, 1))
            i = NINTH.index(f)
            beside = turn(beside, -i)
            nine = beside if nine is None else jnp.where(nine_row == SLOT - 1 - i, beside, nine)
        else:
            (pack_e[f],) = slots(f, SLOT)
    pack_e[FIELDS] = nine

    @pl.when(last_x)
    def _():
        start_lon(lon_e)
        send_lat()

    for f in range(FIELDS):
        if f == CKPT:
            pack_w[f], pack_w[FIELDS] = slots(f, 0, (0, -1))
        else:
            (pack_w[f],) = slots(f, 0)

    @pl.when(inner_x)
    def _():
        known(1, 1, 5, 7)
        start_lon(lon_w)

    @pl.when(jnp.logical_not(last_x))
    def _():
        known(0, 0, 4, 6)
        start_lon(lon_e)

    for f in range(FIELDS):
        for side in range(2):
            for j in range(per):
                raw[f, strips + per * side + j, :rows, :] = gather(
                    lambda l: raw[f, l + 1, :rows, :], group_row, side, j
                )

    for copy in scalar_loads:
        copy.wait()

    total_lanes = lanes * nx

    def heat_of(column):
        column = gx * lanes + column
        column = jnp.where(column < 0, column + total_lanes, column)
        column = jnp.where(column >= total_lanes, column - total_lanes, column)
        phase = (
            2.0 * math.pi * column.astype(jnp.float32) / total_lanes
            - 2.0 * math.pi * step_ref[0].astype(jnp.float32) / DAY_STEPS
        )
        return jnp.cos(phase)

    lane_one = lax.broadcasted_iota(jnp.int32, (1, lanes), 1)
    heat_main = heat_of(lane_one)
    heat_side = (
        heat_of(lane_one % GROUP - halo),
        heat_of(lane_one % GROUP + (lanes - kept)),
    )
    row_global = gy * rows + jnp.where(row_ring < rows + wide, row_ring, row_ring - ring)
    open_face = (row_global >= 0) & (row_global < rows * ny - 1)

    def level_terms(l):
        up = jnp.where(l < levels - 1, level_ref[l], 0.0)
        down = jnp.where(l > 0, level_ref[jnp.maximum(l - 1, 0)], 0.0)
        return up, down, damp_ref[l]

    group_one = lane_ring // GROUP
    for j in range(per):
        terms = [level_terms(j + per * g) for g in range(groups)]
        for k in range(3):
            vert[k, j] = choose(group_one, [jnp.full((ring, lanes), term[k]) for term in terms])

    class Main:
        def __init__(self, l):
            self.t = l + 1
            self.l = l
            self.heat = heat_main

        def terms(self):
            return level_terms(self.l)

        def above(self, ref):
            return ref[self.t + 1]

        def below(self, ref):
            return ref[self.t - 1]

    class Strip:
        def __init__(self, k):
            self.t = strips + k
            self.j = k % per
            self.base = strips + k - self.j
            self.heat = heat_side[k // per]

        def terms(self):
            return vert[0, self.j], vert[1, self.j], vert[2, self.j]

        def above(self, ref):
            if self.j < per - 1:
                return ref[self.t + 1]
            return turn(ref[self.base], -GROUP)

        def below(self, ref):
            if self.j > 0:
                return ref[self.t - 1]
            return turn(ref[self.base + per - 1], GROUP)

    def each_main(body):
        def step(l, carry):
            body(Main(l))
            return carry

        lax.fori_loop(0, levels, step, 0, unroll=True)

    def each_strip(side, body):
        for j in range(per):
            body(Strip(per * side + j))

    def off_forward(c, ref, extra=None):
        up, down, _ = c.terms()
        v = ref[c.t]
        above = turn(v, -1, 0)
        below = turn(v, 1, 0)
        if extra is not None:
            more = jnp.concatenate([extra[c.t], extra[c.t]], axis=0)
            above = jnp.where(row_ring == rows + wide - 1, more, above)
            below = jnp.where(row_ring == rows + wide, more, below)
        off = (
            turn(v, -1) * coef[1, c.t]
            - turn(v, 1) * coef[2, c.t]
            + above * coef[5, c.t]
            - below * coef[6, c.t]
            - up * c.above(ref)
            - down * c.below(ref)
        )
        return v, off

    def off_adjoint(c, ref):
        up, down, _ = c.terms()
        v = ref[c.t]
        off = (
            turn(v, 1) * coef[3, c.t]
            - turn(v, -1) * coef[0, c.t]
            + turn(v, 1, 0) * coef[7, c.t]
            - turn(v, -1, 0) * coef[4, c.t]
            - up * c.above(ref)
            - down * c.below(ref)
        )
        return v, off

    def resid_forward(c, ref, extra=None):
        _, _, damp = c.terms()
        x, off = off_forward(c, ref, extra)
        t = jnp.tanh(x)
        local = damp * (1.0 - t * t)
        diag = coef[8, c.t]
        r = x * diag + off + damp * t - cf[c.t]
        w = RELAXATION / (coef[9, c.t] + local)
        d = -w * r
        fw[c.t] = w
        fg[c.t] = 1.0 - w * (diag + local)
        fd[c.t] = d
        fa[c.t] = d

    def resid_adjoint(c, ref):
        m, off = off_adjoint(c, ref)
        d = ad[c.t] - (1.0 - ag[c.t]) * m - aw[c.t] * off
        ad2[c.t] = d
        aa[c.t] = d

    def lin_forward(c, src):
        v, off = off_forward(c, src)
        return fg[c.t] * v + fd[c.t] - fw[c.t] * off

    def lin_adjoint(c, src, base):
        v, off = off_adjoint(c, src)
        return ag[c.t] * v + base[c.t] - aw[c.t] * off

    def prepare(c):
        up, down, damp = c.terms()
        de = raw[ED, c.t]
        fe = 0.5 * raw[EW, c.t]
        dn = jnp.where(open_face, raw[ND, c.t], 0.0)
        fn = jnp.where(open_face, 0.5 * raw[NW, c.t], 0.0)
        dnx = rawx[0, c.t]
        fnx = 0.5 * rawx[1, c.t]
        anx, bnx = fnx + dnx, fnx - dnx
        a, b = fe + de, fe - de
        an, bn = fn + dn, fn - dn
        a_w = turn(a, 1)
        b_w = turn(b, 1)
        last = row_ring == rows + wide
        an_s = jnp.where(last, jnp.concatenate([anx, anx], axis=0), turn(an, 1, 0))
        bn_s = jnp.where(last, jnp.concatenate([bnx, bnx], axis=0), turn(bn, 1, 0))
        diag = 1.0 + (a - b_w) + (an - bn_s) + (up + down)
        total = 1.0 + de + 0.5 * (a_w - b_w) + dn + 0.5 * (an_s - bn_s) + (up + down)
        for k, value in enumerate((a, b, a_w, b_w, an, bn, an_s, bn_s, diag, total)):
            coef[k, c.t] = value
        cf[c.t] = raw[CKPT, c.t] + raw[SOURCE, c.t] * c.heat
        t = jnp.tanh(raw[TRAJ, c.t])
        local = damp * (1.0 - t * t)
        w = RELAXATION / (total + local)
        start_delta = w * raw[ADJF, c.t]
        aw[c.t] = w
        ag[c.t] = 1.0 - w * (diag + local)
        ad[c.t] = start_delta
        aa[c.t] = start_delta
        resid_forward(c, raw.at[CKPT])

    pairs = ((fa, fb, aa, ab), (fb, fa, ab, aa))
    last = pairs[(INNER - 2) % 2]

    def sweeps(each, base):
        for k in range(INNER - 2):
            f_src, f_dst, a_src, a_dst = pairs[k % 2]

            def body(c):
                f_dst[c.t] = lin_forward(c, f_src)
                a_dst[c.t] = lin_adjoint(c, a_src, base)

            each(body)

    def close1(c):
        xm[0, c.t, :rows, :] = raw[CKPT, c.t, :rows, :] + lin_forward(c, last[0])[:rows]
        xm[1, c.t, :rows, :] = lin_adjoint(c, last[2], ad)[:rows]

    def second(c):
        resid_forward(c, xm.at[0], x1x)
        resid_adjoint(c, xm.at[1])

    def close2(c):
        x2[c.t] = xm[0, c.t] + lin_forward(c, last[0])
        mu2[c.t] = xm[1, c.t, :rows, :] + lin_adjoint(c, last[2], ad2)[:rows]

    def finish(c):
        _, _, damp = c.terms()
        x, off = off_forward(c, x2)
        r = x * coef[8, c.t] + off + damp * jnp.tanh(x) - cf[c.t]
        res[c.t] = r[:rows]

    @pl.when(first_x)
    def _():
        known(1, 1, 5, 7)
        start_lon(lon_w)

    arrive(0, up0, down0)
    each_main(prepare)
    sweeps(each_main, ad)
    each_main(close1)
    start_up(one_main[0])
    start_down(one_main[1])

    spot = lane_ring % GROUP
    from_w = (spot > 0) & (spot < halo)
    from_e = (spot >= kept) & (spot < GROUP - 1)
    spot_row = spot[:rows]
    for f in range(FIELDS):
        for side in range(2):
            for j in range(per):
                raw[f, strips + per * side + j, rows:, :] = gather(
                    lambda l: raw[f, l + 1, rows:, :], group_row, side, j
                )
    for k in range(2):
        for side in range(2):
            for j in range(per):
                rawx[k, strips + per * side + j] = gather(lambda l: rawx[k, l + 1], group_row, side, j)
    def unpack(side):
        recv, recvx, where, lead, nines = (
            (recv_w, recvx_w, from_w, 1, NINTH),
            (recv_e, recvx_e, from_e, kept, (CKPT,)),
        )[side]
        beyond = spot == (0 if side == 0 else GROUP - 1)
        for j in range(per):
            t = strips + per * side + j
            shift = lead - SLOT * j
            for f in range(FIELDS):
                tile = jnp.where(where, turn(recv[f], shift), raw[f, t])
                if f in nines:
                    tile = jnp.where(beyond, turn(recv[FIELDS], shift + nines.index(f)), tile)
                raw[f, t] = tile
            for k in range(2):
                rawx[k, t] = jnp.where(where[:rows], turn(recvx[k], shift), rawx[k, t])

    for side, k, copies in ((1, 5, lon_w), (0, 2, lon_e)):
        arrive_lon(k, copies)
        unpack(side)
        each = functools.partial(each_strip, side)
        each(prepare)
        sweeps(each, ad)
        each(close1)
        start_up(one_strips[side][0])
        start_down(one_strips[side][1])

    arrive(8, *one_main)
    each_main(second)
    sweeps(each_main, ad2)
    each_main(close2)
    each_main(finish)

    east_edge = lane_row >= lanes - DEPTH

    def merge_east():
        for ref, out in ((x2, state_out), (mu2, adj_out), (res, resid_out)):
            for l in range(levels):
                j, g = l % per, l // per
                e = turn(ref[strips + per + j][:rows], lanes - kept - GROUP * g)
                out[l] = jnp.where(east_edge, e, ref[l + 1][:rows])

    for side in (1, 0):
        arrive(10 + 2 * side, *one_strips[side])
        each = functools.partial(each_strip, side)
        each(second)
        sweeps(each, ad2)
        each(close2)
        each(finish)
        if side == 1:
            merge_east()
            wait_rows(2 * levels * rows, load_sem.at[1])

    west_edge = lane_row < DEPTH

    def west_merged(ref, l, here):
        j, g = l % per, l // per
        return jnp.where(west_edge, turn(ref[strips + j][:rows], -(GROUP * g + halo)), here)

    for l in range(levels):
        x = west_merged(x2, l, state_out[l])
        state_out[l] = x
        adj_out[l] = west_merged(mu2, l, adj_out[l]) + late_ref[1, l] * (x - late_ref[0, l])
        resid_out[l] = west_merged(res, l, resid_out[l])

    flush()


def hand_over(a, b, c, x, y, z, sem):
    gives = [
        pltpu.make_async_copy(held, ref, sem.at[k])
        for k, (held, ref) in enumerate(((a, x), (b, y), (c, z)))
    ]
    for copy in gives:
        copy.start()
    for copy in gives:
        copy.wait()


def solution(mesh):
    nx, ny = mesh.shape["gx"], mesh.shape["gy"]

    def per_device(*arrays):
        levels, rows, lanes = arrays[0].shape
        groups = lanes // GROUP
        assert rows >= 2 * INNER and rows >= INNER + 1 and levels % groups == 0 and nx > 2
        per = levels // groups
        assert per * SLOT <= GROUP and GROUP >= 3 * DEPTH and len(NINTH) <= SLOT
        ring = 2 * rows
        tiles = levels + 2 + 2 * per
        f32 = jnp.float32
        out = jax.ShapeDtypeStruct((levels, rows, lanes), f32)
        hbm = pl.BlockSpec(memory_space=pltpu.HBM)
        vmem = pl.BlockSpec(memory_space=pltpu.VMEM)

        def buf(*shape):
            return pltpu.VMEM(shape, f32)

        def full():
            return buf(tiles, ring, lanes)

        def dma(n):
            return pltpu.SemaphoreType.DMA((n,))

        results = pl.pallas_call(
            functools.partial(kernel, nx, ny),
            name="step_pair",
            out_shape=(pltpu.VMEM(out.shape, f32),) * 3,
            in_specs=[hbm] * 13,
            out_specs=(vmem,) * 3,
            scratch_shapes=[
                buf(FIELDS, tiles, ring, lanes),
                buf(2, tiles, rows, lanes),
                buf(FIELDS + 1, rows, lanes),
                buf(FIELDS + 1, rows, lanes),
                buf(FIELDS + 1, ring, lanes),
                buf(FIELDS + 1, ring, lanes),
                buf(2, rows, lanes),
                buf(2, rows, lanes),
                buf(10, tiles, ring, lanes),
                full(),
                buf(2, tiles, ring, lanes),
                buf(tiles, rows, lanes),
                full(),
                buf(tiles, rows, lanes),
                buf(tiles, rows, lanes),
            ]
            + [full() for _ in range(11)]
            + [
                buf(3, per, ring, lanes),
                buf(2, levels, rows, lanes),
                buf(FIELDS * levels * rows, lanes),
                pltpu.SMEM((levels,), f32),
                pltpu.SMEM((levels,), f32),
                pltpu.SMEM((1,), jnp.int32),
                dma(5),
                dma(3),
                dma(14),
                pltpu.SemaphoreType.REGULAR((4,)),
            ],
            compiler_params=pltpu.CompilerParams(
                collective_id=0, has_side_effects=True, vmem_limit_bytes=67043328 - 3 * 4 * math.prod(out.shape)
            ),
        )(*arrays)
        return pl.pallas_call(
            hand_over,
            name="hand_over",
            out_shape=(out, out, out),
            in_specs=[vmem] * 3,
            out_specs=(hbm, hbm, hbm),
            scratch_shapes=[dma(3)],
            compiler_params=pltpu.CompilerParams(vmem_limit_bytes=4 * 2**20),
        )(*results)

    block = P(None, "gy", "gx")
    return jax.shard_map(
        per_device,
        mesh=mesh,
        in_specs=(block,) * 7 + (P(), P(), block, block, block, P()),
        out_specs=(block,) * 3,
        check_vma=False,
    )
```

```python
import functools
import math

import jax
import jax.numpy as jnp
from jax import lax
from jax.experimental import pallas as pl
from jax.experimental.pallas import tpu as pltpu
from jax.sharding import PartitionSpec as P

OUTER = 2
INNER = 4
DAY_STEPS = 96
RELAXATION = 0.7

FIELDS = 8
ND, NW, CKPT, ED, EW, SOURCE, TRAJ, ADJF = range(FIELDS)
CORNER = 5

DEPTH = OUTER * INNER + 1
SLOT = DEPTH - 1
GROUP = 32
NINTH = (CKPT, ED, EW)

MESH = pl.DeviceIdType.MESH


def kernel(
    nx,
    ny,
    ckpt_h,
    traj_h,
    adjf_h,
    ed_h,
    nd_h,
    ew_h,
    nw_h,
    level_h,
    damp_h,
    source_h,
    obs_h,
    weight_h,
    step_h,
    state_out,
    resid_out,
    adj_out,
    raw,
    rawx,
    pack_e,
    pack_w,
    recv_e,
    recv_w,
    coef,
    cf,
    xm,
    x1x,
    x2,
    mu2,
    res,
    fw,
    fg,
    fd,
    fa,
    fb,
    aw,
    ag,
    ad,
    ad2,
    aa,
    ab,
    vert,
    late_ref,
    bytes_ref,
    level_ref,
    damp_ref,
    step_ref,
    load_sem,
    send,
    got,
    hello,
):
    levels, rows, lanes = state_out.shape
    wide = INNER
    ring = 2 * rows
    groups = lanes // GROUP
    per = levels // groups
    strips = levels + 2
    tiles = strips + 2 * per
    halo = DEPTH
    kept = GROUP - halo
    gx = lax.axis_index("gx")
    gy = lax.axis_index("gy")
    east = lax.rem(gx + 1, nx)
    west = lax.rem(gx + nx - 1, nx)
    has_n = gy < ny - 1
    has_s = gy > 0
    north = gy + 1
    south = gy - 1
    first_x = gx == 0
    last_x = gx == nx - 1

    inside = pl.ds(1, levels)
    main = pl.ds(0, rows)

    order = (nd_h, nw_h, ckpt_h, ed_h, ew_h, source_h, traj_h, adjf_h)
    loads = [
        pltpu.make_async_copy(h, raw.at[f, inside, main, :], load_sem.at[0])
        for f, h in enumerate(order)
    ]
    late_loads = [
        pltpu.make_async_copy(obs_h, late_ref.at[0], load_sem.at[1]),
        pltpu.make_async_copy(weight_h, late_ref.at[1], load_sem.at[1]),
    ]
    scalar_loads = [
        pltpu.make_async_copy(level_h, level_ref, load_sem.at[2]),
        pltpu.make_async_copy(damp_h, damp_ref, load_sem.at[3]),
        pltpu.make_async_copy(step_h, step_ref, load_sem.at[4]),
    ]

    barrier = pltpu.get_barrier_semaphore()
    odd_x = lax.rem(gx, 2) == 1
    odd_y = lax.rem(gy, 2) == 1
    even_y = jnp.logical_not(odd_y)
    inner_x = jnp.logical_not(first_x)
    before_e = jnp.logical_or(last_x, odd_x)
    before_w = jnp.logical_and(inner_x, odd_x)
    before_de = jnp.logical_or(last_x, even_y)
    before_dw = jnp.logical_and(inner_x, even_y)
    neighbours = (
        (east, gy, True, before_e),
        (west, gy, True, before_w),
        (gx, north, has_n, odd_y),
        (gx, south, has_s, odd_y),
        (east, north, has_n, before_de),
        (west, north, has_n, before_dw),
        (east, south, has_s, before_de),
        (west, south, has_s, before_dw),
    )
    answer_to = (1, 0, 3, 2, 1, 0, 1, 0)

    behind = 0
    for column, row, there, before in neighbours:
        behind = behind + jnp.logical_and(there, before).astype(jnp.int32)

        @pl.when(jnp.logical_and(there, jnp.logical_not(before)))
        def _():
            pl.semaphore_signal(
                barrier, inc=1, device_id={"gx": column, "gy": row}, device_id_type=MESH
            )

    for copy in loads + scalar_loads + late_loads:
        copy.start()

    @pl.when(behind > 0)
    def _():
        pl.semaphore_wait(barrier, behind)

    for k, (column, row, there, before) in enumerate(neighbours):

        @pl.when(jnp.logical_and(there, before))
        def _():
            pl.semaphore_signal(
                hello.at[answer_to[k]], inc=1, device_id={"gx": column, "gy": row}, device_id_type=MESH
            )

    def known(side, *ks):
        count = 0
        for k in ks:
            _, _, there, before = neighbours[k]
            count = count + jnp.logical_and(there, jnp.logical_not(before)).astype(jnp.int32)

        @pl.when(count > 0)
        def _():
            pl.semaphore_wait(hello.at[side], count)

    def wait_rows(n, sem):
        part = bytes_ref.at[pl.ds(0, n), :]
        pltpu.make_async_copy(part, part, sem).wait()

    def rows_of(copies):
        return sum(math.prod(copy.src_ref.shape) for copy in copies) // lanes

    def remote(src, dst, send, got, column, row):
        return pltpu.make_async_remote_copy(
            src_ref=src,
            dst_ref=dst,
            send_sem=send,
            recv_sem=got,
            device_id={"gx": column, "gy": row},
            device_id_type=MESH,
        )

    low = pl.ds(0, wide)
    high = pl.ds(rows - wide, wide)
    from_n = pl.ds(rows, wide)
    from_s = pl.ds(ring - wide, wide)
    next_low = pl.ds(wide, 1)
    next_high = pl.ds(rows - wide - 1, 1)
    near_low = pl.ds(0, wide - 1)
    near_high = pl.ds(rows - wide + 1, wide - 1)
    near_n = pl.ds(rows, wide - 1)
    near_s = pl.ds(ring - wide + 1, wide - 1)
    last_low = pl.ds(wide - 1, 1)
    last_high = pl.ds(rows - wide, 1)
    last_n = pl.ds(rows + wide - 1, 1)
    last_s = pl.ds(ring - wide, 1)
    extra_n = pl.ds(wide - 1, 1)
    extra_s = pl.ds(wide, 1)

    faces = pl.ds(ND, 2)

    def copy(k, src, dst, column, row):
        return remote(src, dst, send.at[0], got.at[k], column, row)

    up0 = [
        copy(0, raw.at[:, inside, high, :], raw.at[:, inside, from_s, :], gx, north),
        copy(0, raw.at[faces, inside, next_high, :], rawx.at[:, inside, extra_s, :], gx, north),
    ]
    down0 = [copy(0, raw.at[:, inside, low, :], raw.at[:, inside, from_n, :], gx, south)]

    some = pl.ds(0, CORNER)

    def lon_copies(k, pack, recv, column):
        return (
            [copy(k, pack, recv.at[:, main, :], column, gy)],
            [
                copy(k, pack.at[:, near_high, :], recv.at[:, near_s, :], column, north),
                copy(k, pack.at[some, last_high, :], recv.at[some, last_s, :], column, north),
            ],
            [
                copy(k, pack.at[:, near_low, :], recv.at[:, near_n, :], column, south),
                copy(k, pack.at[some, last_low, :], recv.at[some, last_n, :], column, south),
            ],
        )

    lon_e = lon_copies(1, pack_e, recv_w, east)
    lon_w = lon_copies(2, pack_w, recv_e, west)

    def one(k, part):
        return (
            [
                copy(k, xm.at[:, part, high, :], xm.at[:, part, from_s, :], gx, north),
                copy(k, xm.at[0, part, next_high, :], x1x.at[part, extra_s, :], gx, north),
            ],
            [
                copy(k, xm.at[:, part, low, :], xm.at[:, part, from_n, :], gx, south),
                copy(k, xm.at[0, part, next_low, :], x1x.at[part, extra_n, :], gx, south),
            ],
        )

    one_main = one(3, inside)
    one_strips = (one(4, pl.ds(strips, per)), one(5, pl.ds(strips + per, per)))

    def start_up(up):
        @pl.when(has_n)
        def _():
            for copy in up:
                copy.start()

    def start_down(down):
        @pl.when(has_s)
        def _():
            for copy in down:
                copy.start()

    def start_lon(copies):
        copies[0][0].start()
        start_up(copies[1])
        start_down(copies[2])

    def wait_all(always, up, down, with_up, with_down, sem):
        n, n_up, n_down = rows_of(always), rows_of(up), rows_of(down)
        cases = (
            (jnp.logical_and(with_up, with_down), n + n_up + n_down),
            (jnp.logical_and(with_up, jnp.logical_not(with_down)), n + n_up),
            (jnp.logical_and(with_down, jnp.logical_not(with_up)), n + n_down),
            (jnp.logical_not(jnp.logical_or(with_up, with_down)), n),
        )
        for case, total in cases:
            if total:

                @pl.when(case)
                def _():
                    wait_rows(total, sem)

    def arrive(k, up, down):
        wait_all([], up, down, has_s, has_n, got.at[k])

    def arrive_lon(k, copies):
        wait_all(*copies, has_s, has_n, got.at[k])

    def flush():
        exchanges = ((up0, down0), one_main, *one_strips, lon_e[1:], lon_w[1:])
        wait_all(
            lon_e[0] + lon_w[0],
            [copy for up, _ in exchanges for copy in up],
            [copy for _, down in exchanges for copy in down],
            has_n,
            has_s,
            send.at[0],
        )

    zero_ring = jnp.zeros((ring, lanes), jnp.float32)
    zero_tile = jnp.zeros((rows, lanes), jnp.float32)
    for t in (0, levels + 1):
        raw[CKPT, t] = zero_ring
        for ref in (fa, fb, aa, ab, x2):
            ref[t] = zero_ring
        for k in range(2):
            xm[k, t] = zero_ring

    def clear(part):
        zero = jnp.zeros((wide, lanes), jnp.float32)

        def body(l, carry):
            for f in range(FIELDS):
                raw[f, l + 1, part, :] = zero
            for k in range(2):
                xm[k, l + 1, part, :] = zero
            return carry

        lax.fori_loop(0, levels, body, 0)
        for t in range(strips, tiles):
            for k in range(2):
                xm[k, t, part, :] = zero
        for f in range(FIELDS + 1):
            recv_e[f, part, :] = zero
            recv_w[f, part, :] = zero

    def clear_extra(part):
        zero = jnp.zeros((1, lanes), jnp.float32)
        for t in [*range(1, levels + 1), *range(strips, tiles)]:
            x1x[t, part, :] = zero

    @pl.when(jnp.logical_not(has_n))
    def _():
        clear(from_n)
        clear_extra(extra_n)

    @pl.when(jnp.logical_not(has_s))
    def _():
        clear(from_s)
        clear_extra(extra_s)
        zero = jnp.zeros((1, lanes), jnp.float32)
        for k in range(2):
            for t in range(1, levels + 1):
                rawx[k, t, extra_s, :] = zero

    wait_rows(levels * FIELDS * rows, load_sem.at[0])

    def send_lat():
        known(2, 2)
        start_up(up0)
        known(3, 3)
        start_down(down0)

    @pl.when(jnp.logical_not(last_x))
    def _():
        send_lat()


    lane_row = lax.broadcasted_iota(jnp.int32, (rows, lanes), 1)
    lane_ring = lax.broadcasted_iota(jnp.int32, (ring, lanes), 1)
    row_ring = lax.broadcasted_iota(jnp.int32, (ring, lanes), 0)

    def turn(v, shift, axis=1):
        shift = shift % v.shape[axis]
        return pltpu.roll(v, shift, axis) if shift else v

    def choose(place, values):
        out = values[-1]
        for k in range(len(values) - 2, -1, -1):
            out = jnp.where(place == k, values[k], out)
        return out

    def gather(read, place, side, j):
        start = halo if side == 0 else kept
        return choose(place, [turn(read(j + per * g), GROUP * g + start) for g in range(groups)])

    group_row = lane_row // GROUP
    nine_row = lane_row % SLOT

    def slots(f, shift, turns=(0,)):
        rolled = [turn(raw[f, level_of(k) + 1, :rows, :], SLOT * k + shift) for k in range(levels)]
        return [choose((lane_row // SLOT + move) % levels, rolled) for move in turns]

    def level_of(k):
        return k % per + per * (k // per)

    nine = None
    for f in range(FIELDS):
        if f in NINTH:
            pack_e[f], beside = slots(f, SLOT, (0, 1))
            i = NINTH.index(f)
            beside = turn(beside, -i)
            nine = beside if nine is None else jnp.where(nine_row == SLOT - 1 - i, beside, nine)
        else:
            (pack_e[f],) = slots(f, SLOT)
    pack_e[FIELDS] = nine

    @pl.when(last_x)
    def _():
        start_lon(lon_e)
        send_lat()

    for f in range(FIELDS):
        if f == CKPT:
            pack_w[f], pack_w[FIELDS] = slots(f, 0, (0, -1))
        else:
            (pack_w[f],) = slots(f, 0)

    @pl.when(inner_x)
    def _():
        known(1, 1, 5, 7)
        start_lon(lon_w)

    @pl.when(jnp.logical_not(last_x))
    def _():
        known(0, 0, 4, 6)
        start_lon(lon_e)

    for f in range(FIELDS):
        for side in range(2):
            for j in range(per):
                raw[f, strips + per * side + j, :rows, :] = gather(
                    lambda l: raw[f, l + 1, :rows, :], group_row, side, j
                )

    for copy in scalar_loads:
        copy.wait()

    total_lanes = lanes * nx

    def heat_of(column):
        column = gx * lanes + column
        column = jnp.where(column < 0, column + total_lanes, column)
        column = jnp.where(column >= total_lanes, column - total_lanes, column)
        phase = (
            2.0 * math.pi * column.astype(jnp.float32) / total_lanes
            - 2.0 * math.pi * step_ref[0].astype(jnp.float32) / DAY_STEPS
        )
        return jnp.cos(phase)

    lane_one = lax.broadcasted_iota(jnp.int32, (1, lanes), 1)
    heat_main = heat_of(lane_one)
    heat_side = (
        heat_of(lane_one % GROUP - halo),
        heat_of(lane_one % GROUP + (lanes - kept)),
    )
    row_global = gy * rows + jnp.where(row_ring < rows + wide, row_ring, row_ring - ring)
    open_face = (row_global >= 0) & (row_global < rows * ny - 1)

    def level_terms(l):
        up = jnp.where(l < levels - 1, level_ref[l], 0.0)
        down = jnp.where(l > 0, level_ref[jnp.maximum(l - 1, 0)], 0.0)
        return up, down, damp_ref[l]

    group_one = lane_ring // GROUP
    for j in range(per):
        terms = [level_terms(j + per * g) for g in range(groups)]
        for k in range(3):
            vert[k, j] = choose(group_one, [jnp.full((ring, lanes), term[k]) for term in terms])

    class Main:
        def __init__(self, l):
            self.t = l + 1
            self.l = l
            self.heat = heat_main

        def terms(self):
            return level_terms(self.l)

        def above(self, ref):
            return ref[self.t + 1]

        def below(self, ref):
            return ref[self.t - 1]

    class Strip:
        def __init__(self, k):
            self.t = strips + k
            self.j = k % per
            self.base = strips + k - self.j
            self.heat = heat_side[k // per]

        def terms(self):
            return vert[0, self.j], vert[1, self.j], vert[2, self.j]

        def above(self, ref):
            if self.j < per - 1:
                return ref[self.t + 1]
            return turn(ref[self.base], -GROUP)

        def below(self, ref):
            if self.j > 0:
                return ref[self.t - 1]
            return turn(ref[self.base + per - 1], GROUP)

    def each_main(body):
        def step(l, carry):
            body(Main(l))
            return carry

        lax.fori_loop(0, levels, step, 0, unroll=True)

    def each_strip(side, body):
        for j in range(per):
            body(Strip(per * side + j))

    def off_forward(c, ref, extra=None):
        up, down, _ = c.terms()
        v = ref[c.t]
        above = turn(v, -1, 0)
        below = turn(v, 1, 0)
        if extra is not None:
            more = jnp.concatenate([extra[c.t], extra[c.t]], axis=0)
            above = jnp.where(row_ring == rows + wide - 1, more, above)
            below = jnp.where(row_ring == rows + wide, more, below)
        off = (
            turn(v, -1) * coef[1, c.t]
            - turn(v, 1) * coef[2, c.t]
            + above * coef[5, c.t]
            - below * coef[6, c.t]
            - up * c.above(ref)
            - down * c.below(ref)
        )
        return v, off

    def off_adjoint(c, ref):
        up, down, _ = c.terms()
        v = ref[c.t]
        off = (
            turn(v, 1) * coef[3, c.t]
            - turn(v, -1) * coef[0, c.t]
            + turn(v, 1, 0) * coef[7, c.t]
            - turn(v, -1, 0) * coef[4, c.t]
            - up * c.above(ref)
            - down * c.below(ref)
        )
        return v, off

    def resid_forward(c, ref, extra=None):
        _, _, damp = c.terms()
        x, off = off_forward(c, ref, extra)
        t = jnp.tanh(x)
        local = damp * (1.0 - t * t)
        diag = coef[8, c.t]
        r = x * diag + off + damp * t - cf[c.t]
        w = RELAXATION / (coef[9, c.t] + local)
        d = -w * r
        fw[c.t] = w
        fg[c.t] = 1.0 - w * (diag + local)
        fd[c.t] = d
        fa[c.t] = d

    def resid_adjoint(c, ref):
        m, off = off_adjoint(c, ref)
        d = ad[c.t] - (1.0 - ag[c.t]) * m - aw[c.t] * off
        ad2[c.t] = d
        aa[c.t] = d

    def lin_forward(c, src):
        v, off = off_forward(c, src)
        return fg[c.t] * v + fd[c.t] - fw[c.t] * off

    def lin_adjoint(c, src, base):
        v, off = off_adjoint(c, src)
        return ag[c.t] * v + base[c.t] - aw[c.t] * off

    def prepare(c):
        up, down, damp = c.terms()
        de = raw[ED, c.t]
        fe = 0.5 * raw[EW, c.t]
        dn = jnp.where(open_face, raw[ND, c.t], 0.0)
        fn = jnp.where(open_face, 0.5 * raw[NW, c.t], 0.0)
        dnx = rawx[0, c.t]
        fnx = 0.5 * rawx[1, c.t]
        anx, bnx = fnx + dnx, fnx - dnx
        a, b = fe + de, fe - de
        an, bn = fn + dn, fn - dn
        a_w = turn(a, 1)
        b_w = turn(b, 1)
        last = row_ring == rows + wide
        an_s = jnp.where(last, jnp.concatenate([anx, anx], axis=0), turn(an, 1, 0))
        bn_s = jnp.where(last, jnp.concatenate([bnx, bnx], axis=0), turn(bn, 1, 0))
        diag = 1.0 + (a - b_w) + (an - bn_s) + (up + down)
        total = 1.0 + de + 0.5 * (a_w - b_w) + dn + 0.5 * (an_s - bn_s) + (up + down)
        for k, value in enumerate((a, b, a_w, b_w, an, bn, an_s, bn_s, diag, total)):
            coef[k, c.t] = value
        cf[c.t] = raw[CKPT, c.t] + raw[SOURCE, c.t] * c.heat
        t = jnp.tanh(raw[TRAJ, c.t])
        local = damp * (1.0 - t * t)
        w = RELAXATION / (total + local)
        start_delta = w * raw[ADJF, c.t]
        aw[c.t] = w
        ag[c.t] = 1.0 - w * (diag + local)
        ad[c.t] = start_delta
        aa[c.t] = start_delta
        resid_forward(c, raw.at[CKPT])

    pairs = ((fa, fb, aa, ab), (fb, fa, ab, aa))
    last = pairs[(INNER - 2) % 2]

    def sweeps(each, base):
        for k in range(INNER - 2):
            f_src, f_dst, a_src, a_dst = pairs[k % 2]

            def body(c):
                f_dst[c.t] = lin_forward(c, f_src)
                a_dst[c.t] = lin_adjoint(c, a_src, base)

            each(body)

    def close1(c):
        xm[0, c.t, :rows, :] = raw[CKPT, c.t, :rows, :] + lin_forward(c, last[0])[:rows]
        xm[1, c.t, :rows, :] = lin_adjoint(c, last[2], ad)[:rows]

    def second(c):
        resid_forward(c, xm.at[0], x1x)
        resid_adjoint(c, xm.at[1])

    def close2(c):
        x2[c.t] = xm[0, c.t] + lin_forward(c, last[0])
        mu2[c.t] = xm[1, c.t, :rows, :] + lin_adjoint(c, last[2], ad2)[:rows]

    def finish(c):
        _, _, damp = c.terms()
        x, off = off_forward(c, x2)
        r = x * coef[8, c.t] + off + damp * jnp.tanh(x) - cf[c.t]
        res[c.t] = r[:rows]

    @pl.when(first_x)
    def _():
        known(1, 1, 5, 7)
        start_lon(lon_w)

    arrive(0, up0, down0)
    each_main(prepare)
    sweeps(each_main, ad)
    each_main(close1)
    start_up(one_main[0])
    start_down(one_main[1])

    spot = lane_ring % GROUP
    from_w = (spot > 0) & (spot < halo)
    from_e = (spot >= kept) & (spot < GROUP - 1)
    spot_row = spot[:rows]
    for f in range(FIELDS):
        for side in range(2):
            for j in range(per):
                raw[f, strips + per * side + j, rows:, :] = gather(
                    lambda l: raw[f, l + 1, rows:, :], group_row, side, j
                )
    for k in range(2):
        for side in range(2):
            for j in range(per):
                rawx[k, strips + per * side + j] = gather(lambda l: rawx[k, l + 1], group_row, side, j)
    def unpack(side):
        recv, where, lead, nines = ((recv_w, from_w, 1, NINTH), (recv_e, from_e, kept, (CKPT,)))[side]
        beyond = spot == (0 if side == 0 else GROUP - 1)
        for j in range(per):
            t = strips + per * side + j
            shift = lead - SLOT * j
            for f in range(FIELDS):
                tile = jnp.where(where, turn(recv[f], shift), raw[f, t])
                if f in nines:
                    tile = jnp.where(beyond, turn(recv[FIELDS], shift + nines.index(f)), tile)
                raw[f, t] = tile

    for side, k, copies in ((1, 2, lon_w), (0, 1, lon_e)):
        arrive_lon(k, copies)
        unpack(side)
        each = functools.partial(each_strip, side)
        each(prepare)
        sweeps(each, ad)
        each(close1)
        start_up(one_strips[side][0])
        start_down(one_strips[side][1])

    arrive(3, *one_main)
    each_main(second)
    sweeps(each_main, ad2)
    each_main(close2)
    each_main(finish)

    east_edge = lane_row >= lanes - DEPTH

    def merge_east():
        for ref, out in ((x2, state_out), (mu2, adj_out), (res, resid_out)):
            for l in range(levels):
                j, g = l % per, l // per
                e = turn(ref[strips + per + j][:rows], lanes - kept - GROUP * g)
                out[l] = jnp.where(east_edge, e, ref[l + 1][:rows])

    for side in (1, 0):
        arrive(4 + side, *one_strips[side])
        each = functools.partial(each_strip, side)
        each(second)
        sweeps(each, ad2)
        each(close2)
        each(finish)
        if side == 1:
            merge_east()
            wait_rows(2 * levels * rows, load_sem.at[1])

    west_edge = lane_row < DEPTH

    def west_merged(ref, l, here):
        j, g = l % per, l // per
        return jnp.where(west_edge, turn(ref[strips + j][:rows], -(GROUP * g + halo)), here)

    for l in range(levels):
        x = west_merged(x2, l, state_out[l])
        state_out[l] = x
        adj_out[l] = west_merged(mu2, l, adj_out[l]) + late_ref[1, l] * (x - late_ref[0, l])
        resid_out[l] = west_merged(res, l, resid_out[l])

    flush()


def hand_over(a, b, c, x, y, z, sem):
    gives = [
        pltpu.make_async_copy(held, ref, sem.at[k])
        for k, (held, ref) in enumerate(((a, x), (b, y), (c, z)))
    ]
    for copy in gives:
        copy.start()
    for copy in gives:
        copy.wait()


def solution(mesh):
    nx, ny = mesh.shape["gx"], mesh.shape["gy"]

    def per_device(*arrays):
        levels, rows, lanes = arrays[0].shape
        groups = lanes // GROUP
        assert rows >= 2 * INNER and rows >= INNER + 1 and levels % groups == 0 and nx > 2
        per = levels // groups
        assert per * SLOT <= GROUP and GROUP >= 3 * DEPTH and len(NINTH) <= SLOT
        ring = 2 * rows
        tiles = levels + 2 + 2 * per
        f32 = jnp.float32
        out = jax.ShapeDtypeStruct((levels, rows, lanes), f32)
        hbm = pl.BlockSpec(memory_space=pltpu.HBM)
        vmem = pl.BlockSpec(memory_space=pltpu.VMEM)

        def buf(*shape):
            return pltpu.VMEM(shape, f32)

        def full():
            return buf(tiles, ring, lanes)

        def dma(n):
            return pltpu.SemaphoreType.DMA((n,))

        results = pl.pallas_call(
            functools.partial(kernel, nx, ny),
            name="step_pair",
            out_shape=(pltpu.VMEM(out.shape, f32),) * 3,
            in_specs=[hbm] * 13,
            out_specs=(vmem,) * 3,
            scratch_shapes=[
                buf(FIELDS, tiles, ring, lanes),
                buf(2, tiles, rows, lanes),
                buf(FIELDS + 1, rows, lanes),
                buf(FIELDS + 1, rows, lanes),
                buf(FIELDS + 1, ring, lanes),
                buf(FIELDS + 1, ring, lanes),
                buf(10, tiles, ring, lanes),
                full(),
                buf(2, tiles, ring, lanes),
                buf(tiles, rows, lanes),
                full(),
                buf(tiles, rows, lanes),
                buf(tiles, rows, lanes),
            ]
            + [full() for _ in range(11)]
            + [
                buf(3, per, ring, lanes),
                buf(2, levels, rows, lanes),
                buf(2 * FIELDS * levels * rows, lanes),
                pltpu.SMEM((levels,), f32),
                pltpu.SMEM((levels,), f32),
                pltpu.SMEM((1,), jnp.int32),
                dma(5),
                dma(1),
                dma(6),
                pltpu.SemaphoreType.REGULAR((4,)),
            ],
            compiler_params=pltpu.CompilerParams(
                collective_id=0, has_side_effects=True, vmem_limit_bytes=67043328 - 3 * 4 * math.prod(out.shape)
            ),
        )(*arrays)
        return pl.pallas_call(
            hand_over,
            name="hand_over",
            out_shape=(out, out, out),
            in_specs=[vmem] * 3,
            out_specs=(hbm, hbm, hbm),
            scratch_shapes=[dma(3)],
            compiler_params=pltpu.CompilerParams(vmem_limit_bytes=4 * 2**20),
        )(*results)

    block = P(None, "gy", "gx")
    return jax.shard_map(
        per_device,
        mesh=mesh,
        in_specs=(block,) * 7 + (P(), P(), block, block, block, P()),
        out_specs=(block,) * 3,
        check_vma=False,
    )
```

```python
import functools
import math

import jax
import jax.numpy as jnp
from jax import lax
from jax.experimental import pallas as pl
from jax.experimental.pallas import tpu as pltpu
from jax.sharding import PartitionSpec as P

OUTER = 2
INNER = 4
DAY_STEPS = 96
RELAXATION = 0.7

FIELDS = 8
ND, NW, CKPT, ED, EW, SOURCE, TRAJ, ADJF = range(FIELDS)
FORWARD = 6
CORNER = 5

DEPTH = OUTER * INNER + 1
SLOT = DEPTH - 1
GROUP = 32
NINTH = (CKPT, ED, EW)

MESH = pl.DeviceIdType.MESH


def kernel(
    nx,
    ny,
    ckpt_h,
    traj_h,
    adjf_h,
    ed_h,
    nd_h,
    ew_h,
    nw_h,
    level_h,
    damp_h,
    source_h,
    obs_h,
    weight_h,
    step_h,
    state_out,
    resid_out,
    adj_out,
    raw,
    rawx,
    pack_e,
    pack_w,
    recv_e,
    recv_w,
    coef,
    cf,
    xm,
    x1x,
    x2,
    mu2,
    res,
    fw,
    fg,
    fd,
    fa,
    fb,
    aw,
    ag,
    ad,
    ad2,
    aa,
    ab,
    vert,
    late_ref,
    bytes_ref,
    level_ref,
    damp_ref,
    step_ref,
    load_sem,
    send,
    got,
    hello,
):
    levels, rows, lanes = state_out.shape
    wide = INNER
    ring = 2 * rows
    groups = lanes // GROUP
    per = levels // groups
    strips = levels + 2
    tiles = strips + 2 * per
    halo = DEPTH
    kept = GROUP - halo
    gx = lax.axis_index("gx")
    gy = lax.axis_index("gy")
    east = lax.rem(gx + 1, nx)
    west = lax.rem(gx + nx - 1, nx)
    has_n = gy < ny - 1
    has_s = gy > 0
    north = gy + 1
    south = gy - 1
    first_x = gx == 0
    last_x = gx == nx - 1

    inside = pl.ds(1, levels)
    main = pl.ds(0, rows)

    order = (nd_h, nw_h, ckpt_h, ed_h, ew_h, source_h, traj_h, adjf_h)
    loads = [
        pltpu.make_async_copy(h, raw.at[f, inside, main, :], load_sem.at[0])
        for f, h in enumerate(order)
    ]
    late_loads = [
        pltpu.make_async_copy(obs_h, late_ref.at[0], load_sem.at[1]),
        pltpu.make_async_copy(weight_h, late_ref.at[1], load_sem.at[1]),
    ]
    scalar_loads = [
        pltpu.make_async_copy(level_h, level_ref, load_sem.at[2]),
        pltpu.make_async_copy(damp_h, damp_ref, load_sem.at[3]),
        pltpu.make_async_copy(step_h, step_ref, load_sem.at[4]),
    ]

    for copy in loads:
        copy.start()

    barrier = pltpu.get_barrier_semaphore()
    odd_x = lax.rem(gx, 2) == 1
    odd_y = lax.rem(gy, 2) == 1
    even_y = jnp.logical_not(odd_y)
    inner_x = jnp.logical_not(first_x)
    before_e = jnp.logical_or(last_x, odd_x)
    before_w = jnp.logical_and(inner_x, odd_x)
    before_de = jnp.logical_or(last_x, even_y)
    before_dw = jnp.logical_and(inner_x, even_y)
    neighbours = (
        (east, gy, True, before_e),
        (west, gy, True, before_w),
        (gx, north, has_n, odd_y),
        (gx, south, has_s, odd_y),
        (east, north, has_n, before_de),
        (west, north, has_n, before_dw),
        (east, south, has_s, before_de),
        (west, south, has_s, before_dw),
    )
    answer_to = (1, 0, 3, 2, 1, 0, 1, 0)

    behind = 0
    for column, row, there, before in neighbours:
        behind = behind + jnp.logical_and(there, before).astype(jnp.int32)

        @pl.when(jnp.logical_and(there, jnp.logical_not(before)))
        def _():
            pl.semaphore_signal(
                barrier, inc=1, device_id={"gx": column, "gy": row}, device_id_type=MESH
            )


    @pl.when(behind > 0)
    def _():
        pl.semaphore_wait(barrier, behind)

    for k, (column, row, there, before) in enumerate(neighbours):

        @pl.when(jnp.logical_and(there, before))
        def _():
            pl.semaphore_signal(
                hello.at[answer_to[k]], inc=1, device_id={"gx": column, "gy": row}, device_id_type=MESH
            )

    def known(side, *ks):
        count = 0
        for k in ks:
            _, _, there, before = neighbours[k]
            count = count + jnp.logical_and(there, jnp.logical_not(before)).astype(jnp.int32)

        @pl.when(count > 0)
        def _():
            pl.semaphore_wait(hello.at[side], count)

    def wait_rows(n, sem):
        part = bytes_ref.at[pl.ds(0, n), :]
        pltpu.make_async_copy(part, part, sem).wait()

    def rows_of(copies):
        return sum(math.prod(copy.src_ref.shape) for copy in copies) // lanes

    def remote(src, dst, send, got, column, row):
        return pltpu.make_async_remote_copy(
            src_ref=src,
            dst_ref=dst,
            send_sem=send,
            recv_sem=got,
            device_id={"gx": column, "gy": row},
            device_id_type=MESH,
        )

    low = pl.ds(0, wide)
    high = pl.ds(rows - wide, wide)
    from_n = pl.ds(rows, wide)
    from_s = pl.ds(ring - wide, wide)
    next_low = pl.ds(wide, 1)
    next_high = pl.ds(rows - wide - 1, 1)
    near_low = pl.ds(0, wide - 1)
    near_high = pl.ds(rows - wide + 1, wide - 1)
    near_n = pl.ds(rows, wide - 1)
    near_s = pl.ds(ring - wide + 1, wide - 1)
    last_low = pl.ds(wide - 1, 1)
    last_high = pl.ds(rows - wide, 1)
    last_n = pl.ds(rows + wide - 1, 1)
    last_s = pl.ds(ring - wide, 1)
    extra_n = pl.ds(wide - 1, 1)
    extra_s = pl.ds(wide, 1)

    faces = pl.ds(ND, 2)

    def copy(k, src, dst, column, row):
        return remote(src, dst, send.at[0], got.at[k], column, row)

    fwd = pl.ds(0, FORWARD)
    adj = pl.ds(FORWARD, FIELDS - FORWARD)
    up0 = [
        copy(0, raw.at[fwd, inside, high, :], raw.at[fwd, inside, from_s, :], gx, north),
        copy(0, raw.at[faces, inside, next_high, :], rawx.at[:, inside, extra_s, :], gx, north),
    ]
    down0 = [copy(0, raw.at[fwd, inside, low, :], raw.at[fwd, inside, from_n, :], gx, south)]
    up0a = [copy(6, raw.at[adj, inside, near_high, :], raw.at[adj, inside, near_s, :], gx, north)]
    down0a = [copy(6, raw.at[adj, inside, near_low, :], raw.at[adj, inside, near_n, :], gx, south)]

    every = pl.ds(0, FIELDS)
    some = pl.ds(0, CORNER)

    def lon_copies(k, pack, recv, column):
        return (
            [copy(k, pack, recv.at[:, main, :], column, gy)],
            [
                copy(k, pack.at[every, near_high, :], recv.at[every, near_s, :], column, north),
                copy(k, pack.at[some, last_high, :], recv.at[some, last_s, :], column, north),
            ],
            [
                copy(k, pack.at[every, near_low, :], recv.at[every, near_n, :], column, south),
                copy(k, pack.at[some, last_low, :], recv.at[some, last_n, :], column, south),
            ],
        )

    lon_e = lon_copies(1, pack_e, recv_w, east)
    lon_w = lon_copies(2, pack_w, recv_e, west)

    def one(k, part):
        return (
            [
                copy(k, xm.at[:, part, high, :], xm.at[:, part, from_s, :], gx, north),
                copy(k, xm.at[0, part, next_high, :], x1x.at[part, extra_s, :], gx, north),
            ],
            [
                copy(k, xm.at[:, part, low, :], xm.at[:, part, from_n, :], gx, south),
                copy(k, xm.at[0, part, next_low, :], x1x.at[part, extra_n, :], gx, south),
            ],
        )

    one_x = (
        [
            copy(3, xm.at[0, inside, high, :], xm.at[0, inside, from_s, :], gx, north),
            copy(3, xm.at[0, inside, next_high, :], x1x.at[inside, extra_s, :], gx, north),
        ],
        [
            copy(3, xm.at[0, inside, low, :], xm.at[0, inside, from_n, :], gx, south),
            copy(3, xm.at[0, inside, next_low, :], x1x.at[inside, extra_n, :], gx, south),
        ],
    )
    one_m = (
        [copy(7, xm.at[1, inside, high, :], xm.at[1, inside, from_s, :], gx, north)],
        [copy(7, xm.at[1, inside, low, :], xm.at[1, inside, from_n, :], gx, south)],
    )
    one_strips = (one(4, pl.ds(strips, per)), one(5, pl.ds(strips + per, per)))

    def start_up(up):
        @pl.when(has_n)
        def _():
            for copy in up:
                copy.start()

    def start_down(down):
        @pl.when(has_s)
        def _():
            for copy in down:
                copy.start()

    def start_lon(copies):
        copies[0][0].start()
        start_up(copies[1])
        start_down(copies[2])

    def wait_all(always, up, down, with_up, with_down, sem):
        n, n_up, n_down = rows_of(always), rows_of(up), rows_of(down)
        cases = (
            (jnp.logical_and(with_up, with_down), n + n_up + n_down),
            (jnp.logical_and(with_up, jnp.logical_not(with_down)), n + n_up),
            (jnp.logical_and(with_down, jnp.logical_not(with_up)), n + n_down),
            (jnp.logical_not(jnp.logical_or(with_up, with_down)), n),
        )
        for case, total in cases:
            if total:

                @pl.when(case)
                def _():
                    wait_rows(total, sem)

    def arrive(k, up, down):
        wait_all([], up, down, has_s, has_n, got.at[k])

    def arrive_lon(k, copies):
        wait_all(*copies, has_s, has_n, got.at[k])

    def flush():
        exchanges = ((up0, down0), (up0a, down0a), one_x, one_m, *one_strips, lon_e[1:], lon_w[1:])
        wait_all(
            lon_e[0] + lon_w[0],
            [copy for up, _ in exchanges for copy in up],
            [copy for _, down in exchanges for copy in down],
            has_n,
            has_s,
            send.at[0],
        )

    zero_ring = jnp.zeros((ring, lanes), jnp.float32)
    zero_tile = jnp.zeros((rows, lanes), jnp.float32)
    for t in (0, levels + 1):
        raw[CKPT, t] = zero_ring
        for ref in (fa, fb, aa, ab, x2):
            ref[t] = zero_ring
        for k in range(2):
            xm[k, t] = zero_ring

    def clear(part):
        zero = jnp.zeros((wide, lanes), jnp.float32)

        def body(l, carry):
            for f in range(FIELDS):
                raw[f, l + 1, part, :] = zero
            for k in range(2):
                xm[k, l + 1, part, :] = zero
            return carry

        lax.fori_loop(0, levels, body, 0)
        for t in range(strips, tiles):
            for k in range(2):
                xm[k, t, part, :] = zero
        for f in range(FIELDS + 1):
            recv_e[f, part, :] = zero
            recv_w[f, part, :] = zero

    def clear_extra(part):
        zero = jnp.zeros((1, lanes), jnp.float32)
        for t in [*range(1, levels + 1), *range(strips, tiles)]:
            x1x[t, part, :] = zero

    @pl.when(jnp.logical_not(has_n))
    def _():
        clear(from_n)
        clear_extra(extra_n)

    @pl.when(jnp.logical_not(has_s))
    def _():
        clear(from_s)
        clear_extra(extra_s)
        zero = jnp.zeros((1, lanes), jnp.float32)
        for k in range(2):
            for t in range(1, levels + 1):
                rawx[k, t, extra_s, :] = zero

    wait_rows(levels * FIELDS * rows, load_sem.at[0])

    def send_lat():
        known(2, 2)
        start_up(up0 + up0a)
        known(3, 3)
        start_down(down0 + down0a)

    for copy in scalar_loads + late_loads:
        copy.start()

    @pl.when(jnp.logical_not(last_x))
    def _():
        send_lat()


    lane_row = lax.broadcasted_iota(jnp.int32, (rows, lanes), 1)
    lane_ring = lax.broadcasted_iota(jnp.int32, (ring, lanes), 1)
    row_ring = lax.broadcasted_iota(jnp.int32, (ring, lanes), 0)

    def turn(v, shift, axis=1):
        shift = shift % v.shape[axis]
        return pltpu.roll(v, shift, axis) if shift else v

    def choose(place, values):
        out = values[-1]
        for k in range(len(values) - 2, -1, -1):
            out = jnp.where(place == k, values[k], out)
        return out

    def gather(read, place, side, j):
        start = halo if side == 0 else kept
        return choose(place, [turn(read(j + per * g), GROUP * g + start) for g in range(groups)])

    group_row = lane_row // GROUP
    nine_row = lane_row % SLOT

    def slots(f, shift, turns=(0,)):
        rolled = [turn(raw[f, level_of(k) + 1, :rows, :], SLOT * k + shift) for k in range(levels)]
        return [choose((lane_row // SLOT + move) % levels, rolled) for move in turns]

    def level_of(k):
        return k % per + per * (k // per)

    nine = None
    for f in sorted(range(FIELDS), key=lambda f: f not in NINTH):
        if f in NINTH:
            pack_e[f], beside = slots(f, SLOT, (0, 1))
            i = NINTH.index(f)
            beside = turn(beside, -i)
            nine = beside if nine is None else jnp.where(nine_row == SLOT - 1 - i, beside, nine)
        else:
            (pack_e[f],) = slots(f, SLOT)
    pack_e[FIELDS] = nine

    @pl.when(last_x)
    def _():
        start_lon(lon_e)
        send_lat()

    for f in range(FIELDS):
        if f == CKPT:
            pack_w[f], pack_w[FIELDS] = slots(f, 0, (0, -1))
        else:
            (pack_w[f],) = slots(f, 0)

    @pl.when(inner_x)
    def _():
        known(1, 1, 5, 7)
        start_lon(lon_w)

    @pl.when(jnp.logical_not(last_x))
    def _():
        known(0, 0, 4, 6)
        start_lon(lon_e)

    for f in range(FIELDS):
        for side in range(2):
            for j in range(per):
                raw[f, strips + per * side + j, :rows, :] = gather(
                    lambda l: raw[f, l + 1, :rows, :], group_row, side, j
                )

    for copy in scalar_loads:
        copy.wait()

    total_lanes = lanes * nx

    def heat_of(column):
        column = gx * lanes + column
        column = jnp.where(column < 0, column + total_lanes, column)
        column = jnp.where(column >= total_lanes, column - total_lanes, column)
        phase = (
            2.0 * math.pi * column.astype(jnp.float32) / total_lanes
            - 2.0 * math.pi * step_ref[0].astype(jnp.float32) / DAY_STEPS
        )
        return jnp.cos(phase)

    lane_one = lax.broadcasted_iota(jnp.int32, (1, lanes), 1)
    heat_main = heat_of(lane_one)
    heat_side = (
        heat_of(lane_one % GROUP - halo),
        heat_of(lane_one % GROUP + (lanes - kept)),
    )
    row_global = gy * rows + jnp.where(row_ring < rows + wide, row_ring, row_ring - ring)
    open_face = (row_global >= 0) & (row_global < rows * ny - 1)

    def level_terms(l):
        up = jnp.where(l < levels - 1, level_ref[l], 0.0)
        down = jnp.where(l > 0, level_ref[jnp.maximum(l - 1, 0)], 0.0)
        return up, down, damp_ref[l]

    group_one = lane_ring // GROUP
    for j in range(per):
        terms = [level_terms(j + per * g) for g in range(groups)]
        for k in range(3):
            vert[k, j] = choose(group_one, [jnp.full((ring, lanes), term[k]) for term in terms])

    class Main:
        def __init__(self, l):
            self.t = l + 1
            self.l = l
            self.heat = heat_main

        def terms(self):
            return level_terms(self.l)

        def above(self, ref):
            return ref[self.t + 1]

        def below(self, ref):
            return ref[self.t - 1]

    class Strip:
        def __init__(self, k):
            self.t = strips + k
            self.j = k % per
            self.base = strips + k - self.j
            self.heat = heat_side[k // per]

        def terms(self):
            return vert[0, self.j], vert[1, self.j], vert[2, self.j]

        def above(self, ref):
            if self.j < per - 1:
                return ref[self.t + 1]
            return turn(ref[self.base], -GROUP)

        def below(self, ref):
            if self.j > 0:
                return ref[self.t - 1]
            return turn(ref[self.base + per - 1], GROUP)

    def each_main(body):
        def step(l, carry):
            body(Main(l))
            return carry

        lax.fori_loop(0, levels, step, 0, unroll=True)

    def each_strip(side, body):
        for j in range(per):
            body(Strip(per * side + j))

    def off_forward(c, ref, extra=None):
        up, down, _ = c.terms()
        v = ref[c.t]
        above = turn(v, -1, 0)
        below = turn(v, 1, 0)
        if extra is not None:
            more = jnp.concatenate([extra[c.t], extra[c.t]], axis=0)
            above = jnp.where(row_ring == rows + wide - 1, more, above)
            below = jnp.where(row_ring == rows + wide, more, below)
        off = (
            turn(v, -1) * coef[1, c.t]
            - turn(v, 1) * coef[2, c.t]
            + above * coef[5, c.t]
            - below * coef[6, c.t]
            - up * c.above(ref)
            - down * c.below(ref)
        )
        return v, off

    def off_adjoint(c, ref):
        up, down, _ = c.terms()
        v = ref[c.t]
        off = (
            turn(v, 1) * coef[3, c.t]
            - turn(v, -1) * coef[0, c.t]
            + turn(v, 1, 0) * coef[7, c.t]
            - turn(v, -1, 0) * coef[4, c.t]
            - up * c.above(ref)
            - down * c.below(ref)
        )
        return v, off

    def resid_forward(c, ref, extra=None):
        _, _, damp = c.terms()
        x, off = off_forward(c, ref, extra)
        t = jnp.tanh(x)
        local = damp * (1.0 - t * t)
        diag = coef[8, c.t]
        r = x * diag + off + damp * t - cf[c.t]
        w = RELAXATION / (coef[9, c.t] + local)
        d = -w * r
        fw[c.t] = w
        fg[c.t] = 1.0 - w * (diag + local)
        fd[c.t] = d
        fa[c.t] = d

    def resid_adjoint(c, ref):
        m, off = off_adjoint(c, ref)
        d = ad[c.t] - (1.0 - ag[c.t]) * m - aw[c.t] * off
        ad2[c.t] = d
        aa[c.t] = d

    def lin_forward(c, src):
        v, off = off_forward(c, src)
        return fg[c.t] * v + fd[c.t] - fw[c.t] * off

    def lin_adjoint(c, src, base):
        v, off = off_adjoint(c, src)
        return ag[c.t] * v + base[c.t] - aw[c.t] * off

    def prepare(c):
        up, down, damp = c.terms()
        de = raw[ED, c.t]
        fe = 0.5 * raw[EW, c.t]
        dn = jnp.where(open_face, raw[ND, c.t], 0.0)
        fn = jnp.where(open_face, 0.5 * raw[NW, c.t], 0.0)
        dnx = rawx[0, c.t]
        fnx = 0.5 * rawx[1, c.t]
        anx, bnx = fnx + dnx, fnx - dnx
        a, b = fe + de, fe - de
        an, bn = fn + dn, fn - dn
        a_w = turn(a, 1)
        b_w = turn(b, 1)
        last = row_ring == rows + wide
        an_s = jnp.where(last, jnp.concatenate([anx, anx], axis=0), turn(an, 1, 0))
        bn_s = jnp.where(last, jnp.concatenate([bnx, bnx], axis=0), turn(bn, 1, 0))
        diag = 1.0 + (a - b_w) + (an - bn_s) + (up + down)
        total = 1.0 + de + 0.5 * (a_w - b_w) + dn + 0.5 * (an_s - bn_s) + (up + down)
        for k, value in enumerate((a, b, a_w, b_w, an, bn, an_s, bn_s, diag, total)):
            coef[k, c.t] = value
        cf[c.t] = raw[CKPT, c.t] + raw[SOURCE, c.t] * c.heat
        resid_forward(c, raw.at[CKPT])

    def prepare_adjoint(c):
        _, _, damp = c.terms()
        diag, total = coef[8, c.t], coef[9, c.t]
        t = jnp.tanh(raw[TRAJ, c.t])
        local = damp * (1.0 - t * t)
        w = RELAXATION / (total + local)
        start_delta = w * raw[ADJF, c.t]
        aw[c.t] = w
        ag[c.t] = 1.0 - w * (diag + local)
        ad[c.t] = start_delta
        aa[c.t] = start_delta

    pairs = ((fa, fb, aa, ab), (fb, fa, ab, aa))
    last = pairs[(INNER - 2) % 2]

    def sweeps(each, base):
        for k in range(INNER - 2):
            f_src, f_dst, a_src, a_dst = pairs[k % 2]

            def body(c):
                f_dst[c.t] = lin_forward(c, f_src)
                a_dst[c.t] = lin_adjoint(c, a_src, base)

            each(body)

    def close_x(c):
        xm[0, c.t, :rows, :] = raw[CKPT, c.t, :rows, :] + lin_forward(c, last[0])[:rows]

    def close_m(c):
        xm[1, c.t, :rows, :] = lin_adjoint(c, last[2], ad)[:rows]

    def second_x(c):
        resid_forward(c, xm.at[0], x1x)

    def second_m(c):
        resid_adjoint(c, xm.at[1])

    def both(first, then):
        def body(c):
            first(c)
            then(c)

        return body

    def close2(c):
        x2[c.t] = xm[0, c.t] + lin_forward(c, last[0])
        mu2[c.t] = xm[1, c.t, :rows, :] + lin_adjoint(c, last[2], ad2)[:rows]

    def finish(c):
        _, _, damp = c.terms()
        x, off = off_forward(c, x2)
        r = x * coef[8, c.t] + off + damp * jnp.tanh(x) - cf[c.t]
        res[c.t] = r[:rows]

    @pl.when(first_x)
    def _():
        known(1, 1, 5, 7)
        start_lon(lon_w)

    arrive(0, up0, down0)
    each_main(prepare)
    arrive(6, up0a, down0a)
    each_main(prepare_adjoint)
    sweeps(each_main, ad)
    each_main(close_x)
    start_down(one_x[1])
    start_up(one_x[0])
    each_main(close_m)
    start_down(one_m[1])
    start_up(one_m[0])

    spot = lane_ring % GROUP
    from_w = (spot > 0) & (spot < halo)
    from_e = (spot >= kept) & (spot < GROUP - 1)
    spot_row = spot[:rows]
    for f in range(FIELDS):
        for side in range(2):
            for j in range(per):
                raw[f, strips + per * side + j, rows:, :] = gather(
                    lambda l: raw[f, l + 1, rows:, :], group_row, side, j
                )
    for k in range(2):
        for side in range(2):
            for j in range(per):
                rawx[k, strips + per * side + j] = gather(lambda l: rawx[k, l + 1], group_row, side, j)
    def unpack(side):
        recv, where, lead, nines = ((recv_w, from_w, 1, NINTH), (recv_e, from_e, kept, (CKPT,)))[side]
        beyond = spot == (0 if side == 0 else GROUP - 1)
        for j in range(per):
            t = strips + per * side + j
            shift = lead - SLOT * j
            for f in range(FIELDS):
                tile = jnp.where(where, turn(recv[f], shift), raw[f, t])
                if f in nines:
                    tile = jnp.where(beyond, turn(recv[FIELDS], shift + nines.index(f)), tile)
                raw[f, t] = tile

    for side, k, copies in ((1, 2, lon_w), (0, 1, lon_e)):
        arrive_lon(k, copies)
        unpack(side)
        each = functools.partial(each_strip, side)
        each(both(prepare, prepare_adjoint))
        sweeps(each, ad)
        each(both(close_x, close_m))
        start_down(one_strips[side][1])
        start_up(one_strips[side][0])

    arrive(3, *one_x)
    each_main(second_x)
    arrive(7, *one_m)
    each_main(second_m)
    sweeps(each_main, ad2)
    each_main(close2)
    each_main(finish)

    east_edge = lane_row >= lanes - DEPTH

    def merge_east():
        for ref, out in ((x2, state_out), (mu2, adj_out), (res, resid_out)):
            for l in range(levels):
                j, g = l % per, l // per
                e = turn(ref[strips + per + j][:rows], lanes - kept - GROUP * g)
                out[l] = jnp.where(east_edge, e, ref[l + 1][:rows])

    for side in (1, 0):
        arrive(4 + side, *one_strips[side])
        each = functools.partial(each_strip, side)
        each(both(second_x, second_m))
        sweeps(each, ad2)
        each(close2)
        each(finish)
        if side == 1:
            merge_east()
            wait_rows(2 * levels * rows, load_sem.at[1])

    west_edge = lane_row < DEPTH

    def west_merged(ref, l, here):
        j, g = l % per, l // per
        return jnp.where(west_edge, turn(ref[strips + j][:rows], -(GROUP * g + halo)), here)

    for l in range(levels):
        x = west_merged(x2, l, state_out[l])
        state_out[l] = x
        adj_out[l] = west_merged(mu2, l, adj_out[l]) + late_ref[1, l] * (x - late_ref[0, l])
        resid_out[l] = west_merged(res, l, resid_out[l])

    flush()


def hand_over(a, b, c, x, y, z, sem):
    gives = [
        pltpu.make_async_copy(held, ref, sem.at[k])
        for k, (held, ref) in enumerate(((a, x), (b, y), (c, z)))
    ]
    for copy in gives:
        copy.start()
    for copy in gives:
        copy.wait()


def solution(mesh):
    nx, ny = mesh.shape["gx"], mesh.shape["gy"]

    def per_device(*arrays):
        levels, rows, lanes = arrays[0].shape
        groups = lanes // GROUP
        assert rows >= 2 * INNER and rows >= INNER + 1 and levels % groups == 0 and nx > 2
        per = levels // groups
        assert per * SLOT <= GROUP and GROUP >= 3 * DEPTH and len(NINTH) <= SLOT
        ring = 2 * rows
        tiles = levels + 2 + 2 * per
        f32 = jnp.float32
        out = jax.ShapeDtypeStruct((levels, rows, lanes), f32)
        hbm = pl.BlockSpec(memory_space=pltpu.HBM)
        vmem = pl.BlockSpec(memory_space=pltpu.VMEM)

        def buf(*shape):
            return pltpu.VMEM(shape, f32)

        def full():
            return buf(tiles, ring, lanes)

        def dma(n):
            return pltpu.SemaphoreType.DMA((n,))

        results = pl.pallas_call(
            functools.partial(kernel, nx, ny),
            name="step_pair",
            out_shape=(pltpu.VMEM(out.shape, f32),) * 3,
            in_specs=[hbm] * 13,
            out_specs=(vmem,) * 3,
            scratch_shapes=[
                buf(FIELDS, tiles, ring, lanes),
                buf(2, tiles, rows, lanes),
                buf(FIELDS + 1, rows, lanes),
                buf(FIELDS + 1, rows, lanes),
                buf(FIELDS + 1, ring, lanes),
                buf(FIELDS + 1, ring, lanes),
                buf(10, tiles, ring, lanes),
                full(),
                buf(2, tiles, ring, lanes),
                buf(tiles, rows, lanes),
                full(),
                buf(tiles, rows, lanes),
                buf(tiles, rows, lanes),
            ]
            + [full() for _ in range(11)]
            + [
                buf(3, per, ring, lanes),
                buf(2, levels, rows, lanes),
                buf(2 * FIELDS * levels * rows, lanes),
                pltpu.SMEM((levels,), f32),
                pltpu.SMEM((levels,), f32),
                pltpu.SMEM((1,), jnp.int32),
                dma(5),
                dma(1),
                dma(8),
                pltpu.SemaphoreType.REGULAR((4,)),
            ],
            compiler_params=pltpu.CompilerParams(
                collective_id=0, has_side_effects=True, vmem_limit_bytes=67043328 - 3 * 4 * math.prod(out.shape)
            ),
        )(*arrays)
        return pl.pallas_call(
            hand_over,
            name="hand_over",
            out_shape=(out, out, out),
            in_specs=[vmem] * 3,
            out_specs=(hbm, hbm, hbm),
            scratch_shapes=[dma(3)],
            compiler_params=pltpu.CompilerParams(vmem_limit_bytes=4 * 2**20),
        )(*results)

    block = P(None, "gy", "gx")
    return jax.shard_map(
        per_device,
        mesh=mesh,
        in_specs=(block,) * 7 + (P(), P(), block, block, block, P()),
        out_specs=(block,) * 3,
        check_vma=False,
    )
```

```python
import functools
import math

import jax
import jax.numpy as jnp
from jax import lax
from jax.experimental import pallas as pl
from jax.experimental.pallas import tpu as pltpu
from jax.sharding import PartitionSpec as P

OUTER = 2
INNER = 4
DAY_STEPS = 96
RELAXATION = 0.7

FIELDS = 8
ND, NW, CKPT, ED, EW, SOURCE, TRAJ, ADJF = range(FIELDS)
FORWARD = 6
CORNER = 5

DEPTH = OUTER * INNER + 1
SLOT = DEPTH - 1
GROUP = 32
NINTH = (CKPT, ED, EW)

MESH = pl.DeviceIdType.MESH


def kernel(
    nx,
    ny,
    ckpt_h,
    traj_h,
    adjf_h,
    ed_h,
    nd_h,
    ew_h,
    nw_h,
    level_h,
    damp_h,
    source_h,
    obs_h,
    weight_h,
    step_h,
    state_out,
    resid_out,
    adj_out,
    raw,
    rawx,
    pack_e,
    pack_w,
    recv_e,
    recv_w,
    coef,
    cf,
    xm,
    x1x,
    x2,
    mu2,
    res,
    fw,
    fg,
    fd,
    fa,
    fb,
    aw,
    ag,
    ad,
    ad2,
    aa,
    ab,
    vert,
    late_ref,
    bytes_ref,
    level_ref,
    damp_ref,
    step_ref,
    load_sem,
    send,
    got,
    hello,
):
    levels, rows, lanes = state_out.shape
    wide = INNER
    ring = 2 * rows
    groups = lanes // GROUP
    per = levels // groups
    strips = levels + 2
    tiles = strips + 2 * per
    halo = DEPTH
    kept = GROUP - halo
    gx = lax.axis_index("gx")
    gy = lax.axis_index("gy")
    east = lax.rem(gx + 1, nx)
    west = lax.rem(gx + nx - 1, nx)
    has_n = gy < ny - 1
    has_s = gy > 0
    north = gy + 1
    south = gy - 1
    first_x = gx == 0
    last_x = gx == nx - 1

    inside = pl.ds(1, levels)
    main = pl.ds(0, rows)

    order = (nd_h, nw_h, ckpt_h, ed_h, ew_h, source_h, traj_h, adjf_h)
    loads = [
        pltpu.make_async_copy(h, raw.at[f, inside, main, :], load_sem.at[0])
        for f, h in enumerate(order)
    ]
    late_loads = [
        pltpu.make_async_copy(obs_h, late_ref.at[0], load_sem.at[1]),
        pltpu.make_async_copy(weight_h, late_ref.at[1], load_sem.at[1]),
    ]
    scalar_loads = [
        pltpu.make_async_copy(level_h, level_ref, load_sem.at[2]),
        pltpu.make_async_copy(damp_h, damp_ref, load_sem.at[3]),
        pltpu.make_async_copy(step_h, step_ref, load_sem.at[4]),
    ]

    for copy in loads:
        copy.start()

    barrier = pltpu.get_barrier_semaphore()
    odd_x = lax.rem(gx, 2) == 1
    odd_y = lax.rem(gy, 2) == 1
    even_y = jnp.logical_not(odd_y)
    inner_x = jnp.logical_not(first_x)
    before_lat = odd_y != last_x
    before_e = jnp.logical_or(last_x, odd_x)
    before_w = jnp.logical_and(inner_x, odd_x)
    before_de = jnp.logical_or(last_x, even_y)
    before_dw = jnp.logical_and(inner_x, even_y)
    neighbours = (
        (east, gy, True, before_e),
        (west, gy, True, before_w),
        (gx, north, has_n, before_lat),
        (gx, south, has_s, before_lat),
        (east, north, has_n, before_de),
        (west, north, has_n, before_dw),
        (east, south, has_s, before_de),
        (west, south, has_s, before_dw),
    )
    answer_to = (1, 0, 3, 2, 1, 0, 1, 0)

    behind = 0
    for column, row, there, before in neighbours:
        behind = behind + jnp.logical_and(there, before).astype(jnp.int32)

        @pl.when(jnp.logical_and(there, jnp.logical_not(before)))
        def _():
            pl.semaphore_signal(
                barrier, inc=1, device_id={"gx": column, "gy": row}, device_id_type=MESH
            )


    @pl.when(behind > 0)
    def _():
        pl.semaphore_wait(barrier, behind)

    for k, (column, row, there, before) in enumerate(neighbours):

        @pl.when(jnp.logical_and(there, before))
        def _():
            pl.semaphore_signal(
                hello.at[answer_to[k]], inc=1, device_id={"gx": column, "gy": row}, device_id_type=MESH
            )

    def known(side, *ks):
        count = 0
        for k in ks:
            _, _, there, before = neighbours[k]
            count = count + jnp.logical_and(there, jnp.logical_not(before)).astype(jnp.int32)

        @pl.when(count > 0)
        def _():
            pl.semaphore_wait(hello.at[side], count)

    def wait_rows(n, sem):
        part = bytes_ref.at[pl.ds(0, n), :]
        pltpu.make_async_copy(part, part, sem).wait()

    def rows_of(copies):
        return sum(math.prod(copy.src_ref.shape) for copy in copies) // lanes

    def remote(src, dst, send, got, column, row):
        return pltpu.make_async_remote_copy(
            src_ref=src,
            dst_ref=dst,
            send_sem=send,
            recv_sem=got,
            device_id={"gx": column, "gy": row},
            device_id_type=MESH,
        )

    low = pl.ds(0, wide)
    high = pl.ds(rows - wide, wide)
    from_n = pl.ds(rows, wide)
    from_s = pl.ds(ring - wide, wide)
    next_low = pl.ds(wide, 1)
    next_high = pl.ds(rows - wide - 1, 1)
    near_low = pl.ds(0, wide - 1)
    near_high = pl.ds(rows - wide + 1, wide - 1)
    near_n = pl.ds(rows, wide - 1)
    near_s = pl.ds(ring - wide + 1, wide - 1)
    last_low = pl.ds(wide - 1, 1)
    last_high = pl.ds(rows - wide, 1)
    last_n = pl.ds(rows + wide - 1, 1)
    last_s = pl.ds(ring - wide, 1)
    extra_n = pl.ds(wide - 1, 1)
    extra_s = pl.ds(wide, 1)

    faces = pl.ds(ND, 2)

    def copy(k, src, dst, column, row):
        return remote(src, dst, send.at[0], got.at[k], column, row)

    fwd = pl.ds(0, FORWARD)
    adj = pl.ds(FORWARD, FIELDS - FORWARD)
    up0 = [
        copy(0, raw.at[fwd, inside, high, :], raw.at[fwd, inside, from_s, :], gx, north),
        copy(0, raw.at[faces, inside, next_high, :], rawx.at[:, inside, extra_s, :], gx, north),
    ]
    down0 = [copy(0, raw.at[fwd, inside, low, :], raw.at[fwd, inside, from_n, :], gx, south)]
    up0a = [copy(6, raw.at[adj, inside, near_high, :], raw.at[adj, inside, near_s, :], gx, north)]
    down0a = [copy(6, raw.at[adj, inside, near_low, :], raw.at[adj, inside, near_n, :], gx, south)]

    every = pl.ds(0, FIELDS)
    some = pl.ds(0, CORNER)

    def lon_copies(k, pack, recv, column):
        return (
            [copy(k, pack, recv.at[:, main, :], column, gy)],
            [
                copy(k, pack.at[every, near_high, :], recv.at[every, near_s, :], column, north),
                copy(k, pack.at[some, last_high, :], recv.at[some, last_s, :], column, north),
            ],
            [
                copy(k, pack.at[every, near_low, :], recv.at[every, near_n, :], column, south),
                copy(k, pack.at[some, last_low, :], recv.at[some, last_n, :], column, south),
            ],
        )

    lon_e = lon_copies(1, pack_e, recv_w, east)
    lon_w = lon_copies(2, pack_w, recv_e, west)

    def one(k, part):
        return (
            [
                copy(k, xm.at[:, part, high, :], xm.at[:, part, from_s, :], gx, north),
                copy(k, xm.at[0, part, next_high, :], x1x.at[part, extra_s, :], gx, north),
            ],
            [
                copy(k, xm.at[:, part, low, :], xm.at[:, part, from_n, :], gx, south),
                copy(k, xm.at[0, part, next_low, :], x1x.at[part, extra_n, :], gx, south),
            ],
        )

    one_x = (
        [
            copy(3, xm.at[0, inside, high, :], xm.at[0, inside, from_s, :], gx, north),
            copy(3, xm.at[0, inside, next_high, :], x1x.at[inside, extra_s, :], gx, north),
        ],
        [
            copy(3, xm.at[0, inside, low, :], xm.at[0, inside, from_n, :], gx, south),
            copy(3, xm.at[0, inside, next_low, :], x1x.at[inside, extra_n, :], gx, south),
        ],
    )
    one_m = (
        [copy(7, xm.at[1, inside, high, :], xm.at[1, inside, from_s, :], gx, north)],
        [copy(7, xm.at[1, inside, low, :], xm.at[1, inside, from_n, :], gx, south)],
    )
    one_strips = (one(4, pl.ds(strips, per)), one(5, pl.ds(strips + per, per)))

    def start_up(up):
        @pl.when(has_n)
        def _():
            for copy in up:
                copy.start()

    def start_down(down):
        @pl.when(has_s)
        def _():
            for copy in down:
                copy.start()

    def start_lon(copies):
        copies[0][0].start()
        start_up(copies[1])
        start_down(copies[2])

    def wait_all(always, up, down, with_up, with_down, sem):
        n, n_up, n_down = rows_of(always), rows_of(up), rows_of(down)
        cases = (
            (jnp.logical_and(with_up, with_down), n + n_up + n_down),
            (jnp.logical_and(with_up, jnp.logical_not(with_down)), n + n_up),
            (jnp.logical_and(with_down, jnp.logical_not(with_up)), n + n_down),
            (jnp.logical_not(jnp.logical_or(with_up, with_down)), n),
        )
        for case, total in cases:
            if total:

                @pl.when(case)
                def _():
                    wait_rows(total, sem)

    def arrive(k, up, down):
        wait_all([], up, down, has_s, has_n, got.at[k])

    def arrive_lon(k, copies):
        wait_all(*copies, has_s, has_n, got.at[k])

    def flush():
        exchanges = ((up0, down0), (up0a, down0a), one_x, one_m, *one_strips, lon_e[1:], lon_w[1:])
        wait_all(
            lon_e[0] + lon_w[0],
            [copy for up, _ in exchanges for copy in up],
            [copy for _, down in exchanges for copy in down],
            has_n,
            has_s,
            send.at[0],
        )

    zero_ring = jnp.zeros((ring, lanes), jnp.float32)
    zero_tile = jnp.zeros((rows, lanes), jnp.float32)
    for t in (0, levels + 1):
        raw[CKPT, t] = zero_ring
        for ref in (fa, fb, aa, ab, x2):
            ref[t] = zero_ring
        for k in range(2):
            xm[k, t] = zero_ring

    def clear(part):
        zero = jnp.zeros((wide, lanes), jnp.float32)

        def body(l, carry):
            for f in range(FIELDS):
                raw[f, l + 1, part, :] = zero
            for k in range(2):
                xm[k, l + 1, part, :] = zero
            return carry

        lax.fori_loop(0, levels, body, 0)
        for t in range(strips, tiles):
            for k in range(2):
                xm[k, t, part, :] = zero
        for f in range(FIELDS + 1):
            recv_e[f, part, :] = zero
            recv_w[f, part, :] = zero

    def clear_extra(part):
        zero = jnp.zeros((1, lanes), jnp.float32)
        for t in [*range(1, levels + 1), *range(strips, tiles)]:
            x1x[t, part, :] = zero

    @pl.when(jnp.logical_not(has_n))
    def _():
        clear(from_n)
        clear_extra(extra_n)

    @pl.when(jnp.logical_not(has_s))
    def _():
        clear(from_s)
        clear_extra(extra_s)
        zero = jnp.zeros((1, lanes), jnp.float32)
        for k in range(2):
            for t in range(1, levels + 1):
                rawx[k, t, extra_s, :] = zero

    wait_rows(levels * FIELDS * rows, load_sem.at[0])

    def send_lat():
        known(2, 2)
        start_up(up0 + up0a)
        known(3, 3)
        start_down(down0 + down0a)

    for copy in scalar_loads + late_loads:
        copy.start()

    @pl.when(jnp.logical_not(last_x))
    def _():
        send_lat()


    lane_row = lax.broadcasted_iota(jnp.int32, (rows, lanes), 1)
    lane_ring = lax.broadcasted_iota(jnp.int32, (ring, lanes), 1)
    row_ring = lax.broadcasted_iota(jnp.int32, (ring, lanes), 0)

    def turn(v, shift, axis=1):
        shift = shift % v.shape[axis]
        return pltpu.roll(v, shift, axis) if shift else v

    def choose(place, values):
        out = values[-1]
        for k in range(len(values) - 2, -1, -1):
            out = jnp.where(place == k, values[k], out)
        return out

    def gather(read, place, side, j):
        start = halo if side == 0 else kept
        return choose(place, [turn(read(j + per * g), GROUP * g + start) for g in range(groups)])

    group_row = lane_row // GROUP
    nine_row = lane_row % SLOT

    def slots(f, shift, turns=(0,)):
        rolled = [turn(raw[f, level_of(k) + 1, :rows, :], SLOT * k + shift) for k in range(levels)]
        return [choose((lane_row // SLOT + move) % levels, rolled) for move in turns]

    def level_of(k):
        return k % per + per * (k // per)

    nine = None
    for f in sorted(range(FIELDS), key=lambda f: f not in NINTH):
        if f in NINTH:
            pack_e[f], beside = slots(f, SLOT, (0, 1))
            i = NINTH.index(f)
            beside = turn(beside, -i)
            nine = beside if nine is None else jnp.where(nine_row == SLOT - 1 - i, beside, nine)
        else:
            (pack_e[f],) = slots(f, SLOT)
    pack_e[FIELDS] = nine

    @pl.when(last_x)
    def _():
        start_lon(lon_e)
        send_lat()

    for f in range(FIELDS):
        if f == CKPT:
            pack_w[f], pack_w[FIELDS] = slots(f, 0, (0, -1))
        else:
            (pack_w[f],) = slots(f, 0)

    @pl.when(inner_x)
    def _():
        known(1, 1, 5, 7)
        start_lon(lon_w)

    @pl.when(jnp.logical_not(last_x))
    def _():
        known(0, 0, 4, 6)
        start_lon(lon_e)

    for f in range(FIELDS):
        for side in range(2):
            for j in range(per):
                raw[f, strips + per * side + j, :rows, :] = gather(
                    lambda l: raw[f, l + 1, :rows, :], group_row, side, j
                )

    for copy in scalar_loads:
        copy.wait()

    total_lanes = lanes * nx

    def heat_of(column):
        column = gx * lanes + column
        column = jnp.where(column < 0, column + total_lanes, column)
        column = jnp.where(column >= total_lanes, column - total_lanes, column)
        phase = (
            2.0 * math.pi * column.astype(jnp.float32) / total_lanes
            - 2.0 * math.pi * step_ref[0].astype(jnp.float32) / DAY_STEPS
        )
        return jnp.cos(phase)

    lane_one = lax.broadcasted_iota(jnp.int32, (1, lanes), 1)
    heat_main = heat_of(lane_one)
    heat_side = (
        heat_of(lane_one % GROUP - halo),
        heat_of(lane_one % GROUP + (lanes - kept)),
    )
    row_global = gy * rows + jnp.where(row_ring < rows + wide, row_ring, row_ring - ring)
    open_face = (row_global >= 0) & (row_global < rows * ny - 1)

    def level_terms(l):
        up = jnp.where(l < levels - 1, level_ref[l], 0.0)
        down = jnp.where(l > 0, level_ref[jnp.maximum(l - 1, 0)], 0.0)
        return up, down, damp_ref[l]

    group_one = lane_ring // GROUP
    for j in range(per):
        terms = [level_terms(j + per * g) for g in range(groups)]
        for k in range(3):
            vert[k, j] = choose(group_one, [jnp.full((ring, lanes), term[k]) for term in terms])

    class Main:
        def __init__(self, l):
            self.t = l + 1
            self.l = l
            self.heat = heat_main

        def terms(self):
            return level_terms(self.l)

        def above(self, ref):
            return ref[self.t + 1]

        def below(self, ref):
            return ref[self.t - 1]

    class Strip:
        def __init__(self, k):
            self.t = strips + k
            self.j = k % per
            self.base = strips + k - self.j
            self.heat = heat_side[k // per]

        def terms(self):
            return vert[0, self.j], vert[1, self.j], vert[2, self.j]

        def above(self, ref):
            if self.j < per - 1:
                return ref[self.t + 1]
            return turn(ref[self.base], -GROUP)

        def below(self, ref):
            if self.j > 0:
                return ref[self.t - 1]
            return turn(ref[self.base + per - 1], GROUP)

    def each_main(body):
        def step(l, carry):
            body(Main(l))
            return carry

        lax.fori_loop(0, levels, step, 0, unroll=True)

    def each_strip(side, body):
        for j in range(per):
            body(Strip(per * side + j))

    def off_forward(c, ref, extra=None):
        up, down, _ = c.terms()
        v = ref[c.t]
        above = turn(v, -1, 0)
        below = turn(v, 1, 0)
        if extra is not None:
            more = jnp.concatenate([extra[c.t], extra[c.t]], axis=0)
            above = jnp.where(row_ring == rows + wide - 1, more, above)
            below = jnp.where(row_ring == rows + wide, more, below)
        off = (
            turn(v, -1) * coef[1, c.t]
            - turn(v, 1) * coef[2, c.t]
            + above * coef[5, c.t]
            - below * coef[6, c.t]
            - up * c.above(ref)
            - down * c.below(ref)
        )
        return v, off

    def off_adjoint(c, ref):
        up, down, _ = c.terms()
        v = ref[c.t]
        off = (
            turn(v, 1) * coef[3, c.t]
            - turn(v, -1) * coef[0, c.t]
            + turn(v, 1, 0) * coef[7, c.t]
            - turn(v, -1, 0) * coef[4, c.t]
            - up * c.above(ref)
            - down * c.below(ref)
        )
        return v, off

    def resid_forward(c, ref, extra=None):
        _, _, damp = c.terms()
        x, off = off_forward(c, ref, extra)
        t = jnp.tanh(x)
        local = damp * (1.0 - t * t)
        diag = coef[8, c.t]
        r = x * diag + off + damp * t - cf[c.t]
        w = RELAXATION / (coef[9, c.t] + local)
        d = -w * r
        fw[c.t] = w
        fg[c.t] = 1.0 - w * (diag + local)
        fd[c.t] = d
        fa[c.t] = d

    def resid_adjoint(c, ref):
        m, off = off_adjoint(c, ref)
        d = ad[c.t] - (1.0 - ag[c.t]) * m - aw[c.t] * off
        ad2[c.t] = d
        aa[c.t] = d

    def lin_forward(c, src):
        v, off = off_forward(c, src)
        return fg[c.t] * v + fd[c.t] - fw[c.t] * off

    def lin_adjoint(c, src, base):
        v, off = off_adjoint(c, src)
        return ag[c.t] * v + base[c.t] - aw[c.t] * off

    def prepare(c):
        up, down, damp = c.terms()
        de = raw[ED, c.t]
        fe = 0.5 * raw[EW, c.t]
        dn = jnp.where(open_face, raw[ND, c.t], 0.0)
        fn = jnp.where(open_face, 0.5 * raw[NW, c.t], 0.0)
        dnx = rawx[0, c.t]
        fnx = 0.5 * rawx[1, c.t]
        anx, bnx = fnx + dnx, fnx - dnx
        a, b = fe + de, fe - de
        an, bn = fn + dn, fn - dn
        a_w = turn(a, 1)
        b_w = turn(b, 1)
        last = row_ring == rows + wide
        an_s = jnp.where(last, jnp.concatenate([anx, anx], axis=0), turn(an, 1, 0))
        bn_s = jnp.where(last, jnp.concatenate([bnx, bnx], axis=0), turn(bn, 1, 0))
        diag = 1.0 + (a - b_w) + (an - bn_s) + (up + down)
        total = 1.0 + de + 0.5 * (a_w - b_w) + dn + 0.5 * (an_s - bn_s) + (up + down)
        for k, value in enumerate((a, b, a_w, b_w, an, bn, an_s, bn_s, diag, total)):
            coef[k, c.t] = value
        cf[c.t] = raw[CKPT, c.t] + raw[SOURCE, c.t] * c.heat
        resid_forward(c, raw.at[CKPT])

    def prepare_adjoint(c):
        _, _, damp = c.terms()
        diag, total = coef[8, c.t], coef[9, c.t]
        t = jnp.tanh(raw[TRAJ, c.t])
        local = damp * (1.0 - t * t)
        w = RELAXATION / (total + local)
        start_delta = w * raw[ADJF, c.t]
        aw[c.t] = w
        ag[c.t] = 1.0 - w * (diag + local)
        ad[c.t] = start_delta
        aa[c.t] = start_delta

    pairs = ((fa, fb, aa, ab), (fb, fa, ab, aa))
    last = pairs[(INNER - 2) % 2]

    def sweeps(each, base):
        for k in range(INNER - 2):
            f_src, f_dst, a_src, a_dst = pairs[k % 2]

            def body(c):
                f_dst[c.t] = lin_forward(c, f_src)
                a_dst[c.t] = lin_adjoint(c, a_src, base)

            each(body)

    def close_x(c):
        xm[0, c.t, :rows, :] = raw[CKPT, c.t, :rows, :] + lin_forward(c, last[0])[:rows]

    def close_m(c):
        xm[1, c.t, :rows, :] = lin_adjoint(c, last[2], ad)[:rows]

    def second_x(c):
        resid_forward(c, xm.at[0], x1x)

    def second_m(c):
        resid_adjoint(c, xm.at[1])

    def both(first, then):
        def body(c):
            first(c)
            then(c)

        return body

    def close2(c):
        x2[c.t] = xm[0, c.t] + lin_forward(c, last[0])
        mu2[c.t] = xm[1, c.t, :rows, :] + lin_adjoint(c, last[2], ad2)[:rows]

    def finish(c):
        _, _, damp = c.terms()
        x, off = off_forward(c, x2)
        r = x * coef[8, c.t] + off + damp * jnp.tanh(x) - cf[c.t]
        res[c.t] = r[:rows]

    @pl.when(first_x)
    def _():
        known(1, 1, 5, 7)
        start_lon(lon_w)

    arrive(0, up0, down0)
    each_main(prepare)
    arrive(6, up0a, down0a)
    each_main(prepare_adjoint)
    sweeps(each_main, ad)
    each_main(close_x)
    start_down(one_x[1])
    start_up(one_x[0])
    each_main(close_m)
    start_down(one_m[1])
    start_up(one_m[0])

    spot = lane_ring % GROUP
    from_w = (spot > 0) & (spot < halo)
    from_e = (spot >= kept) & (spot < GROUP - 1)
    spot_row = spot[:rows]
    for f in range(FIELDS):
        for side in range(2):
            for j in range(per):
                raw[f, strips + per * side + j, rows:, :] = gather(
                    lambda l: raw[f, l + 1, rows:, :], group_row, side, j
                )
    for k in range(2):
        for side in range(2):
            for j in range(per):
                rawx[k, strips + per * side + j] = gather(lambda l: rawx[k, l + 1], group_row, side, j)
    def unpack(side):
        recv, where, lead, nines = ((recv_w, from_w, 1, NINTH), (recv_e, from_e, kept, (CKPT,)))[side]
        beyond = spot == (0 if side == 0 else GROUP - 1)
        for j in range(per):
            t = strips + per * side + j
            shift = lead - SLOT * j
            for f in range(FIELDS):
                tile = jnp.where(where, turn(recv[f], shift), raw[f, t])
                if f in nines:
                    tile = jnp.where(beyond, turn(recv[FIELDS], shift + nines.index(f)), tile)
                raw[f, t] = tile

    for side, k, copies in ((1, 2, lon_w), (0, 1, lon_e)):
        arrive_lon(k, copies)
        unpack(side)
        each = functools.partial(each_strip, side)
        each(both(prepare, prepare_adjoint))
        sweeps(each, ad)
        each(both(close_x, close_m))
        start_down(one_strips[side][1])
        start_up(one_strips[side][0])

    arrive(3, *one_x)
    each_main(second_x)
    arrive(7, *one_m)
    each_main(second_m)
    sweeps(each_main, ad2)
    each_main(close2)
    each_main(finish)

    east_edge = lane_row >= lanes - DEPTH

    def merge_east():
        for ref, out in ((x2, state_out), (mu2, adj_out), (res, resid_out)):
            for l in range(levels):
                j, g = l % per, l // per
                e = turn(ref[strips + per + j][:rows], lanes - kept - GROUP * g)
                out[l] = jnp.where(east_edge, e, ref[l + 1][:rows])

    for side in (1, 0):
        arrive(4 + side, *one_strips[side])
        each = functools.partial(each_strip, side)
        each(both(second_x, second_m))
        sweeps(each, ad2)
        each(close2)
        each(finish)
        if side == 1:
            merge_east()
            wait_rows(2 * levels * rows, load_sem.at[1])

    west_edge = lane_row < DEPTH

    def west_merged(ref, l, here):
        j, g = l % per, l // per
        return jnp.where(west_edge, turn(ref[strips + j][:rows], -(GROUP * g + halo)), here)

    for l in range(levels):
        x = west_merged(x2, l, state_out[l])
        state_out[l] = x
        adj_out[l] = west_merged(mu2, l, adj_out[l]) + late_ref[1, l] * (x - late_ref[0, l])
        resid_out[l] = west_merged(res, l, resid_out[l])

    flush()


def hand_over(a, b, c, x, y, z, sem):
    gives = [
        pltpu.make_async_copy(held, ref, sem.at[k])
        for k, (held, ref) in enumerate(((a, x), (b, y), (c, z)))
    ]
    for copy in gives:
        copy.start()
    for copy in gives:
        copy.wait()


def solution(mesh):
    nx, ny = mesh.shape["gx"], mesh.shape["gy"]

    def per_device(*arrays):
        levels, rows, lanes = arrays[0].shape
        groups = lanes // GROUP
        assert rows >= 2 * INNER and rows >= INNER + 1 and levels % groups == 0 and nx > 2
        per = levels // groups
        assert per * SLOT <= GROUP and GROUP >= 3 * DEPTH and len(NINTH) <= SLOT
        ring = 2 * rows
        tiles = levels + 2 + 2 * per
        f32 = jnp.float32
        out = jax.ShapeDtypeStruct((levels, rows, lanes), f32)
        hbm = pl.BlockSpec(memory_space=pltpu.HBM)
        vmem = pl.BlockSpec(memory_space=pltpu.VMEM)

        def buf(*shape):
            return pltpu.VMEM(shape, f32)

        def full():
            return buf(tiles, ring, lanes)

        def dma(n):
            return pltpu.SemaphoreType.DMA((n,))

        results = pl.pallas_call(
            functools.partial(kernel, nx, ny),
            name="step_pair",
            out_shape=(pltpu.VMEM(out.shape, f32),) * 3,
            in_specs=[hbm] * 13,
            out_specs=(vmem,) * 3,
            scratch_shapes=[
                buf(FIELDS, tiles, ring, lanes),
                buf(2, tiles, rows, lanes),
                buf(FIELDS + 1, rows, lanes),
                buf(FIELDS + 1, rows, lanes),
                buf(FIELDS + 1, ring, lanes),
                buf(FIELDS + 1, ring, lanes),
                buf(10, tiles, ring, lanes),
                full(),
                buf(2, tiles, ring, lanes),
                buf(tiles, rows, lanes),
                full(),
                buf(tiles, rows, lanes),
                buf(tiles, rows, lanes),
            ]
            + [full() for _ in range(11)]
            + [
                buf(3, per, ring, lanes),
                buf(2, levels, rows, lanes),
                buf(2 * FIELDS * levels * rows, lanes),
                pltpu.SMEM((levels,), f32),
                pltpu.SMEM((levels,), f32),
                pltpu.SMEM((1,), jnp.int32),
                dma(5),
                dma(1),
                dma(8),
                pltpu.SemaphoreType.REGULAR((4,)),
            ],
            compiler_params=pltpu.CompilerParams(
                collective_id=0, has_side_effects=True, vmem_limit_bytes=67043328 - 3 * 4 * math.prod(out.shape)
            ),
        )(*arrays)
        return pl.pallas_call(
            hand_over,
            name="hand_over",
            out_shape=(out, out, out),
            in_specs=[vmem] * 3,
            out_specs=(hbm, hbm, hbm),
            scratch_shapes=[dma(3)],
            compiler_params=pltpu.CompilerParams(vmem_limit_bytes=4 * 2**20),
        )(*results)

    block = P(None, "gy", "gx")
    return jax.shard_map(
        per_device,
        mesh=mesh,
        in_specs=(block,) * 7 + (P(), P(), block, block, block, P()),
        out_specs=(block,) * 3,
        check_vma=False,
    )
```

```python
import functools
import math

import jax
import jax.numpy as jnp
from jax import lax
from jax.experimental import pallas as pl
from jax.experimental.pallas import tpu as pltpu
from jax.sharding import PartitionSpec as P

OUTER = 2
INNER = 4
DAY_STEPS = 96
RELAXATION = 0.7

FIELDS = 8
ND, NW, CKPT, ED, EW, SOURCE, TRAJ, ADJF = range(FIELDS)
FORWARD = 6
CORNER = 5

DEPTH = OUTER * INNER + 1
SLOT = DEPTH - 1
GROUP = 32
NINTH = (CKPT, ED, EW)

MESH = pl.DeviceIdType.MESH


def kernel(
    nx,
    ny,
    ckpt_h,
    traj_h,
    adjf_h,
    ed_h,
    nd_h,
    ew_h,
    nw_h,
    level_h,
    damp_h,
    source_h,
    obs_h,
    weight_h,
    step_h,
    state_out,
    resid_out,
    adj_out,
    raw,
    rawx,
    pack_e,
    pack_w,
    recv_e,
    recv_w,
    coef,
    cf,
    xm,
    x1x,
    x2,
    mu2,
    res,
    fw,
    fg,
    fd,
    fa,
    fb,
    aw,
    ag,
    ad,
    ad2,
    aa,
    ab,
    vert,
    late_ref,
    bytes_ref,
    level_ref,
    damp_ref,
    step_ref,
    load_sem,
    send,
    got,
    hello,
):
    levels, rows, lanes = state_out.shape
    wide = INNER
    ring = 2 * rows
    groups = lanes // GROUP
    per = levels // groups
    strips = levels + 2
    tiles = strips + 2 * per
    halo = DEPTH
    kept = GROUP - halo
    gx = lax.axis_index("gx")
    gy = lax.axis_index("gy")
    east = lax.rem(gx + 1, nx)
    west = lax.rem(gx + nx - 1, nx)
    has_n = gy < ny - 1
    has_s = gy > 0
    north = gy + 1
    south = gy - 1
    first_x = gx == 0
    last_x = gx == nx - 1

    inside = pl.ds(1, levels)
    main = pl.ds(0, rows)

    order = (nd_h, nw_h, ckpt_h, ed_h, ew_h, source_h, traj_h, adjf_h)
    loads = [
        pltpu.make_async_copy(h, raw.at[f, inside, main, :], load_sem.at[0])
        for f, h in enumerate(order)
    ]
    late_loads = [
        pltpu.make_async_copy(obs_h, late_ref.at[0], load_sem.at[1]),
        pltpu.make_async_copy(weight_h, late_ref.at[1], load_sem.at[1]),
    ]
    scalar_loads = [
        pltpu.make_async_copy(level_h, level_ref, load_sem.at[2]),
        pltpu.make_async_copy(damp_h, damp_ref, load_sem.at[3]),
        pltpu.make_async_copy(step_h, step_ref, load_sem.at[4]),
    ]

    for copy in loads:
        copy.start()

    barrier = pltpu.get_barrier_semaphore()
    odd_x = lax.rem(gx, 2) == 1
    odd_y = lax.rem(gy, 2) == 1
    even_y = jnp.logical_not(odd_y)
    inner_x = jnp.logical_not(first_x)
    before_lat = odd_y != last_x
    before_e = jnp.logical_or(last_x, odd_x)
    before_w = jnp.logical_and(inner_x, odd_x)
    before_de = jnp.logical_or(last_x, even_y)
    before_dw = jnp.logical_and(inner_x, even_y)
    neighbours = (
        (east, gy, True, before_e),
        (west, gy, True, before_w),
        (gx, north, has_n, before_lat),
        (gx, south, has_s, before_lat),
        (east, north, has_n, before_de),
        (west, north, has_n, before_dw),
        (east, south, has_s, before_de),
        (west, south, has_s, before_dw),
    )
    answer_to = (1, 0, 3, 2, 1, 0, 1, 0)

    behind = 0
    for k in (7, 5, 1, 2, 3, 0, 4, 6):
        column, row, there, before = neighbours[k]
        behind = behind + jnp.logical_and(there, before).astype(jnp.int32)

        @pl.when(jnp.logical_and(there, jnp.logical_not(before)))
        def _():
            pl.semaphore_signal(
                barrier, inc=1, device_id={"gx": column, "gy": row}, device_id_type=MESH
            )


    @pl.when(behind > 0)
    def _():
        pl.semaphore_wait(barrier, behind)

    for k, (column, row, there, before) in enumerate(neighbours):

        @pl.when(jnp.logical_and(there, before))
        def _():
            pl.semaphore_signal(
                hello.at[answer_to[k]], inc=1, device_id={"gx": column, "gy": row}, device_id_type=MESH
            )

    def known(side, *ks):
        count = 0
        for k in ks:
            _, _, there, before = neighbours[k]
            count = count + jnp.logical_and(there, jnp.logical_not(before)).astype(jnp.int32)

        @pl.when(count > 0)
        def _():
            pl.semaphore_wait(hello.at[side], count)

    def wait_rows(n, sem):
        part = bytes_ref.at[pl.ds(0, n), :]
        pltpu.make_async_copy(part, part, sem).wait()

    def rows_of(copies):
        return sum(math.prod(copy.src_ref.shape) for copy in copies) // lanes

    def remote(src, dst, send, got, column, row):
        return pltpu.make_async_remote_copy(
            src_ref=src,
            dst_ref=dst,
            send_sem=send,
            recv_sem=got,
            device_id={"gx": column, "gy": row},
            device_id_type=MESH,
        )

    low = pl.ds(0, wide)
    high = pl.ds(rows - wide, wide)
    from_n = pl.ds(rows, wide)
    from_s = pl.ds(ring - wide, wide)
    next_low = pl.ds(wide, 1)
    next_high = pl.ds(rows - wide - 1, 1)
    near_low = pl.ds(0, wide - 1)
    near_high = pl.ds(rows - wide + 1, wide - 1)
    near_n = pl.ds(rows, wide - 1)
    near_s = pl.ds(ring - wide + 1, wide - 1)
    last_low = pl.ds(wide - 1, 1)
    last_high = pl.ds(rows - wide, 1)
    last_n = pl.ds(rows + wide - 1, 1)
    last_s = pl.ds(ring - wide, 1)
    extra_n = pl.ds(wide - 1, 1)
    extra_s = pl.ds(wide, 1)

    faces = pl.ds(ND, 2)

    def copy(k, src, dst, column, row):
        return remote(src, dst, send.at[0], got.at[k], column, row)

    fwd = pl.ds(0, FORWARD)
    adj = pl.ds(FORWARD, FIELDS - FORWARD)
    up0 = [
        copy(0, raw.at[fwd, inside, high, :], raw.at[fwd, inside, from_s, :], gx, north),
        copy(0, raw.at[faces, inside, next_high, :], rawx.at[:, inside, extra_s, :], gx, north),
    ]
    down0 = [copy(0, raw.at[fwd, inside, low, :], raw.at[fwd, inside, from_n, :], gx, south)]
    up0a = [copy(6, raw.at[adj, inside, near_high, :], raw.at[adj, inside, near_s, :], gx, north)]
    down0a = [copy(6, raw.at[adj, inside, near_low, :], raw.at[adj, inside, near_n, :], gx, south)]

    every = pl.ds(0, FIELDS)
    some = pl.ds(0, CORNER)

    def lon_copies(k, pack, recv, column):
        return (
            [copy(k, pack, recv.at[:, main, :], column, gy)],
            [
                copy(k, pack.at[every, near_high, :], recv.at[every, near_s, :], column, north),
                copy(k, pack.at[some, last_high, :], recv.at[some, last_s, :], column, north),
            ],
            [
                copy(k, pack.at[every, near_low, :], recv.at[every, near_n, :], column, south),
                copy(k, pack.at[some, last_low, :], recv.at[some, last_n, :], column, south),
            ],
        )

    lon_e = lon_copies(1, pack_e, recv_w, east)
    lon_w = lon_copies(2, pack_w, recv_e, west)

    def one(k, part):
        return (
            [
                copy(k, xm.at[:, part, high, :], xm.at[:, part, from_s, :], gx, north),
                copy(k, xm.at[0, part, next_high, :], x1x.at[part, extra_s, :], gx, north),
            ],
            [
                copy(k, xm.at[:, part, low, :], xm.at[:, part, from_n, :], gx, south),
                copy(k, xm.at[0, part, next_low, :], x1x.at[part, extra_n, :], gx, south),
            ],
        )

    one_x = (
        [
            copy(3, xm.at[0, inside, high, :], xm.at[0, inside, from_s, :], gx, north),
            copy(3, xm.at[0, inside, next_high, :], x1x.at[inside, extra_s, :], gx, north),
        ],
        [
            copy(3, xm.at[0, inside, low, :], xm.at[0, inside, from_n, :], gx, south),
            copy(3, xm.at[0, inside, next_low, :], x1x.at[inside, extra_n, :], gx, south),
        ],
    )
    one_m = (
        [copy(7, xm.at[1, inside, high, :], xm.at[1, inside, from_s, :], gx, north)],
        [copy(7, xm.at[1, inside, low, :], xm.at[1, inside, from_n, :], gx, south)],
    )
    one_strips = (one(4, pl.ds(strips, per)), one(5, pl.ds(strips + per, per)))

    def start_up(up):
        @pl.when(has_n)
        def _():
            for copy in up:
                copy.start()

    def start_down(down):
        @pl.when(has_s)
        def _():
            for copy in down:
                copy.start()

    def start_lon(copies):
        copies[0][0].start()
        start_up(copies[1])
        start_down(copies[2])

    def wait_all(always, up, down, with_up, with_down, sem):
        n, n_up, n_down = rows_of(always), rows_of(up), rows_of(down)
        cases = (
            (jnp.logical_and(with_up, with_down), n + n_up + n_down),
            (jnp.logical_and(with_up, jnp.logical_not(with_down)), n + n_up),
            (jnp.logical_and(with_down, jnp.logical_not(with_up)), n + n_down),
            (jnp.logical_not(jnp.logical_or(with_up, with_down)), n),
        )
        for case, total in cases:
            if total:

                @pl.when(case)
                def _():
                    wait_rows(total, sem)

    def arrive(k, up, down):
        wait_all([], up, down, has_s, has_n, got.at[k])

    def arrive_lon(k, copies):
        wait_all(*copies, has_s, has_n, got.at[k])

    def flush():
        exchanges = ((up0, down0), (up0a, down0a), one_x, one_m, *one_strips, lon_e[1:], lon_w[1:])
        wait_all(
            lon_e[0] + lon_w[0],
            [copy for up, _ in exchanges for copy in up],
            [copy for _, down in exchanges for copy in down],
            has_n,
            has_s,
            send.at[0],
        )

    zero_ring = jnp.zeros((ring, lanes), jnp.float32)
    zero_tile = jnp.zeros((rows, lanes), jnp.float32)
    for t in (0, levels + 1):
        raw[CKPT, t] = zero_ring
        for ref in (fa, fb, aa, ab, x2):
            ref[t] = zero_ring
        for k in range(2):
            xm[k, t] = zero_ring

    def clear(part):
        zero = jnp.zeros((wide, lanes), jnp.float32)

        def body(l, carry):
            for f in range(FIELDS):
                raw[f, l + 1, part, :] = zero
            for k in range(2):
                xm[k, l + 1, part, :] = zero
            return carry

        lax.fori_loop(0, levels, body, 0)
        for t in range(strips, tiles):
            for k in range(2):
                xm[k, t, part, :] = zero
        for f in range(FIELDS + 1):
            recv_e[f, part, :] = zero
            recv_w[f, part, :] = zero

    def clear_extra(part):
        zero = jnp.zeros((1, lanes), jnp.float32)
        for t in [*range(1, levels + 1), *range(strips, tiles)]:
            x1x[t, part, :] = zero

    @pl.when(jnp.logical_not(has_n))
    def _():
        clear(from_n)
        clear_extra(extra_n)

    @pl.when(jnp.logical_not(has_s))
    def _():
        clear(from_s)
        clear_extra(extra_s)
        zero = jnp.zeros((1, lanes), jnp.float32)
        for k in range(2):
            for t in range(1, levels + 1):
                rawx[k, t, extra_s, :] = zero

    wait_rows(levels * FIELDS * rows, load_sem.at[0])

    def send_lat():
        known(2, 2)
        start_up(up0 + up0a)
        known(3, 3)
        start_down(down0 + down0a)

    for copy in scalar_loads + late_loads:
        copy.start()

    @pl.when(jnp.logical_not(last_x))
    def _():
        send_lat()


    lane_row = lax.broadcasted_iota(jnp.int32, (rows, lanes), 1)
    lane_ring = lax.broadcasted_iota(jnp.int32, (ring, lanes), 1)
    row_ring = lax.broadcasted_iota(jnp.int32, (ring, lanes), 0)

    def turn(v, shift, axis=1):
        shift = shift % v.shape[axis]
        return pltpu.roll(v, shift, axis) if shift else v

    def choose(place, values):
        out = values[-1]
        for k in range(len(values) - 2, -1, -1):
            out = jnp.where(place == k, values[k], out)
        return out

    def gather(read, place, side, j):
        start = halo if side == 0 else kept
        return choose(place, [turn(read(j + per * g), GROUP * g + start) for g in range(groups)])

    group_row = lane_row // GROUP
    nine_row = lane_row % SLOT

    def slots(f, shift, turns=(0,)):
        rolled = [turn(raw[f, level_of(k) + 1, :rows, :], SLOT * k + shift) for k in range(levels)]
        return [choose((lane_row // SLOT + move) % levels, rolled) for move in turns]

    def level_of(k):
        return k % per + per * (k // per)

    nine = None
    for f in sorted(range(FIELDS), key=lambda f: f not in NINTH):
        if f in NINTH:
            pack_e[f], beside = slots(f, SLOT, (0, 1))
            i = NINTH.index(f)
            beside = turn(beside, -i)
            nine = beside if nine is None else jnp.where(nine_row == SLOT - 1 - i, beside, nine)
        else:
            (pack_e[f],) = slots(f, SLOT)
    pack_e[FIELDS] = nine

    @pl.when(last_x)
    def _():
        start_lon(lon_e)
        send_lat()

    for f in range(FIELDS):
        if f == CKPT:
            pack_w[f], pack_w[FIELDS] = slots(f, 0, (0, -1))
        else:
            (pack_w[f],) = slots(f, 0)

    @pl.when(inner_x)
    def _():
        known(1, 1, 5, 7)
        start_lon(lon_w)

    @pl.when(jnp.logical_not(last_x))
    def _():
        known(0, 0, 4, 6)
        start_lon(lon_e)

    for f in range(FIELDS):
        for side in range(2):
            for j in range(per):
                raw[f, strips + per * side + j, :rows, :] = gather(
                    lambda l: raw[f, l + 1, :rows, :], group_row, side, j
                )

    for copy in scalar_loads:
        copy.wait()

    total_lanes = lanes * nx

    def heat_of(column):
        column = gx * lanes + column
        column = jnp.where(column < 0, column + total_lanes, column)
        column = jnp.where(column >= total_lanes, column - total_lanes, column)
        phase = (
            2.0 * math.pi * column.astype(jnp.float32) / total_lanes
            - 2.0 * math.pi * step_ref[0].astype(jnp.float32) / DAY_STEPS
        )
        return jnp.cos(phase)

    lane_one = lax.broadcasted_iota(jnp.int32, (1, lanes), 1)
    heat_main = heat_of(lane_one)
    heat_side = (
        heat_of(lane_one % GROUP - halo),
        heat_of(lane_one % GROUP + (lanes - kept)),
    )
    row_global = gy * rows + jnp.where(row_ring < rows + wide, row_ring, row_ring - ring)
    open_face = (row_global >= 0) & (row_global < rows * ny - 1)

    def level_terms(l):
        up = jnp.where(l < levels - 1, level_ref[l], 0.0)
        down = jnp.where(l > 0, level_ref[jnp.maximum(l - 1, 0)], 0.0)
        return up, down, damp_ref[l]

    group_one = lane_ring // GROUP
    for j in range(per):
        terms = [level_terms(j + per * g) for g in range(groups)]
        for k in range(3):
            vert[k, j] = choose(group_one, [jnp.full((ring, lanes), term[k]) for term in terms])

    class Main:
        def __init__(self, l):
            self.t = l + 1
            self.l = l
            self.heat = heat_main

        def terms(self):
            return level_terms(self.l)

        def above(self, ref):
            return ref[self.t + 1]

        def below(self, ref):
            return ref[self.t - 1]

    class Strip:
        def __init__(self, k):
            self.t = strips + k
            self.j = k % per
            self.base = strips + k - self.j
            self.heat = heat_side[k // per]

        def terms(self):
            return vert[0, self.j], vert[1, self.j], vert[2, self.j]

        def above(self, ref):
            if self.j < per - 1:
                return ref[self.t + 1]
            return turn(ref[self.base], -GROUP)

        def below(self, ref):
            if self.j > 0:
                return ref[self.t - 1]
            return turn(ref[self.base + per - 1], GROUP)

    def each_main(body):
        def step(l, carry):
            body(Main(l))
            return carry

        lax.fori_loop(0, levels, step, 0, unroll=True)

    def each_strip(side, body):
        for j in range(per):
            body(Strip(per * side + j))

    def off_forward(c, ref, extra=None):
        up, down, _ = c.terms()
        v = ref[c.t]
        above = turn(v, -1, 0)
        below = turn(v, 1, 0)
        if extra is not None:
            more = jnp.concatenate([extra[c.t], extra[c.t]], axis=0)
            above = jnp.where(row_ring == rows + wide - 1, more, above)
            below = jnp.where(row_ring == rows + wide, more, below)
        off = (
            turn(v, -1) * coef[1, c.t]
            - turn(v, 1) * coef[2, c.t]
            + above * coef[5, c.t]
            - below * coef[6, c.t]
            - up * c.above(ref)
            - down * c.below(ref)
        )
        return v, off

    def off_adjoint(c, ref):
        up, down, _ = c.terms()
        v = ref[c.t]
        off = (
            turn(v, 1) * coef[3, c.t]
            - turn(v, -1) * coef[0, c.t]
            + turn(v, 1, 0) * coef[7, c.t]
            - turn(v, -1, 0) * coef[4, c.t]
            - up * c.above(ref)
            - down * c.below(ref)
        )
        return v, off

    def resid_forward(c, ref, extra=None):
        _, _, damp = c.terms()
        x, off = off_forward(c, ref, extra)
        t = jnp.tanh(x)
        local = damp * (1.0 - t * t)
        diag = coef[8, c.t]
        r = x * diag + off + damp * t - cf[c.t]
        w = RELAXATION / (coef[9, c.t] + local)
        d = -w * r
        fw[c.t] = w
        fg[c.t] = 1.0 - w * (diag + local)
        fd[c.t] = d
        fa[c.t] = d

    def resid_adjoint(c, ref):
        m, off = off_adjoint(c, ref)
        d = ad[c.t] - (1.0 - ag[c.t]) * m - aw[c.t] * off
        ad2[c.t] = d
        aa[c.t] = d

    def lin_forward(c, src):
        v, off = off_forward(c, src)
        return fg[c.t] * v + fd[c.t] - fw[c.t] * off

    def lin_adjoint(c, src, base):
        v, off = off_adjoint(c, src)
        return ag[c.t] * v + base[c.t] - aw[c.t] * off

    def prepare(c):
        up, down, damp = c.terms()
        de = raw[ED, c.t]
        fe = 0.5 * raw[EW, c.t]
        dn = jnp.where(open_face, raw[ND, c.t], 0.0)
        fn = jnp.where(open_face, 0.5 * raw[NW, c.t], 0.0)
        dnx = rawx[0, c.t]
        fnx = 0.5 * rawx[1, c.t]
        anx, bnx = fnx + dnx, fnx - dnx
        a, b = fe + de, fe - de
        an, bn = fn + dn, fn - dn
        a_w = turn(a, 1)
        b_w = turn(b, 1)
        last = row_ring == rows + wide
        an_s = jnp.where(last, jnp.concatenate([anx, anx], axis=0), turn(an, 1, 0))
        bn_s = jnp.where(last, jnp.concatenate([bnx, bnx], axis=0), turn(bn, 1, 0))
        diag = 1.0 + (a - b_w) + (an - bn_s) + (up + down)
        total = 1.0 + de + 0.5 * (a_w - b_w) + dn + 0.5 * (an_s - bn_s) + (up + down)
        for k, value in enumerate((a, b, a_w, b_w, an, bn, an_s, bn_s, diag, total)):
            coef[k, c.t] = value
        cf[c.t] = raw[CKPT, c.t] + raw[SOURCE, c.t] * c.heat
        resid_forward(c, raw.at[CKPT])

    def prepare_adjoint(c):
        _, _, damp = c.terms()
        diag, total = coef[8, c.t], coef[9, c.t]
        t = jnp.tanh(raw[TRAJ, c.t])
        local = damp * (1.0 - t * t)
        w = RELAXATION / (total + local)
        start_delta = w * raw[ADJF, c.t]
        aw[c.t] = w
        ag[c.t] = 1.0 - w * (diag + local)
        ad[c.t] = start_delta
        aa[c.t] = start_delta

    pairs = ((fa, fb, aa, ab), (fb, fa, ab, aa))
    last = pairs[(INNER - 2) % 2]

    def sweeps(each, base):
        for k in range(INNER - 2):
            f_src, f_dst, a_src, a_dst = pairs[k % 2]

            def body(c):
                f_dst[c.t] = lin_forward(c, f_src)
                a_dst[c.t] = lin_adjoint(c, a_src, base)

            each(body)

    def close_x(c):
        xm[0, c.t, :rows, :] = raw[CKPT, c.t, :rows, :] + lin_forward(c, last[0])[:rows]

    def close_m(c):
        xm[1, c.t, :rows, :] = lin_adjoint(c, last[2], ad)[:rows]

    def second_x(c):
        resid_forward(c, xm.at[0], x1x)

    def second_m(c):
        resid_adjoint(c, xm.at[1])

    def both(first, then):
        def body(c):
            first(c)
            then(c)

        return body

    def close2(c):
        x2[c.t] = xm[0, c.t] + lin_forward(c, last[0])
        mu2[c.t] = xm[1, c.t, :rows, :] + lin_adjoint(c, last[2], ad2)[:rows]

    def finish(c):
        _, _, damp = c.terms()
        x, off = off_forward(c, x2)
        r = x * coef[8, c.t] + off + damp * jnp.tanh(x) - cf[c.t]
        res[c.t] = r[:rows]

    @pl.when(first_x)
    def _():
        known(1, 1, 5, 7)
        start_lon(lon_w)

    arrive(0, up0, down0)
    each_main(prepare)
    arrive(6, up0a, down0a)
    each_main(prepare_adjoint)
    sweeps(each_main, ad)
    each_main(close_x)
    start_down(one_x[1])
    start_up(one_x[0])
    each_main(close_m)
    start_down(one_m[1])
    start_up(one_m[0])

    spot = lane_ring % GROUP
    from_w = (spot > 0) & (spot < halo)
    from_e = (spot >= kept) & (spot < GROUP - 1)
    spot_row = spot[:rows]
    for f in range(FIELDS):
        for side in range(2):
            for j in range(per):
                raw[f, strips + per * side + j, rows:, :] = gather(
                    lambda l: raw[f, l + 1, rows:, :], group_row, side, j
                )
    for k in range(2):
        for side in range(2):
            for j in range(per):
                rawx[k, strips + per * side + j] = gather(lambda l: rawx[k, l + 1], group_row, side, j)
    def unpack(side):
        recv, where, lead, nines = ((recv_w, from_w, 1, NINTH), (recv_e, from_e, kept, (CKPT,)))[side]
        beyond = spot == (0 if side == 0 else GROUP - 1)
        for j in range(per):
            t = strips + per * side + j
            shift = lead - SLOT * j
            for f in range(FIELDS):
                tile = jnp.where(where, turn(recv[f], shift), raw[f, t])
                if f in nines:
                    tile = jnp.where(beyond, turn(recv[FIELDS], shift + nines.index(f)), tile)
                raw[f, t] = tile

    for side, k, copies in ((1, 2, lon_w), (0, 1, lon_e)):
        arrive_lon(k, copies)
        unpack(side)
        each = functools.partial(each_strip, side)
        each(both(prepare, prepare_adjoint))
        sweeps(each, ad)
        each(both(close_x, close_m))
        start_down(one_strips[side][1])
        start_up(one_strips[side][0])

    arrive(3, *one_x)
    each_main(second_x)
    arrive(7, *one_m)
    each_main(second_m)
    sweeps(each_main, ad2)
    each_main(close2)
    each_main(finish)

    east_edge = lane_row >= lanes - DEPTH

    def merge_east():
        for ref, out in ((x2, state_out), (mu2, adj_out), (res, resid_out)):
            for l in range(levels):
                j, g = l % per, l // per
                e = turn(ref[strips + per + j][:rows], lanes - kept - GROUP * g)
                out[l] = jnp.where(east_edge, e, ref[l + 1][:rows])

    for side in (1, 0):
        arrive(4 + side, *one_strips[side])
        each = functools.partial(each_strip, side)
        each(both(second_x, second_m))
        sweeps(each, ad2)
        each(close2)
        each(finish)
        if side == 1:
            merge_east()
            wait_rows(2 * levels * rows, load_sem.at[1])

    west_edge = lane_row < DEPTH

    def west_merged(ref, l, here):
        j, g = l % per, l // per
        return jnp.where(west_edge, turn(ref[strips + j][:rows], -(GROUP * g + halo)), here)

    for l in range(levels):
        x = west_merged(x2, l, state_out[l])
        state_out[l] = x
        adj_out[l] = west_merged(mu2, l, adj_out[l]) + late_ref[1, l] * (x - late_ref[0, l])
        resid_out[l] = west_merged(res, l, resid_out[l])

    flush()


def hand_over(a, b, c, x, y, z, sem):
    gives = [
        pltpu.make_async_copy(held, ref, sem.at[k])
        for k, (held, ref) in enumerate(((a, x), (b, y), (c, z)))
    ]
    for copy in gives:
        copy.start()
    for copy in gives:
        copy.wait()


def solution(mesh):
    nx, ny = mesh.shape["gx"], mesh.shape["gy"]

    def per_device(*arrays):
        levels, rows, lanes = arrays[0].shape
        groups = lanes // GROUP
        assert rows >= 2 * INNER and rows >= INNER + 1 and levels % groups == 0 and nx > 2
        per = levels // groups
        assert per * SLOT <= GROUP and GROUP >= 3 * DEPTH and len(NINTH) <= SLOT
        ring = 2 * rows
        tiles = levels + 2 + 2 * per
        f32 = jnp.float32
        out = jax.ShapeDtypeStruct((levels, rows, lanes), f32)
        hbm = pl.BlockSpec(memory_space=pltpu.HBM)
        vmem = pl.BlockSpec(memory_space=pltpu.VMEM)

        def buf(*shape):
            return pltpu.VMEM(shape, f32)

        def full():
            return buf(tiles, ring, lanes)

        def dma(n):
            return pltpu.SemaphoreType.DMA((n,))

        results = pl.pallas_call(
            functools.partial(kernel, nx, ny),
            name="step_pair",
            out_shape=(pltpu.VMEM(out.shape, f32),) * 3,
            in_specs=[hbm] * 13,
            out_specs=(vmem,) * 3,
            scratch_shapes=[
                buf(FIELDS, tiles, ring, lanes),
                buf(2, tiles, rows, lanes),
                buf(FIELDS + 1, rows, lanes),
                buf(FIELDS + 1, rows, lanes),
                buf(FIELDS + 1, ring, lanes),
                buf(FIELDS + 1, ring, lanes),
                buf(10, tiles, ring, lanes),
                full(),
                buf(2, tiles, ring, lanes),
                buf(tiles, rows, lanes),
                full(),
                buf(tiles, rows, lanes),
                buf(tiles, rows, lanes),
            ]
            + [full() for _ in range(11)]
            + [
                buf(3, per, ring, lanes),
                buf(2, levels, rows, lanes),
                buf(2 * FIELDS * levels * rows, lanes),
                pltpu.SMEM((levels,), f32),
                pltpu.SMEM((levels,), f32),
                pltpu.SMEM((1,), jnp.int32),
                dma(5),
                dma(1),
                dma(8),
                pltpu.SemaphoreType.REGULAR((4,)),
            ],
            compiler_params=pltpu.CompilerParams(
                collective_id=0, has_side_effects=True, vmem_limit_bytes=67043328 - 3 * 4 * math.prod(out.shape)
            ),
        )(*arrays)
        return pl.pallas_call(
            hand_over,
            name="hand_over",
            out_shape=(out, out, out),
            in_specs=[vmem] * 3,
            out_specs=(hbm, hbm, hbm),
            scratch_shapes=[dma(3)],
            compiler_params=pltpu.CompilerParams(vmem_limit_bytes=4 * 2**20),
        )(*results)

    block = P(None, "gy", "gx")
    return jax.shard_map(
        per_device,
        mesh=mesh,
        in_specs=(block,) * 7 + (P(), P(), block, block, block, P()),
        out_specs=(block,) * 3,
        check_vma=False,
    )
```
